128 devices in a mesh: row: 16 (over x_hi, y, core), col: 4 (over z), dp: 2 (over x_lo).
Axes of the slice: x: 4 (x_hi: 2, x_lo: 2; x = x_hi * 2 + x_lo), y: 4, z: 4, core: 2. Of those that a mesh axis runs over, the one named last changes fastest.
Arguments:
- slides: bfloat16 [2, 256, 128, 512], P('dp', 'row', 'col'), may hold values from -6 to 6
- cotangent: bfloat16 [2, 256, 128, 512], P('dp', 'row', 'col'), may hold values from -6 to 6
- kernel: float32 [2, 7, 7, 512], replicated, may hold values from -0.875 to 0.875
- kernel_bias: float32 [2, 512], replicated, may hold values from -3 to 3
- norm_gain: float32 [2, 512], replicated, may hold values from 0.1 to 1.9
- norm_bias: float32 [2, 512], replicated, may hold values from -3 to 3
- weight_in: bfloat16 [2, 512, 2048], P(None, 'dp'), may hold values from -0.25 to 0.25
- bias_in: float32 [2, 2048], replicated, may hold values from -3 to 3
- weight_out: bfloat16 [2, 2048, 512], P(None, None, 'dp'), may hold values from -0.125 to 0.125
- bias_out: float32 [2, 512], replicated, may hold values from -3 to 3
- layer_scale: float32 [2, 512], replicated, may hold values from 0.3 to 1.5
Outputs:
- output: bfloat16 [2, 256, 128, 512], P('dp', 'row', 'col')
- grad_slides: bfloat16 [2, 256, 128, 512], P('dp', 'row', 'col')
- grad_weight_in: float32 [2, 512, 2048], P(None, 'dp')
- grad_weight_out: float32 [2, 2048, 512], P(None, None, 'dp')
- grad_kernel: float32 [2, 7, 7, 512], replicated
- grad_channel: float32 [2, 5, 512], replicated
- grad_bias_in: float32 [2, 2048], replicated
The draws below stay inside these ranges and needn't reach their ends.
All inputs are finite; a program needn't handle non-finite values.
Results may differ from the reference program's by a relative error of at most 0.01.
Values may be sent and summed in bfloat16 or wider, within the bound.
A program may use at most 128 MiB of HBM per device.

```python
import math
import jax
import jax.numpy as jnp
from jax import lax

D = 512
FF = 2048
LAYERS = 2
SLIDES = 2
HEIGHT = 256
WIDTH = 128


def shard_levels(rng, shape, pieces, smallest, high):
    def one(position, blocks):
        steps = jax.random.uniform(jax.random.fold_in(jax.random.fold_in(rng, 6), position), (blocks,), jnp.float32, smallest / len(pieces), high / len(pieces))
        return jnp.repeat(jnp.exp(steps), shape[position] // blocks).reshape((-1,) + (1,) * (len(shape) - position - 1))

    loudness = one(*pieces[0])
    for cut in pieces[1:]:
        loudness = loudness * one(*cut)
    return loudness


def normal_values(key, dims, spread, reach, cuts=(), held_as=jnp.bfloat16):
    factor_of = shard_levels(key, dims, cuts, -0.22, 0.18) if cuts else 1.0
    entries = jax.random.normal(key, dims, jnp.float32) * spread * factor_of
    return jnp.minimum(jnp.maximum(entries, -reach), reach).astype(held_as)


def setup_inputs(seed: int = 0) -> dict:
    key_list = jax.random.split(jax.random.key(seed), 12)
    slides = normal_values(key_list[0], (SLIDES, HEIGHT, WIDTH, D), 1.0, 6.0, ((0, 2), (1, 16), (2, 4)))
    cotangent = normal_values(key_list[1], (SLIDES, HEIGHT, WIDTH, D), 1.0, 6.0, ((0, 2), (1, 16), (2, 4)))
    kernel = normal_values(key_list[2], (LAYERS, 7, 7, D), 49 ** -0.5, 0.875, (), jnp.float32)
    kernel_bias = normal_values(key_list[3], (LAYERS, D), 0.5, 3.0, (), jnp.float32)
    norm_gain = jnp.clip(1.0 + 0.18 * jax.random.normal(key_list[4], (LAYERS, D), jnp.float32), 0.1, 1.9)
    norm_bias = normal_values(key_list[5], (LAYERS, D), 0.5, 3.0, (), jnp.float32)
    weight_in = normal_values(key_list[6], (LAYERS, D, FF), D ** -0.5, 0.25, ((1, 2),))
    bias_in = normal_values(key_list[7], (LAYERS, FF), 0.5, 3.0, (), jnp.float32)
    weight_out = normal_values(key_list[8], (LAYERS, FF, D), FF ** -0.5, 0.125, ((2, 2),))
    bias_out = normal_values(key_list[9], (LAYERS, D), 0.5, 3.0, (), jnp.float32)
    layer_scale = jnp.clip(jnp.exp(jax.random.uniform(key_list[10], (LAYERS, D), jnp.float32, math.log(0.3), math.log(1.5))), 0.3, 1.5)
    return dict(slides=slides, cotangent=cotangent, kernel=kernel, kernel_bias=kernel_bias, norm_gain=norm_gain, norm_bias=norm_bias, weight_in=weight_in, bias_in=bias_in, weight_out=weight_out, bias_out=bias_out, layer_scale=layer_scale)


COEF = 0.7978845608028654
CUBIC = 0.044715
EPSILON = 1e-06

def gelu_tanh(values):
    inner = COEF * (values + CUBIC * values * values * values)
    return 0.5 * values * (1.0 + jnp.tanh(inner))

def gelu_slope(values):
    tangent = jnp.tanh(COEF * (values + CUBIC * values * values * values))
    return 0.5 * (1.0 + tangent) + 0.5 * values * (1.0 - tangent * tangent) * COEF * (1.0 + 3.0 * CUBIC * values * values)

def depthwise(padded, taps):
    height = padded.shape[1] - 6
    width = padded.shape[2] - 6
    total = jnp.zeros((padded.shape[0], height, width, padded.shape[3]), jnp.float32)
    for row_tap in range(7):
        for col_tap in range(7):
            window = padded[:, row_tap:row_tap + height, col_tap:col_tap + width, :].astype(jnp.float32)
            total = total + window * taps[row_tap, col_tap]
    return total

def tap_grads(padded, upstream):
    height = upstream.shape[1]
    width = upstream.shape[2]
    rows_out = []
    for row_tap in range(7):
        line = []
        for col_tap in range(7):
            window = padded[:, row_tap:row_tap + height, col_tap:col_tap + width, :].astype(jnp.float32)
            line.append(lax.optimization_barrier(jnp.sum(window * upstream, axis=(0, 1, 2))))
        rows_out.append(jnp.stack(line))
    return jnp.stack(rows_out)

def forward_layer(padded, current, taps, tap_bias, gain, shift, weight_in, bias_in, weight_out, bias_out, scale):
    channels = current.shape[-1]
    mixed = (depthwise(padded, taps) + tap_bias).reshape(-1, channels)
    center = mixed - lax.optimization_barrier(jnp.mean(mixed, -1, keepdims=True))
    rstd = lax.rsqrt(lax.optimization_barrier(jnp.mean(center * center, -1, keepdims=True)) + EPSILON)
    normed = center * rstd
    normal_low = (normed * gain + shift).astype(jnp.bfloat16)
    hidden = jnp.dot(normal_low, weight_in, preferred_element_type=jnp.float32) + bias_in
    activated = gelu_tanh(hidden).astype(jnp.bfloat16)
    branch = jnp.dot(activated, weight_out, preferred_element_type=jnp.float32) + bias_out
    result = current.reshape(-1, channels).astype(jnp.float32) + scale * branch
    result = result.astype(jnp.bfloat16).reshape(current.shape)
    return (result, (normed, rstd, normal_low, hidden, activated, branch))

def backward_layer(upstream, saved, gain, weight_in, weight_out, scale):
    normed, rstd, normal_low, hidden, activated, branch = saved
    contract_rows = (((0,), (0,)), ((), ()))
    contract_cols = (((1,), (1,)), ((), ()))
    grad_scale = lax.optimization_barrier(jnp.sum(upstream * branch, 0))
    grad_branch = upstream * scale
    grad_bias_out = lax.optimization_barrier(jnp.sum(grad_branch, 0))
    branch_low = grad_branch.astype(jnp.bfloat16)
    grad_weight_out = lax.dot_general(activated, branch_low, contract_rows, preferred_element_type=jnp.float32)
    grad_act = lax.dot_general(branch_low, weight_out, contract_cols, preferred_element_type=jnp.float32)
    grad_hidden = grad_act * gelu_slope(hidden)
    grad_bias_in = lax.optimization_barrier(jnp.sum(grad_hidden, 0))
    hidden_low = grad_hidden.astype(jnp.bfloat16)
    grad_weight_in = lax.dot_general(normal_low, hidden_low, contract_rows, preferred_element_type=jnp.float32)
    grad_normal = lax.dot_general(hidden_low, weight_in, contract_cols, preferred_element_type=jnp.float32)
    grad_gain = lax.optimization_barrier(jnp.sum(grad_normal * normed, 0))
    grad_shift = lax.optimization_barrier(jnp.sum(grad_normal, 0))
    scaled = grad_normal * gain
    grad_mixed = rstd * (scaled - lax.optimization_barrier(jnp.mean(scaled, -1, keepdims=True)) - normed * lax.optimization_barrier(jnp.mean(scaled * normed, -1, keepdims=True)))
    grad_tap_bias = lax.optimization_barrier(jnp.sum(grad_mixed, 0))
    channel_grads = jnp.stack([grad_tap_bias, grad_gain, grad_shift, grad_bias_out, grad_scale])
    return (grad_mixed, grad_weight_in, grad_weight_out, grad_bias_in, channel_grads)

def pad_map(values):
    return jnp.pad(values, ((0, 0), (3, 3), (3, 3), (0, 0)))

def reference(slides, cotangent, kernel, kernel_bias, norm_gain, norm_bias, weight_in, bias_in, weight_out, bias_out, layer_scale):
    layers = weight_in.shape[0]
    channels = slides.shape[-1]
    current = slides
    caches = []
    paddings = []
    for which in range(layers):
        padded = pad_map(current)
        current, cache = forward_layer(padded, current, kernel[which], kernel_bias[which], norm_gain[which], norm_bias[which], weight_in[which], bias_in[which], weight_out[which], bias_out[which], layer_scale[which])
        caches.append(cache)
        paddings.append(padded)
    output = current
    upstream = cotangent.astype(jnp.float32).reshape(-1, channels)
    grads_in = [None] * layers
    grads_out = [None] * layers
    grads_kernel = [None] * layers
    grads_channel = [None] * layers
    grads_bias = [None] * layers
    for which in reversed(range(layers)):
        grad_mixed, grad_in, grad_out, grad_bias, channel_grads = backward_layer(upstream, caches[which], norm_gain[which], weight_in[which], weight_out[which], layer_scale[which])
        shaped = grad_mixed.reshape(slides.shape)
        grads_kernel[which] = tap_grads(paddings[which], shaped)
        back = depthwise(pad_map(shaped), kernel[which][::-1, ::-1])
        upstream = upstream + back.reshape(-1, channels)
        grads_in[which] = grad_in
        grads_out[which] = grad_out
        grads_channel[which] = channel_grads
        grads_bias[which] = grad_bias
    grad_slides = upstream.astype(jnp.bfloat16).reshape(slides.shape)
    return (output, grad_slides, jnp.stack(grads_in), jnp.stack(grads_out), jnp.stack(grads_kernel), jnp.stack(grads_channel), jnp.stack(grads_bias))
```

```python
import functools

import jax
import jax.numpy as jnp
from jax import lax
from jax.experimental import pallas as pl
from jax.experimental.pallas import tpu as pltpu
from jax.sharding import PartitionSpec as P

COEF = 0.7978845608028654
CUBIC = 0.044715
EPSILON = 1e-06

MESH = pl.DeviceIdType.MESH
BF = jnp.bfloat16
F32 = jnp.float32


class Place:
    def __init__(self):
        row = lax.axis_index("row")
        self.z = lax.axis_index("col")
        self.half = lax.axis_index("dp")
        self.core = lax.rem(row, 2)
        self.y = lax.rem(lax.div(row, 2), 4)
        self.x = lax.div(row, 8) * 2 + self.half

    def device(self, x=None, y=None, z=None, core=None):
        x = self.x if x is None else x
        y = self.y if y is None else y
        z = self.z if z is None else z
        core = self.core if core is None else core
        return {"row": (lax.div(x, 2) * 4 + y) * 2 + core, "col": z, "dp": lax.rem(x, 2)}

    def along(self, axis, offset):
        value = lax.rem(getattr(self, axis) + offset, 4)
        return value, self.device(**{axis: value})

    def sibling(self):
        return self.device(core=1 - self.core)


def meet(partners):
    barrier = pltpu.get_barrier_semaphore()
    for partner in partners:
        pl.semaphore_signal(barrier, inc=1, device_id=partner, device_id_type=MESH)
    pl.semaphore_wait(barrier, len(partners))


def part(start, size):
    if isinstance(start, int):
        return pl.ds(start, size)
    return pl.ds(pl.multiple_of(start, size), size)


def remote(src, dst, send, recv, target):
    return pltpu.make_async_remote_copy(
        src_ref=src, dst_ref=dst, send_sem=send, recv_sem=recv, device_id=target, device_id_type=MESH
    )


ORDERS = (("y", "z"), ("z", "y"))


class WeightIn:
    received = (2, 128, 2048)
    first = (2, 64, 512)
    second = (2, 64, 128)
    third = (64, 128)

    def offered(grad, half, core):
        return grad.at[part(half * 256 + core * 128, 128), :]

    def cut(got, turn, index):
        return got.at[:, turn * 64 : turn * 64 + 64, part(index * 512, 512)]

    def cut_again(block, index):
        return block.at[:, :, part(index * 128, 128)]

    def placed(final, core, turn, one, two):
        return final.at[part(core * 128 + turn * 64, 64), part(one * 512 + two * 128, 128)]

    def line(final, core, turn, one):
        return final.at[part(core * 128 + turn * 64, 64), part(one * 512, 512)]

    def of_core(final, core):
        return final.at[part(core * 128, 128), :]


class WeightOut:
    received = (2, 2048, 128)
    first = (2, 256, 128)
    second = (2, 64, 128)
    third = (64, 128)

    def offered(grad, half, core):
        return grad.at[:, part(half * 256 + core * 128, 128)]

    def cut(got, turn, index):
        return got.at[:, part(turn * 1024 + index * 256, 256), :]

    def cut_again(block, index):
        return block.at[:, part(index * 64, 64), :]

    def placed(final, core, turn, one, two):
        return final.at[part(turn * 1024 + one * 256 + two * 64, 64), part(core * 128, 128)]

    def line(final, core, turn, one):
        return final.at[part(turn * 1024 + one * 256, 256), part(core * 128, 128)]

    def of_core(final, core):
        return final.at[:, part(core * 128, 128)]


class Small:
    received = (1, 64, 512)
    first = (1, 32, 128)
    second = (1, 8, 128)
    third = (8, 128)

    def offered(grad, half, core):
        return grad.at[part(core * 64, 64), :]

    def cut(got, turn, index):
        return got.at[:, turn * 32 : turn * 32 + 32, part(index * 128, 128)]

    def cut_again(block, index):
        return block.at[:, part(index * 8, 8), :]

    def placed(final, core, turn, one, two):
        return final.at[part(core * 64 + turn * 32 + two * 8, 8), part(one * 128, 128)]

    def line(final, core, turn, one):
        return final.at[part(core * 64 + turn * 32, 32), part(one * 128, 128)]

    def of_core(final, core):
        return final.at[part(core * 64, 64), :]


class Reduction:
    def __init__(self, me, kind, grad, final, bufs, sems):
        self.me, self.kind, self.grad, self.final = me, kind, grad, final
        self.got, self.r1, self.b1, self.r2, self.b2, self.r3 = bufs
        self.sems = sems
        self.halves = 1 if kind is Small else 2
        self.copies = []

    def sem(self, way, turn, step, slot):
        return self.sems.at[way, (turn * 7 + step) * 4 + slot]

    def go(self, src, dst, turn, step, send_slot, recv_slot, target):
        copy = remote(
            src, dst, self.sem(0, turn, step, send_slot), self.sem(1, turn, step, recv_slot), target
        )
        copy.start()
        self.copies.append(copy)

    def landed(self, dst, turn, step, slot):
        remote(
            dst, dst, self.sem(0, turn, step, slot), self.sem(1, turn, step, slot), self.me.sibling()
        ).wait_recv()

    def core_start(self):
        for half in range(self.halves):
            src = self.kind.offered(self.grad, half, 1 - self.me.core)
            self.go(src, self.got.at[half], 0, 0, half, half, self.me.sibling())

    def core_finish(self):
        for half in range(self.halves):
            self.landed(self.got.at[half], 0, 0, half)
            own = self.kind.offered(self.grad, half, self.me.core)
            total = own[...].astype(F32) + self.got[half].astype(F32)
            self.got[half] = total.astype(self.got.dtype)

    def block(self, turn, step, index):
        if step == 0:
            return self.kind.cut(self.got, turn, index)
        return self.kind.cut_again(self.b1.at[turn], index)

    def split_start(self, step):
        target = (self.r1, self.r2)[step]
        for turn in range(2):
            for offset in (1, 3, 2):
                index, device = self.me.along(ORDERS[turn][step], offset)
                self.go(
                    self.block(turn, step, index),
                    target.at[turn, offset - 1],
                    turn,
                    1 + step,
                    offset,
                    offset,
                    device,
                )

    def split_finish(self, step):
        target, result = ((self.r1, self.b1), (self.r2, self.b2))[step]
        for turn in range(2):
            index = getattr(self.me, ORDERS[turn][step])
            total = self.block(turn, step, index)[...].astype(F32)
            for offset in (1, 3, 2):
                self.landed(target.at[turn, offset - 1], turn, 1 + step, offset)
                total = total + target[turn, offset - 1].astype(F32)
            result[turn] = total.astype(result.dtype)

    def across_start(self):
        for turn in range(2):
            block = self.b2.at[turn]
            for offset in (1, 3, 2):
                index, device = self.me.along("x", offset)
                src = block.at[lax.rem(index, 2) if self.halves == 2 else 0]
                self.go(src, self.r3.at[turn, self.me.x], turn, 3, offset, self.me.x, device)
            self.r3[turn, self.me.x] = block[self.me.half if self.halves == 2 else 0]

    def across_finish(self):
        me = self.me
        for turn in range(2):
            for offset in (1, 3, 2):
                index, _ = me.along("x", offset)
                self.landed(self.r3.at[turn, index], turn, 3, index)
            total = self.r3[turn, 0].astype(F32)
            for index in range(1, 4):
                total = total + self.r3[turn, index].astype(F32)
            one, two = (getattr(me, axis) for axis in ORDERS[turn])
            block = self.kind.placed(self.final, me.core, turn, one, two)
            block[...] = total.astype(self.final.dtype)

    def join_start(self, step):
        me = self.me
        for turn in range(2):
            one, two = (getattr(me, axis) for axis in ORDERS[turn])
            for offset in (1, 3, 2):
                _, device = me.along(ORDERS[turn][step], offset)
                if step == 1:
                    block = self.kind.placed(self.final, me.core, turn, one, two)
                else:
                    block = self.kind.line(self.final, me.core, turn, one)
                self.go(block, block, turn, 5 - step, offset, offset, device)

    def join_finish(self, step):
        me = self.me
        for turn in range(2):
            one, two = (getattr(me, axis) for axis in ORDERS[turn])
            for offset in (1, 3, 2):
                source = lax.rem((two if step == 1 else one) + 4 - offset, 4)
                if step == 1:
                    block = self.kind.placed(self.final, me.core, turn, one, source)
                else:
                    block = self.kind.line(self.final, me.core, turn, source)
                self.landed(block, turn, 5 - step, offset)

    def share_start(self):
        block = self.kind.of_core(self.final, self.me.core)
        self.go(block, block, 0, 6, 0, 0, self.me.sibling())

    def share_finish(self):
        block = self.kind.of_core(self.final, 1 - self.me.core)
        self.landed(block, 0, 6, 0)

    def drain(self):
        for copy in self.copies:
            copy.wait_send()


def reduction_scratch(kind):
    dtype = F32 if kind is Small else BF
    return [
        pltpu.VMEM(kind.received, dtype),
        pltpu.VMEM((2, 3, *kind.first), dtype),
        pltpu.VMEM((2, *kind.first), dtype),
        pltpu.VMEM((2, 3, *kind.second), dtype),
        pltpu.VMEM((2, *kind.second), dtype),
        pltpu.VMEM((2, 4, *kind.third), dtype),
        pltpu.SemaphoreType.DMA((2, 56)),
    ]


UNITS = ((Small, None), (WeightOut, 1), (WeightIn, 1), (WeightOut, 0), (WeightIn, 0))


class Gather:
    def __init__(self, me, shard_in, shard_out, full_in, full_out, sems):
        self.me = me
        self.shards = (shard_in, shard_out)
        self.full = (full_in, full_out)
        self.local, self.send, self.recv, self.send_core, self.recv_core = sems
        self.sides = (me.along("x", 1)[1], me.along("x", 3)[1])
        self.copies = []

    def block(self, which, kind, half, core, side):
        full = self.full[kind].at[which]
        if kind == 0:
            return full.at[part(half * 256 + core * 128 + side * 64, 64), :]
        return full.at[part(core * 1024 + side * 512, 512), part(half * 256, 256)]

    def place(self, which, kind):
        half = part(self.me.half * 256, 256)
        full = self.full[kind].at[which]
        own = full.at[half, :] if kind == 0 else full.at[:, half]
        return pltpu.make_async_copy(self.shards[kind].at[which], own, self.local.at[which, kind])

    def hop(self, which, kind, half, core, side, across):
        block = self.block(which, kind, half, core, side)
        if across:
            sems, target = (self.send, self.recv), self.sides[side]
        else:
            sems, target = (self.send_core, self.recv_core), self.me.sibling()
        return remote(block, block, *(s.at[which, kind, side] for s in sems), target)

    def start(self, which, kind):
        self.place(which, kind).wait()
        for side in range(2):
            copy = self.hop(which, kind, self.me.half, self.me.core, side, True)
            copy.start()
            self.copies.append(copy)

    def forward(self, which, kind):
        other = 1 - self.me.half
        for side in range(2):
            self.hop(which, kind, other, self.me.core, side, True).wait_recv()
            copy = self.hop(which, kind, other, self.me.core, side, False)
            copy.start()
            self.copies.append(copy)

    def finish(self, which, kind):
        for side in range(2):
            self.hop(which, kind, 1 - self.me.half, 1 - self.me.core, side, False).wait_recv()

    def drain(self):
        for copy in self.copies:
            copy.wait_send()


SPAN = 38
BACK, FRONT = 14, 8


def word(i, j):
    start = (i * SPAN + j) * 8
    return pl.ds(start if isinstance(start, int) else pl.multiple_of(start, 8), 8)


def put_row(padded, row, first, values, halves=(0, 1)):
    for half in halves:
        i = row - 8 * half
        if 0 <= i < BACK:
            for group in range(4):
                padded[pl.ds((i * SPAN + first) * 8 + half * 4 + group, values.shape[0], stride=8), :] = (
                    values[:, group * 128 : group * 128 + 128]
                )


def rolled(values):
    return jnp.concatenate([values[4:], values[:4]], axis=0)


class Halo:
    def __init__(self, me, padded, tile, bufs):
        self.me, self.padded, self.tile = me, padded, tile
        self.rows, self.side_out, self.sides, self.corner_out, self.corners, self.sems = bufs
        self.copies = []
        self.row = (lax.div(me.x, 2) * 4 + me.y) * 2 + me.core

    def target(self, down, right):
        row = lax.rem(self.row + down + 16, 16)
        col = lax.rem(self.me.z + right + 4, 4)
        return {"row": row, "col": col, "dp": self.me.half}

    def messages(self):
        tile = self.tile
        yield tile.at[pl.ds(0, 96), :], self.rows.at[1], (-1, 0)
        yield tile.at[pl.ds(416, 96), :], self.rows.at[0], (1, 0)
        for side in range(2):
            yield self.side_out.at[side], self.sides.at[1 - side], (0, 2 * side - 1)
        for low in range(2):
            for side in range(2):
                yield (
                    self.corner_out.at[low, side],
                    self.corners.at[1 - low, 1 - side],
                    (2 * low - 1, 2 * side - 1),
                )

    def start(self):
        padded = self.padded
        for side, first in ((0, 3), (1, 32)):
            for j in range(3):
                lines = [padded[word(i, first + j), :] for i in range(3, 11)]
                self.side_out[side, j * 64 : j * 64 + 64, :] = jnp.concatenate(lines, 0).astype(BF)
            for low, top in ((0, 3), (1, 8)):
                lines = [
                    rolled(padded[word(top + i, first + j), :]) for i in range(3) for j in range(3)
                ]
                self.corner_out[low, side] = jnp.concatenate(lines + lines[:1], 0).astype(BF)
        for number, (src, dst, (down, right)) in enumerate(self.messages()):
            copy = remote(
                src, dst, self.sems.at[0, number], self.sems.at[1, number], self.target(down, right)
            )
            copy.start()
            self.copies.append(copy)

    def finish(self):
        padded = self.padded
        for number, (src, dst, _) in enumerate(self.messages()):
            remote(
                src, dst, self.sems.at[0, number], self.sems.at[1, number], self.target(1, 0)
            ).wait_recv()
        inside = [
            (self.row > 0).astype(F32),
            (self.row < 15).astype(F32),
        ]
        across = [
            (self.me.z > 0).astype(F32),
            (self.me.z < 3).astype(F32),
        ]
        for low in range(2):
            for r in range(3):
                values = self.rows[low, r * 32 : r * 32 + 32, :].astype(F32) * inside[low]
                put_row(padded, r + 19 * low, 3, values, (low,))
        for side, first in ((0, 0), (1, 35)):
            for j in range(3):
                lines = self.sides[side, j * 64 : j * 64 + 64, :].astype(F32) * across[side]
                for m in range(8):
                    line = lines[m * 8 : m * 8 + 8]
                    padded[word(m + 3, first + j), :] = line
                    at = first + j
                    if m >= 5:
                        padded[pl.ds(((m - 5) * SPAN + at) * 8 + 4, 4), :] = line[:4]
                    if m < 3:
                        padded[pl.ds(((m + 11) * SPAN + at) * 8, 4), :] = line[4:]
            for low in range(2):
                lines = self.corners[low, side].astype(F32) * (inside[low] * across[side])
                for i in range(3):
                    for j in range(3):
                        line = lines[(i * 3 + j) * 8 : (i * 3 + j) * 8 + 8]
                        start = ((i + 11 * low) * SPAN + first + j) * 8 + 4 * low
                        padded[pl.ds(start, 4), :] = line[4 * low : 4 * low + 4]

    def drain(self):
        for copy in self.copies:
            copy.wait_send()


def spread_taps(kernel, which, taps):
    for first in range(0, 56, 8):
        count = min(8, 49 - first)
        if count <= 0:
            break
        for group in range(4):
            values = kernel[which, first : first + count, group * 128 : group * 128 + 128]
            for half in range(2):
                if count == 8:
                    taps[pl.ds(first * 8 + half * 4 + group, 8, stride=8), :] = values
                else:
                    taps[pl.ds(first * 8 + half * 4 + group, 1), :] = values


def depthwise(padded, taps, result, flipped):
    def column(j, _):
        total = [None] * FRONT
        for q in range(7):
            values = [padded[word(i, j + q), :] for i in range(BACK)]
            for p in range(7):
                number = (6 - p) * 7 + 6 - q if flipped else p * 7 + q
                tap = taps[number * 8 : number * 8 + 8, :]
                for i in range(FRONT):
                    term = values[i + p] * tap
                    total[i] = term if total[i] is None else total[i] + term
        for i in range(FRONT):
            result[pl.ds(pl.multiple_of((i * 32 + j) * 8, 8), 8), :] = total[i]
        return 0

    lax.fori_loop(0, 32, column, 0)


def tap_grads(padded, upstream, small, base):
    for q in range(7):

        def column(j, totals):
            values = [padded[word(i, j + q), :] for i in range(BACK)]
            grads = [upstream[word(i + 3, j + 3), :] for i in range(FRONT)]
            result = []
            for p in range(7):
                total = totals[p]
                for i in range(FRONT):
                    total = total + values[i + p] * grads[i]
                result.append(total)
            return tuple(result)

        zero = jnp.zeros((8, 128), F32)
        totals = lax.fori_loop(0, 32, column, (zero,) * 7)
        for p in range(7):
            both = totals[p][:4] + totals[p][4:]
            for group in range(4):
                small[base + p * 7 + q : base + p * 7 + q + 1, group * 128 : group * 128 + 128] = both[
                    group : group + 1
                ]


def pixels(result, row):
    half, i = row // 8, row % 8
    return jnp.concatenate(
        [result[pl.ds(i * 256 + half * 4 + group, 32, stride=8), :] for group in range(4)], axis=1
    )


def dot(left, right, left_dim=1, right_dim=0):
    return lax.dot_general(
        left, right, (((left_dim,), (right_dim,)), ((), ())), preferred_element_type=F32
    )


def gelu_and_slope(values):
    square = values * values
    tangent = jnp.tanh(COEF * values * (1.0 + CUBIC * square))
    lift = 0.5 * (1.0 + tangent)
    slope = lift + 0.5 * values * (1.0 - tangent * tangent) * (COEF + (3.0 * COEF * CUBIC) * square)
    return values * lift, slope


CHUNK = 256


def step_kernel(
    slides, cotangent, kernel, channel, bias_in, shard_in, shard_out,
    output, grad_slides, final_in, final_out, final_small,
    full_in, full_out, padded0, padded1, padded_g, result, taps,
    normed, rstd, normal, turned, act, slope, hidden_grad, branch, carry, upstream, low,
    gm_tile, middle, grad_in, grad_out, small,
    *rest,
):
    me = Place()
    gather = Gather(me, shard_in, shard_out, full_in, full_out, rest[:5])
    padded = (padded0, padded1)
    tiles = (slides, middle)
    halos = [
        Halo(me, grid, tile, rest[5 + 6 * k : 11 + 6 * k])
        for k, (grid, tile) in enumerate(
            ((padded0, slides), (padded1, middle), (padded_g, gm_tile.at[1]), (padded_g, gm_tile.at[0]))
        )
    ]
    scratch = rest[30:]
    ways = {}
    for number, (kind, which) in enumerate(UNITS):
        bufs = scratch[number * 7 : number * 7 + 6]
        sems = scratch[number * 7 + 6]
        if kind is Small:
            ends = (small, final_small)
        elif kind is WeightIn:
            ends = (grad_in.at[which], final_in.at[which])
        else:
            ends = (grad_out.at[which], final_out.at[which])
        ways[kind, which] = Reduction(me, kind, *ends, bufs, sems)

    def reducing(which):
        return [ways[WeightOut, which], ways[WeightIn, which]]

    def line(which, number):
        return channel[which, number : number + 1, :]

    for which in range(2):
        for kind in range(2):
            gather.place(which, kind).start()

    def fill(grid, tile):
        for r in range(16):
            put_row(grid, r + 3, 3, tile[r * 32 : r * 32 + 32, :].astype(F32))

    fill(padded0, slides)
    partners = [me.along(axis, offset)[1] for axis in "xyz" for offset in (1, 2, 3)]
    around = [
        halos[0].target(down, right)
        for down in (-1, 0, 1)
        for right in (-1, 0, 1)
        if (down, right) != (0, 0)
    ]
    meet(partners + around + [me.sibling()])
    halos[0].start()
    gather.start(0, 0)
    gather.start(0, 1)
    gather.start(1, 0)
    for which in range(2):
        spread_taps(kernel, which, taps.at[which])
    small[...] = jnp.zeros_like(small)
    halos[0].finish()

    def normalise(which):
        depthwise(padded[which], taps.at[which], result, False)
        for r in range(16):
            rows = slice(r * 32, r * 32 + 32)
            mixed = pixels(result, r) + line(which, 0)
            center = mixed - jnp.mean(mixed, -1, keepdims=True)
            inverse = lax.rsqrt(jnp.mean(center * center, -1, keepdims=True) + EPSILON)
            values = center * inverse
            normed[which, rows, :] = values
            rstd[which, rows, :] = jnp.broadcast_to(inverse, (32, 128))
            normal[which, rows, :] = (values * line(which, 1) + line(which, 2)).astype(BF)

    def expand(which, with_grad):
        def chunk(c, _):
            cols = part(c * CHUNK, CHUNK)
            hidden = dot(normal[which], full_in[which, :, cols]) + bias_in[which : which + 1, cols]
            value, tilt = gelu_and_slope(hidden)
            act[which, :, cols] = value.astype(BF)
            if with_grad:
                grads = dot(low[...], full_out[which, cols, :], 1, 1) * tilt
                keep_hidden_grad(which, c, cols, grads)
            else:
                slope[:, cols] = tilt.astype(BF)
            return 0

        lax.fori_loop(0, 2048 // CHUNK, chunk, 0)

    def keep_hidden_grad(which, c, cols, grads):
        hidden_grad[:, cols] = grads.astype(BF)
        bias_grad[which : which + 1, cols] = jnp.sum(grads, 0, keepdims=True)

    bias_grad = rest[29]

    def contract(which):
        def chunk(n, _):
            cols = part(n * CHUNK, CHUNK)
            branch[which, :, cols] = (
                dot(act[which], full_out[which, :, cols]) + channel[which, 3:4, cols]
            )
            return 0

        lax.fori_loop(0, 512 // CHUNK, chunk, 0)

    def residual(which, into):
        for r in range(16):
            rows = slice(r * 32, r * 32 + 32)
            value = tiles[which][rows, :].astype(F32) + line(which, 4) * branch[which, rows, :]
            into[rows, :] = value.astype(BF)

    def enter(which, read):
        for r in range(16):
            rows = slice(r * 32, r * 32 + 32)
            grads = read(rows) * line(which, 4)
            low[rows, :] = grads.astype(BF)
            add_rows(0, grads)

    def add_rows(slot, values):
        total = values[0:8] + values[8:16] + (values[16:24] + values[24:32])
        carry[slot] = carry[slot] + total

    def weight_grads(which):
        def chunk(c, _):
            cols = part(c * CHUNK, CHUNK)
            grad_out[which, cols, :] = dot(act[which, :, cols], low[...], 0, 0).astype(BF)
            grad_in[which, :, cols] = dot(turned[...], hidden_grad[:, cols]).astype(BF)
            return 0

        turned[...] = normal[which].T
        lax.fori_loop(0, 2048 // CHUNK, chunk, 0)

    def normal_grads(which, target):
        def chunk(n, _):
            rows = part(n * CHUNK, CHUNK)
            target[:, rows] = dot(hidden_grad[...], full_in[which, rows, :], 1, 1)
            return 0

        lax.fori_loop(0, 512 // CHUNK, chunk, 0)

    def leave(which, grads_ref):
        for r in range(16):
            rows = slice(r * 32, r * 32 + 32)
            grads = grads_ref[rows, :]
            values = normed[which, rows, :]
            add_rows(2, grads)
            add_rows(1, grads * values)
            scaled = grads * line(which, 1)
            mean = jnp.mean(scaled, -1, keepdims=True)
            tilt = jnp.mean(scaled * values, -1, keepdims=True)
            mixed = (scaled - mean - values * tilt) * rstd[which, rows, 0:1]
            add_rows(3, mixed)
            put_row(padded_g, r + 3, 3, mixed)
            gm_tile[which, rows, :] = mixed.astype(BF)

    def scale_grad(which, read):
        for r in range(16):
            rows = slice(r * 32, r * 32 + 32)
            add_rows(4, read(rows) * branch[which, rows, :])

    def settle(which):
        for slot, row in ((3, 0), (1, 1), (2, 2), (0, 3), (4, 4)):
            at = which * 64 + 49 + row
            small[at : at + 1, :] = jnp.sum(carry[slot], 0, keepdims=True)
        for c in range(4):
            at = which * 64 + 54 + c
            small[at : at + 1, :] = bias_grad[which : which + 1, c * 512 : c * 512 + 512]

    def from_cotangent(rows):
        return cotangent[rows, :].astype(F32)

    def from_upstream(rows):
        return upstream[rows, :]

    gather.forward(0, 0)
    normalise(0)
    gather.finish(0, 0)
    expand(0, False)
    gather.forward(0, 1)
    gather.finish(0, 1)
    contract(0)
    residual(0, middle)
    fill(padded1, middle)
    halos[1].start()
    gather.start(1, 1)
    gather.forward(1, 0)
    carry[...] = jnp.zeros_like(carry)
    enter(1, from_cotangent)
    halos[1].finish()
    normalise(1)
    gather.finish(1, 0)
    gather.forward(1, 1)
    gather.finish(1, 1)
    expand(1, True)
    normal_grads(1, upstream)
    leave(1, upstream)
    halos[2].start()
    weight_grads(1)
    for way in reducing(1):
        way.core_start()
    contract(1)
    residual(1, output)
    scale_grad(1, from_cotangent)
    settle(1)
    for way in reducing(1):
        way.core_finish()
        way.split_start(0)
    tap_grads(padded1, padded_g, small, 64)
    halos[2].finish()
    depthwise(padded_g, taps.at[1], result, True)
    for r in range(16):
        rows = slice(r * 32, r * 32 + 32)
        upstream[rows, :] = from_cotangent(rows) + pixels(result, r)
    for way in reducing(1):
        way.split_finish(0)
        way.split_start(1)
    carry[...] = jnp.zeros_like(carry)
    enter(0, from_upstream)
    scale_grad(0, from_upstream)

    def chunk(c, _):
        cols = part(c * CHUNK, CHUNK)
        grads = dot(low[...], full_out[0, cols, :], 1, 1) * slope[:, cols].astype(F32)
        keep_hidden_grad(0, c, cols, grads)
        return 0

    lax.fori_loop(0, 2048 // CHUNK, chunk, 0)
    for way in reducing(1):
        way.split_finish(1)
        way.across_start()
    weight_grads(0)
    for way in reducing(0):
        way.core_start()
    normal_grads(0, branch.at[1])
    for way in reducing(1):
        way.across_finish()
        way.join_start(1)
    for way in reducing(0):
        way.core_finish()
        way.split_start(0)
    leave(0, branch.at[1])
    halos[3].start()
    settle(0)
    for way in reducing(1):
        way.join_finish(1)
        way.join_start(0)
    tap_grads(padded0, padded_g, small, 0)
    ways[Small, None].core_start()
    halos[3].finish()
    depthwise(padded_g, taps.at[0], result, True)
    for r in range(16):
        rows = slice(r * 32, r * 32 + 32)
        grad_slides[rows, :] = (upstream[rows, :] + pixels(result, r)).astype(BF)
    for way in reducing(1):
        way.join_finish(0)
        way.share_start()
    last = [ways[Small, None]] + reducing(0)
    last[0].core_finish()
    last[0].split_start(0)
    for way in last:
        way.split_finish(0)
        way.split_start(1)
    for way in last:
        way.split_finish(1)
        way.across_start()
    for way in last:
        way.across_finish()
        way.join_start(1)
    for way in last:
        way.join_finish(1)
        way.join_start(0)
    for way in last:
        way.join_finish(0)
        way.share_start()
    for way in reducing(1) + last:
        way.share_finish()
    for way in reducing(1) + last + halos + [gather]:
        way.drain()


def halo_scratch():
    return [
        pltpu.VMEM((2, 96, 512), BF),
        pltpu.VMEM((2, 192, 128), BF),
        pltpu.VMEM((2, 192, 128), BF),
        pltpu.VMEM((2, 2, 80, 128), BF),
        pltpu.VMEM((2, 2, 80, 128), BF),
        pltpu.SemaphoreType.DMA((2, 8)),
    ]


def whole_step(slides, cotangent, kernel, channel, bias_in, weight_in, weight_out):
    vmem = pl.BlockSpec(memory_space=pltpu.VMEM)
    grid = pltpu.VMEM((BACK * SPAN * 8, 128), F32)
    scratch = [
        pltpu.VMEM((2, 512, 2048), BF),
        pltpu.VMEM((2, 2048, 512), BF),
        grid,
        grid,
        grid,
        pltpu.VMEM((8 * 32 * 8, 128), F32),
        pltpu.VMEM((2, 49 * 8, 128), F32),
        pltpu.VMEM((2, 512, 512), F32),
        pltpu.VMEM((2, 512, 128), F32),
        pltpu.VMEM((2, 512, 512), BF),
        pltpu.VMEM((512, 512), BF),
        pltpu.VMEM((2, 512, 2048), BF),
        pltpu.VMEM((512, 2048), BF),
        pltpu.VMEM((512, 2048), BF),
        pltpu.VMEM((2, 512, 512), F32),
        pltpu.VMEM((5, 8, 512), F32),
        pltpu.VMEM((512, 512), F32),
        pltpu.VMEM((512, 512), BF),
        pltpu.VMEM((2, 512, 512), BF),
        pltpu.VMEM((512, 512), BF),
        pltpu.VMEM((2, 512, 2048), BF),
        pltpu.VMEM((2, 2048, 512), BF),
        pltpu.VMEM((128, 512), F32),
    ]
    scratch += [pltpu.SemaphoreType.DMA((2, 2))]
    scratch += [pltpu.SemaphoreType.DMA((2, 2, 2)) for _ in range(4)]
    for _ in range(4):
        scratch += halo_scratch()
    extra = [pltpu.VMEM((2, 2048), F32)]
    reductions = sum([reduction_scratch(kind) for kind, _ in UNITS], [])
    return pl.pallas_call(
        step_kernel,
        out_shape=(
            jax.ShapeDtypeStruct((512, 512), BF),
            jax.ShapeDtypeStruct((512, 512), BF),
            jax.ShapeDtypeStruct((2, 256, 2048), BF),
            jax.ShapeDtypeStruct((2, 2048, 256), BF),
            jax.ShapeDtypeStruct((128, 512), F32),
        ),
        in_specs=[vmem] * 5 + [pl.BlockSpec(memory_space=pl.ANY)] * 2,
        out_specs=[vmem] * 5,
        scratch_shapes=scratch + extra + reductions,
        compiler_params=pltpu.CompilerParams(
            collective_id=0, has_side_effects=True, vmem_limit_bytes=67043328
        ),
        name="whole_step",
    )(slides, cotangent, kernel, channel, bias_in, weight_in, weight_out)


def per_device(
    slides,
    cotangent,
    kernel,
    kernel_bias,
    norm_gain,
    norm_bias,
    weight_in,
    bias_in,
    weight_out,
    bias_out,
    layer_scale,
):
    channels = slides.shape[-1]
    channel = jnp.stack([kernel_bias, norm_gain, norm_bias, bias_out, layer_scale], axis=1)
    output, grad_slides, total_in, total_out, small = whole_step(
        slides.reshape(-1, channels),
        cotangent.reshape(-1, channels),
        kernel.reshape(2, 49, channels),
        channel,
        bias_in,
        weight_in,
        weight_out,
    )
    small = small.reshape(2, 64, channels)
    return (
        output.reshape(slides.shape),
        grad_slides.reshape(slides.shape),
        total_in.astype(F32),
        total_out.astype(F32),
        small[:, :49].reshape(2, 7, 7, channels),
        small[:, 49:54],
        small[:, 54:58].reshape(2, 4 * channels),
    )


def solution(mesh):
    whole = P("dp", "row", "col", None)
    return jax.shard_map(
        per_device,
        mesh=mesh,
        in_specs=(whole, whole) + (P(),) * 4 + (P(None, "dp", None), P(), P(None, None, "dp"), P(), P()),
        out_specs=(whole, whole, P(None, "dp", None), P(None, None, "dp"), P(), P(), P()),
        check_vma=False,
    )
```

```python
import functools

import jax
import jax.numpy as jnp
from jax import lax
from jax.experimental import pallas as pl
from jax.experimental.pallas import tpu as pltpu
from jax.sharding import PartitionSpec as P

COEF = 0.7978845608028654
CUBIC = 0.044715
EPSILON = 1e-06

MESH = pl.DeviceIdType.MESH
BF = jnp.bfloat16
F32 = jnp.float32


class Place:
    def __init__(self):
        row = lax.axis_index("row")
        self.z = lax.axis_index("col")
        self.half = lax.axis_index("dp")
        self.core = lax.rem(row, 2)
        self.y = lax.rem(lax.div(row, 2), 4)
        self.x = lax.div(row, 8) * 2 + self.half

    def device(self, x=None, y=None, z=None, core=None):
        x = self.x if x is None else x
        y = self.y if y is None else y
        z = self.z if z is None else z
        core = self.core if core is None else core
        return {"row": (lax.div(x, 2) * 4 + y) * 2 + core, "col": z, "dp": lax.rem(x, 2)}

    def along(self, axis, offset):
        value = lax.rem(getattr(self, axis) + offset, 4)
        return value, self.device(**{axis: value})

    def sibling(self):
        return self.device(core=1 - self.core)


def meet(partners):
    barrier = pltpu.get_barrier_semaphore()
    for partner in partners:
        pl.semaphore_signal(barrier, inc=1, device_id=partner, device_id_type=MESH)
    pl.semaphore_wait(barrier, len(partners))


def part(start, size):
    if isinstance(start, int):
        return pl.ds(start, size)
    return pl.ds(pl.multiple_of(start, size), size)


def remote(src, dst, send, recv, target):
    return pltpu.make_async_remote_copy(
        src_ref=src, dst_ref=dst, send_sem=send, recv_sem=recv, device_id=target, device_id_type=MESH
    )


ORDERS = (("y", "z"), ("z", "y"))


class WeightIn:
    received = (128, 2048)
    turn = (64, 2048)
    first = (64, 512)
    second = (64, 128)
    third = (64, 128)

    def offered(grad, half, core):
        return grad.at[part(half * 256 + core * 128, 128), :]

    def cut(got, halves, turn, index):
        return got.at[halves, turn * 64 : turn * 64 + 64, part(index * 512, 512)]

    def cut_again(block, index):
        return block.at[:, :, part(index * 128, 128)]

    def placed(final, core, turn, one, two):
        return final.at[part(core * 128 + turn * 64, 64), part(one * 512 + two * 128, 128)]

    def line(final, core, turn, one):
        return final.at[part(core * 128 + turn * 64, 64), part(one * 512, 512)]

    def of_core(final, core):
        return final.at[part(core * 128, 128), :]


class WeightOut:
    received = (2048, 128)
    turn = (1024, 128)
    first = (256, 128)
    second = (64, 128)
    third = (64, 128)

    def offered(grad, half, core):
        return grad.at[:, part(half * 256 + core * 128, 128)]

    def cut(got, halves, turn, index):
        return got.at[halves, part(turn * 1024 + index * 256, 256), :]

    def cut_again(block, index):
        return block.at[:, part(index * 64, 64), :]

    def placed(final, core, turn, one, two):
        return final.at[part(turn * 1024 + one * 256 + two * 64, 64), part(core * 128, 128)]

    def line(final, core, turn, one):
        return final.at[part(turn * 1024 + one * 256, 256), part(core * 128, 128)]

    def of_core(final, core):
        return final.at[:, part(core * 128, 128)]


class Small:
    received = (64, 512)
    turn = (32, 512)
    first = (32, 128)
    second = (8, 128)
    third = (8, 128)

    def offered(grad, half, core):
        return grad.at[part(core * 64, 64), :]

    def cut(got, halves, turn, index):
        return got.at[halves, turn * 32 : turn * 32 + 32, part(index * 128, 128)]

    def cut_again(block, index):
        return block.at[:, part(index * 8, 8), :]

    def placed(final, core, turn, one, two):
        return final.at[part(core * 64 + turn * 32 + two * 8, 8), part(one * 128, 128)]

    def line(final, core, turn, one):
        return final.at[part(core * 64 + turn * 32, 32), part(one * 128, 128)]

    def of_core(final, core):
        return final.at[part(core * 64, 64), :]


class Reduction:
    def __init__(self, me, kind, early, grad, final, bufs, sems):
        self.me, self.kind, self.early, self.grad, self.final = me, kind, early, grad, final
        self.got, self.given, self.r1, self.b1, self.r2, self.b2, self.r3 = bufs
        self.sems = sems
        self.halves = 1 if kind is Small else 2
        self.copies = []
        self.steps = [
            [self.core_start],
            [self.core_finish, lambda: self.split_start(0)],
            [lambda: self.split_finish(0), lambda: self.split_start(1)],
            [lambda: self.split_finish(1), self.across_start],
            [self.across_finish, lambda: self.join_start(1)],
            [lambda: self.join_finish(1), lambda: self.join_start(0)],
            [lambda: self.join_finish(0), self.share_start],
            [self.share_finish],
        ]
        if early:
            self.steps[1:2] = [
                [self.core_finish, self.give_start],
                [self.give_finish, lambda: self.split_start(0)],
            ]

    def advance(self):
        for action in self.steps.pop(0):
            action()

    def sem(self, way, turn, step, slot):
        return self.sems.at[way, (turn * 8 + step) * 4 + slot]

    def go(self, src, dst, turn, step, send_slot, recv_slot, target):
        copy = remote(
            src, dst, self.sem(0, turn, step, send_slot), self.sem(1, turn, step, recv_slot), target
        )
        copy.start()
        self.copies.append(copy)

    def landed(self, dst, turn, step, slot):
        remote(
            dst, dst, self.sem(0, turn, step, slot), self.sem(1, turn, step, slot), self.me.sibling()
        ).wait_recv()

    def core_start(self):
        for half in range(self.halves):
            src = self.kind.offered(self.grad, half, 1 - self.me.core)
            self.go(src, self.got.at[half], 0, 0, half, half, self.me.sibling())

    def core_finish(self):
        for half in range(self.halves):
            self.landed(self.got.at[half], 0, 0, half)
            own = self.kind.offered(self.grad, half, self.me.core)
            total = own[...].astype(F32) + self.got[half].astype(F32)
            self.got[half] = total.astype(self.got.dtype)

    def block(self, turn, step, index):
        if step == 0:
            halves = pl.ds(self.me.half, 1) if self.early else slice(None)
            return self.kind.cut(self.got, halves, turn, index)
        return self.kind.cut_again(self.b1.at[turn], index)

    def split_start(self, step):
        target = (self.r1, self.r2)[step]
        for turn in range(2):
            for offset in (1, 3, 2):
                index, device = self.me.along(ORDERS[turn][step], offset)
                self.go(
                    self.block(turn, step, index),
                    target.at[turn, offset - 1],
                    turn,
                    1 + step,
                    offset,
                    offset,
                    device,
                )

    def split_finish(self, step):
        target, result = ((self.r1, self.b1), (self.r2, self.b2))[step]
        for turn in range(2):
            index = getattr(self.me, ORDERS[turn][step])
            total = self.block(turn, step, index)[...].astype(F32)
            for offset in (1, 3, 2):
                self.landed(target.at[turn, offset - 1], turn, 1 + step, offset)
                total = total + target[turn, offset - 1].astype(F32)
            result[turn] = total.astype(result.dtype)

    def turn_rows(self, half, turn):
        size = self.kind.turn[0]
        return self.got.at[half, turn * size : turn * size + size, :]

    def give_start(self):
        for turn, offset in ((0, 1), (1, 3)):
            _, device = self.me.along("x", offset)
            src = self.turn_rows(1 - self.me.half, turn)
            self.go(src, self.given.at[turn], turn, 7, 0, 0, device)

    def give_finish(self):
        for turn in range(2):
            self.landed(self.given.at[turn], turn, 7, 0)
            own = self.turn_rows(self.me.half, turn)
            total = own[...].astype(F32) + self.given[turn].astype(F32)
            own[...] = total.astype(self.got.dtype)

    def across_start(self):
        for turn in range(2):
            block = self.b2.at[turn]
            if self.early:
                _, device = self.me.along("x", 2)
                self.go(block.at[0], self.r3.at[turn, 0], turn, 3, 0, 0, device)
                continue
            for offset in (1, 3, 2):
                index, device = self.me.along("x", offset)
                src = block.at[lax.rem(index, 2) if self.halves == 2 else 0]
                self.go(src, self.r3.at[turn, self.me.x], turn, 3, offset, self.me.x, device)
            self.r3[turn, self.me.x] = block[self.me.half if self.halves == 2 else 0]

    def across_finish(self):
        me = self.me
        for turn in range(2):
            if self.early:
                self.landed(self.r3.at[turn, 0], turn, 3, 0)
                total = self.b2[turn, 0].astype(F32) + self.r3[turn, 0].astype(F32)
            else:
                for offset in (1, 3, 2):
                    index, _ = me.along("x", offset)
                    self.landed(self.r3.at[turn, index], turn, 3, index)
                total = self.r3[turn, 0].astype(F32)
                for index in range(1, 4):
                    total = total + self.r3[turn, index].astype(F32)
            one, two = (getattr(me, axis) for axis in ORDERS[turn])
            block = self.kind.placed(self.final, me.core, turn, one, two)
            block[...] = total.astype(self.final.dtype)

    def join_start(self, step):
        me = self.me
        for turn in range(2):
            one, two = (getattr(me, axis) for axis in ORDERS[turn])
            for offset in (1, 3, 2):
                _, device = me.along(ORDERS[turn][step], offset)
                if step == 1:
                    block = self.kind.placed(self.final, me.core, turn, one, two)
                else:
                    block = self.kind.line(self.final, me.core, turn, one)
                self.go(block, block, turn, 5 - step, offset, offset, device)

    def join_finish(self, step):
        me = self.me
        for turn in range(2):
            one, two = (getattr(me, axis) for axis in ORDERS[turn])
            for offset in (1, 3, 2):
                source = lax.rem((two if step == 1 else one) + 4 - offset, 4)
                if step == 1:
                    block = self.kind.placed(self.final, me.core, turn, one, source)
                else:
                    block = self.kind.line(self.final, me.core, turn, source)
                self.landed(block, turn, 5 - step, offset)

    def share_start(self):
        block = self.kind.of_core(self.final, self.me.core)
        self.go(block, block, 0, 6, 0, 0, self.me.sibling())

    def share_finish(self):
        block = self.kind.of_core(self.final, 1 - self.me.core)
        self.landed(block, 0, 6, 0)

    def drain(self):
        for copy in self.copies:
            copy.wait_send()


def reduction_scratch(kind, early):
    dtype = F32 if kind is Small else BF
    halves = 1 if kind is Small or early else 2
    return [
        pltpu.VMEM((1 if kind is Small else 2, *kind.received), dtype),
        pltpu.VMEM((2, *kind.turn) if early else (2, 8, 128), dtype),
        pltpu.VMEM((2, 3, halves, *kind.first), dtype),
        pltpu.VMEM((2, halves, *kind.first), dtype),
        pltpu.VMEM((2, 3, halves, *kind.second), dtype),
        pltpu.VMEM((2, halves, *kind.second), dtype),
        pltpu.VMEM((2, 4, *kind.third), dtype),
        pltpu.SemaphoreType.DMA((2, 64)),
    ]


UNITS = (
    (Small, None, False),
    (WeightOut, 1, True),
    (WeightIn, 1, True),
    (WeightOut, 0, False),
    (WeightIn, 0, True),
)


class Gather:
    def __init__(self, me, shard_in, shard_out, full_in, full_out, sems):
        self.me = me
        self.shards = (shard_in, shard_out)
        self.full = (full_in, full_out)
        self.local, self.send, self.recv, self.send_core, self.recv_core = sems
        self.sides = (me.along("x", 1)[1], me.along("x", 3)[1])
        self.copies = []

    def block(self, which, kind, half, core, side):
        full = self.full[kind].at[which]
        if kind == 0:
            return full.at[part(half * 256 + core * 128 + side * 64, 64), :]
        return full.at[part(core * 1024 + side * 512, 512), part(half * 256, 256)]

    def place(self, which, kind):
        half = part(self.me.half * 256, 256)
        full = self.full[kind].at[which]
        own = full.at[half, :] if kind == 0 else full.at[:, half]
        return pltpu.make_async_copy(self.shards[kind].at[which], own, self.local.at[which, kind])

    def hop(self, which, kind, half, core, side, across):
        block = self.block(which, kind, half, core, side)
        if across:
            sems, target = (self.send, self.recv), self.sides[side]
        else:
            sems, target = (self.send_core, self.recv_core), self.me.sibling()
        return remote(block, block, *(s.at[which, kind, side] for s in sems), target)

    def start(self, which, kind):
        self.place(which, kind).wait()
        for side in range(2):
            copy = self.hop(which, kind, self.me.half, self.me.core, side, True)
            copy.start()
            self.copies.append(copy)

    def forward(self, which, kind):
        other = 1 - self.me.half
        for side in range(2):
            self.hop(which, kind, other, self.me.core, side, True).wait_recv()
            copy = self.hop(which, kind, other, self.me.core, side, False)
            copy.start()
            self.copies.append(copy)

    def finish(self, which, kind):
        for side in range(2):
            self.hop(which, kind, 1 - self.me.half, 1 - self.me.core, side, False).wait_recv()

    def drain(self):
        for copy in self.copies:
            copy.wait_send()


SPAN = 38
BACK, FRONT = 14, 8


def word(i, j):
    start = (i * SPAN + j) * 8
    return pl.ds(start if isinstance(start, int) else pl.multiple_of(start, 8), 8)


def put_row(padded, row, first, values, halves=(0, 1)):
    for half in halves:
        i = row - 8 * half
        if 0 <= i < BACK:
            for group in range(4):
                padded[pl.ds((i * SPAN + first) * 8 + half * 4 + group, values.shape[0], stride=8), :] = (
                    values[:, group * 128 : group * 128 + 128]
                )


def rolled(values):
    return jnp.concatenate([values[4:], values[:4]], axis=0)


class Halo:
    def __init__(self, me, padded, tile, bufs):
        self.me, self.padded, self.tile = me, padded, tile
        self.rows, self.side_out, self.sides, self.corner_out, self.corners, self.sems = bufs
        self.copies = []
        self.row = (lax.div(me.x, 2) * 4 + me.y) * 2 + me.core

    def target(self, down, right):
        row = lax.rem(self.row + down + 16, 16)
        col = lax.rem(self.me.z + right + 4, 4)
        return {"row": row, "col": col, "dp": self.me.half}

    def messages(self):
        tile = self.tile
        yield tile.at[pl.ds(0, 96), :], self.rows.at[1], (-1, 0)
        yield tile.at[pl.ds(416, 96), :], self.rows.at[0], (1, 0)
        for side in range(2):
            yield self.side_out.at[side], self.sides.at[1 - side], (0, 2 * side - 1)
        for low in range(2):
            for side in range(2):
                yield (
                    self.corner_out.at[low, side],
                    self.corners.at[1 - low, 1 - side],
                    (2 * low - 1, 2 * side - 1),
                )

    def start(self):
        padded = self.padded
        for side, first in ((0, 3), (1, 32)):
            for j in range(3):
                lines = [padded[word(i, first + j), :] for i in range(3, 11)]
                self.side_out[side, j * 64 : j * 64 + 64, :] = jnp.concatenate(lines, 0).astype(BF)
            for low, top in ((0, 3), (1, 8)):
                lines = [
                    rolled(padded[word(top + i, first + j), :]) for i in range(3) for j in range(3)
                ]
                self.corner_out[low, side] = jnp.concatenate(lines + lines[:1], 0).astype(BF)
        for number, (src, dst, (down, right)) in enumerate(self.messages()):
            copy = remote(
                src, dst, self.sems.at[0, number], self.sems.at[1, number], self.target(down, right)
            )
            copy.start()
            self.copies.append(copy)

    def finish(self):
        padded = self.padded
        for number, (src, dst, _) in enumerate(self.messages()):
            remote(
                src, dst, self.sems.at[0, number], self.sems.at[1, number], self.target(1, 0)
            ).wait_recv()
        inside = [
            (self.row > 0).astype(F32),
            (self.row < 15).astype(F32),
        ]
        across = [
            (self.me.z > 0).astype(F32),
            (self.me.z < 3).astype(F32),
        ]
        for low in range(2):
            for r in range(3):
                values = self.rows[low, r * 32 : r * 32 + 32, :].astype(F32) * inside[low]
                put_row(padded, r + 19 * low, 3, values, (low,))
        for side, first in ((0, 0), (1, 35)):
            for j in range(3):
                lines = self.sides[side, j * 64 : j * 64 + 64, :].astype(F32) * across[side]
                for m in range(8):
                    line = lines[m * 8 : m * 8 + 8]
                    padded[word(m + 3, first + j), :] = line
                    at = first + j
                    if m >= 5:
                        padded[pl.ds(((m - 5) * SPAN + at) * 8 + 4, 4), :] = line[:4]
                    if m < 3:
                        padded[pl.ds(((m + 11) * SPAN + at) * 8, 4), :] = line[4:]
            for low in range(2):
                lines = self.corners[low, side].astype(F32) * (inside[low] * across[side])
                for i in range(3):
                    for j in range(3):
                        line = lines[(i * 3 + j) * 8 : (i * 3 + j) * 8 + 8]
                        start = ((i + 11 * low) * SPAN + first + j) * 8 + 4 * low
                        padded[pl.ds(start, 4), :] = line[4 * low : 4 * low + 4]

    def drain(self):
        for copy in self.copies:
            copy.wait_send()


def spread_taps(kernel, which, taps):
    for p in range(7):
        for group in range(4):
            values = kernel[p, :, which, group * 128 : group * 128 + 128]
            for half in range(2):
                taps[pl.ds(p * 56 + half * 4 + group, 7, stride=8), :] = values


def depthwise(padded, taps, result, flipped, first=0, last=32):
    def column(j, _):
        total = [None] * FRONT
        for q in range(7):
            values = [padded[word(i, j + q), :] for i in range(BACK)]
            for p in range(7):
                number = (6 - p) * 7 + 6 - q if flipped else p * 7 + q
                tap = taps[number * 8 : number * 8 + 8, :]
                for i in range(FRONT):
                    term = values[i + p] * tap
                    total[i] = term if total[i] is None else total[i] + term
        for i in range(FRONT):
            result[pl.ds(pl.multiple_of((i * 32 + j) * 8, 8), 8), :] = total[i]
        return 0

    lax.fori_loop(first, last, column, 0)


def tap_grads(padded, upstream, small, base, columns):
    for q in columns:

        def column(j, totals):
            values = [padded[word(i, j + q), :] for i in range(BACK)]
            grads = [upstream[word(i + 3, j + 3), :] for i in range(FRONT)]
            result = []
            for p in range(7):
                total = totals[p]
                for i in range(FRONT):
                    total = total + values[i + p] * grads[i]
                result.append(total)
            return tuple(result)

        zero = jnp.zeros((8, 128), F32)
        totals = lax.fori_loop(0, 32, column, (zero,) * 7)
        for p in range(7):
            both = totals[p][:4] + totals[p][4:]
            for group in range(4):
                small[base + p * 7 + q : base + p * 7 + q + 1, group * 128 : group * 128 + 128] = both[
                    group : group + 1
                ]


def pixels(result, row):
    half, i = row // 8, row % 8
    return jnp.concatenate(
        [result[pl.ds(i * 256 + half * 4 + group, 32, stride=8), :] for group in range(4)], axis=1
    )


def dot(left, right, left_dim=1, right_dim=0):
    return lax.dot_general(
        left, right, (((left_dim,), (right_dim,)), ((), ())), preferred_element_type=F32
    )


def gelu_and_slope(values):
    square = values * values
    tangent = jnp.tanh(COEF * values * (1.0 + CUBIC * square))
    lift = 0.5 * (1.0 + tangent)
    slope = lift + 0.5 * values * (1.0 - tangent * tangent) * (COEF + (3.0 * COEF * CUBIC) * square)
    return values * lift, slope


CHUNK = 256


def step_kernel(
    slides, cotangent, kernel, kernel_bias, norm_gain, norm_bias, bias_out, layer_scale, bias_in,
    shard_in, shard_out,
    output, grad_slides, final_in, final_out, final_small,
    full_in, full_out, padded0, padded1, padded_g0, padded_g1, result, taps,
    normed, rstd, normal, turned, act, slope, hidden_grad, branch, carry, upstream, low,
    gm_tile, middle, grad_in, grad_out, small,
    *rest,
):
    me = Place()
    gather = Gather(me, shard_in, shard_out, full_in, full_out, rest[:5])
    padded = (padded0, padded1)
    padded_g = (padded_g0, padded_g1)
    tiles = (slides, middle)
    halos = [
        Halo(me, grid, tile, rest[5 + 6 * k : 11 + 6 * k])
        for k, (grid, tile) in enumerate(
            ((padded0, slides), (padded1, middle), (padded_g1, gm_tile.at[1]), (padded_g0, gm_tile.at[0]))
        )
    ]
    scratch = rest[30:]
    ways = {}
    for number, (kind, which, early) in enumerate(UNITS):
        bufs = scratch[number * 8 : number * 8 + 7]
        sems = scratch[number * 8 + 7]
        if kind is Small:
            ends = (small, final_small)
        elif kind is WeightIn:
            ends = (grad_in.at[which], final_in.at[which])
        else:
            ends = (grad_out.at[which], final_out.at[which])
        ways[kind, which] = Reduction(me, kind, early, *ends, bufs, sems)

    def reducing(which):
        return [ways[WeightOut, which], ways[WeightIn, which]]

    def line(which, ref):
        return ref[which : which + 1, :]

    for which in range(2):
        for kind in range(2):
            gather.place(which, kind).start()

    scope = jax.named_scope

    def fill(grid, tile):
        for r in range(16):
            put_row(grid, r + 3, 3, tile[r * 32 : r * 32 + 32, :].astype(F32))

    partners = [me.along(axis, offset)[1] for axis in "xyz" for offset in (1, 2, 3)]
    around = [
        halos[0].target(down, right) for down in (-1, 0, 1) for right in (-1, 0, 1) if down
    ]
    with scope("p00a_fill"):
        fill(padded0, slides)
        for which in range(2):
            spread_taps(kernel, which, taps.at[which])
        small[...] = jnp.zeros_like(small)
        carry[...] = jnp.zeros_like(carry)
    with scope("p00b_meet"):
        meet(partners + around + [me.sibling()])
    with scope("p00c_start"):
        halos[0].start()
        gather.start(0, 0)
        gather.start(0, 1)
        gather.start(1, 0)

    def filter_map(which, first, last):
        depthwise(padded[which], taps.at[which], result, False, first, last)

    def normalise(which):
        for r in range(16):
            rows = slice(r * 32, r * 32 + 32)
            mixed = pixels(result, r) + line(which, kernel_bias)
            center = mixed - jnp.mean(mixed, -1, keepdims=True)
            inverse = lax.rsqrt(jnp.mean(center * center, -1, keepdims=True) + EPSILON)
            values = center * inverse
            normed[which, rows, :] = values
            rstd[which, rows, :] = jnp.broadcast_to(inverse, (32, 128))
            normal[which, rows, :] = (values * line(which, norm_gain) + line(which, norm_bias)).astype(BF)

    def expand(which, with_grad, first=0, last=2048 // CHUNK):
        def chunk(c, _):
            cols = part(c * CHUNK, CHUNK)
            hidden = dot(normal[which], full_in[which, :, cols]) + bias_in[which : which + 1, cols]
            value, tilt = gelu_and_slope(hidden)
            act[which, :, cols] = value.astype(BF)
            if with_grad:
                grads = dot(low[...], full_out[which, cols, :], 1, 1) * tilt
                keep_hidden_grad(which, c, cols, grads)
            else:
                slope[:, cols] = tilt.astype(BF)
            return 0

        lax.fori_loop(first, last, chunk, 0)

    def keep_hidden_grad(which, c, cols, grads):
        hidden_grad[:, cols] = grads.astype(BF)
        bias_grad[which : which + 1, cols] = jnp.sum(grads, 0, keepdims=True)

    bias_grad = rest[29]

    def contract(which):
        def chunk(n, _):
            cols = part(n * CHUNK, CHUNK)
            branch[which, :, cols] = (
                dot(act[which], full_out[which, :, cols]) + bias_out[which : which + 1, cols]
            )
            return 0

        lax.fori_loop(0, 512 // CHUNK, chunk, 0)

    def residual(which, into):
        for r in range(16):
            rows = slice(r * 32, r * 32 + 32)
            value = tiles[which][rows, :].astype(F32) + line(which, layer_scale) * branch[which, rows, :]
            into[rows, :] = value.astype(BF)

    def enter(which, read):
        for r in range(16):
            rows = slice(r * 32, r * 32 + 32)
            grads = read(rows) * line(which, layer_scale)
            low[rows, :] = grads.astype(BF)
            add_rows(which, 0, grads)

    def add_rows(which, slot, values):
        total = values[0:8] + values[8:16] + (values[16:24] + values[24:32])
        carry[which, slot] = carry[which, slot] + total

    def weight_grads(which):
        def chunk(c, _):
            cols = part(c * CHUNK, CHUNK)
            grad_out[which, cols, :] = dot(act[which, :, cols], low[...], 0, 0).astype(BF)
            grad_in[which, :, cols] = dot(turned[...], hidden_grad[:, cols]).astype(BF)
            return 0

        turned[...] = normal[which].T
        lax.fori_loop(0, 2048 // CHUNK, chunk, 0)

    def normal_grads(which, target):
        def chunk(n, _):
            rows = part(n * CHUNK, CHUNK)
            target[:, rows] = dot(hidden_grad[...], full_in[which, rows, :], 1, 1)
            return 0

        lax.fori_loop(0, 512 // CHUNK, chunk, 0)

    def leave(which, grads_ref):
        for r in range(16):
            rows = slice(r * 32, r * 32 + 32)
            grads = grads_ref[rows, :]
            values = normed[which, rows, :]
            add_rows(which, 2, grads)
            add_rows(which, 1, grads * values)
            scaled = grads * line(which, norm_gain)
            mean = jnp.mean(scaled, -1, keepdims=True)
            tilt = jnp.mean(scaled * values, -1, keepdims=True)
            mixed = (scaled - mean - values * tilt) * rstd[which, rows, 0:1]
            add_rows(which, 3, mixed)
            put_row(padded_g[which], r + 3, 3, mixed)
            gm_tile[which, rows, :] = mixed.astype(BF)

    def scale_grad(which, read):
        for r in range(16):
            rows = slice(r * 32, r * 32 + 32)
            add_rows(which, 4, read(rows) * branch[which, rows, :])

    def settle(which):
        for slot, row in ((3, 0), (1, 1), (2, 2), (0, 3), (4, 4)):
            at = which * 64 + 49 + row
            small[at : at + 1, :] = jnp.sum(carry[which, slot], 0, keepdims=True)
        for c in range(4):
            at = which * 64 + 54 + c
            small[at : at + 1, :] = bias_grad[which : which + 1, c * 512 : c * 512 + 512]

    def from_cotangent(rows):
        return cotangent[rows, :].astype(F32)

    def from_upstream(rows):
        return upstream[rows, :]

    with scope("p00e_halo0"):
        enter(1, from_cotangent)
        halos[0].finish()
    with scope("p01_depth0"):
        filter_map(0, 0, 20)
    with scope("p02_forward_in0"):
        gather.forward(0, 0)
    with scope("p03_norm0"):
        filter_map(0, 20, 32)
        normalise(0)
    with scope("p04_finish_in0"):
        gather.finish(0, 0)
    with scope("p05_expand0"):
        expand(0, False, 0, 5)
    with scope("p05_forward_out0"):
        gather.forward(0, 1)
    with scope("p05_expand0b"):
        expand(0, False, 5)
    with scope("p06_finish_out0"):
        gather.finish(0, 1)
    with scope("p06_contract0"):
        contract(0)
        residual(0, middle)
        fill(padded1, middle)
    with scope("p07_halo1"):
        halos[1].start()
        gather.start(1, 1)
        gather.forward(1, 0)
    with scope("p08_halo1_end"):
        halos[1].finish()
    with scope("p09_depth1"):
        filter_map(1, 0, 32)
        normalise(1)
    with scope("p10_weights1"):
        gather.finish(1, 0)
        gather.forward(1, 1)
        gather.finish(1, 1)
    with scope("p11_expand1"):
        expand(1, True)
    with scope("p12_ngrads1"):
        normal_grads(1, upstream)
    with scope("p13_leave1"):
        leave(1, upstream)
        halos[2].start()
    out1, in1 = reducing(1)
    out0, in0 = reducing(0)
    little = ways[Small, None]

    def go(name, *group):
        with scope(name):
            for way in group:
                way.advance()

    with scope("p14_wgrads1"):
        weight_grads(1)
    go("p14_go1", out1, in1)
    with scope("p16_halo2_end"):
        halos[2].finish()
    with scope("p17_depth1"):
        depthwise(padded_g1, taps.at[1], result, True, 0, 10)
    go("p17_go1", out1, in1)
    with scope("p17_depth1b"):
        depthwise(padded_g1, taps.at[1], result, True, 10, 32)
        for r in range(16):
            rows = slice(r * 32, r * 32 + 32)
            upstream[rows, :] = from_cotangent(rows) + pixels(result, r)
    with scope("p18_enter0"):
        enter(0, from_upstream)
        scale_grad(0, from_upstream)

    def chunk(c, _):
        cols = part(c * CHUNK, CHUNK)
        grads = dot(low[...], full_out[0, cols, :], 1, 1) * slope[:, cols].astype(F32)
        keep_hidden_grad(0, c, cols, grads)
        return 0

    with scope("p19_hidden0"):
        lax.fori_loop(0, 2048 // CHUNK, chunk, 0)
    go("p20_go1", out1)
    with scope("p21_wgrads0"):
        weight_grads(0)
    go("p21_go0", out0, in0)
    go("p22_go1", in1, out1)
    with scope("p23_ngrads0"):
        normal_grads(0, normed.at[1])
    with scope("p24_leave0"):
        leave(0, normed.at[1])
        halos[3].start()
    go("p25_go0", out0, in0)
    with scope("p26_contract1"):
        contract(1)
        residual(1, output)
        scale_grad(1, from_cotangent)
        settle(1)
        settle(0)
    go("p27_go1", in1, out1)
    with scope("p28_taps0"):
        tap_grads(padded0, padded_g0, small, 0, range(7))
    go("p29_go0", out0)
    with scope("p29_taps1"):
        tap_grads(padded1, padded_g1, small, 64, range(3))
    go("p29_go0b", in0, in1, out1)
    with scope("p29_taps1b"):
        tap_grads(padded1, padded_g1, small, 64, range(3, 7))
    little.advance()
    go("p30_go0", out0)
    with scope("p30_halo3_end"):
        halos[3].finish()
    with scope("p31_depth0"):
        depthwise(padded_g0, taps.at[0], result, True, 0, 12)
    go("p31_go", little, in0, out0)
    with scope("p33_depth0"):
        depthwise(padded_g0, taps.at[0], result, True, 12, 24)
    go("p33_go", little, in0)
    with scope("p33_depth0b"):
        depthwise(padded_g0, taps.at[0], result, True, 24, 32)
        for r in range(16):
            rows = slice(r * 32, r * 32 + 32)
            grad_slides[rows, :] = (upstream[rows, :] + pixels(result, r)).astype(BF)
    go("p34_go", little, in0, out0, in1, out1)
    go("p35_go", little, in0, out0, in1, out1)
    go("p36_go", little, in0, out0, in1, out1)
    go("p37_go", little, in0)
    every = [out1, in1, little, out0, in0]
    with scope("p38_rest"):
        while any(way.steps for way in every):
            for way in every:
                if way.steps:
                    way.advance()
    with scope("p39_drain"):
        for way in every + halos + [gather]:
            way.drain()


def halo_scratch():
    return [
        pltpu.VMEM((2, 96, 512), BF),
        pltpu.VMEM((2, 192, 128), BF),
        pltpu.VMEM((2, 192, 128), BF),
        pltpu.VMEM((2, 2, 80, 128), BF),
        pltpu.VMEM((2, 2, 80, 128), BF),
        pltpu.SemaphoreType.DMA((2, 8)),
    ]


def whole_step(*operands):
    vmem = pl.BlockSpec(memory_space=pltpu.VMEM)
    grid = pltpu.VMEM((BACK * SPAN * 8, 128), F32)
    scratch = [
        pltpu.VMEM((2, 512, 2048), BF),
        pltpu.VMEM((2, 2048, 512), BF),
        grid,
        grid,
        grid,
        grid,
        pltpu.VMEM((8 * 32 * 8, 128), F32),
        pltpu.VMEM((2, 49 * 8, 128), F32),
        pltpu.VMEM((2, 512, 512), F32),
        pltpu.VMEM((2, 512, 128), F32),
        pltpu.VMEM((2, 512, 512), BF),
        pltpu.VMEM((512, 512), BF),
        pltpu.VMEM((2, 512, 2048), BF),
        pltpu.VMEM((512, 2048), BF),
        pltpu.VMEM((512, 2048), BF),
        pltpu.VMEM((2, 512, 512), F32),
        pltpu.VMEM((2, 5, 8, 512), F32),
        pltpu.VMEM((512, 512), F32),
        pltpu.VMEM((512, 512), BF),
        pltpu.VMEM((2, 512, 512), BF),
        pltpu.VMEM((512, 512), BF),
        pltpu.VMEM((2, 512, 2048), BF),
        pltpu.VMEM((2, 2048, 512), BF),
        pltpu.VMEM((128, 512), F32),
    ]
    scratch += [pltpu.SemaphoreType.DMA((2, 2))]
    scratch += [pltpu.SemaphoreType.DMA((2, 2, 2)) for _ in range(4)]
    for _ in range(4):
        scratch += halo_scratch()
    extra = [pltpu.VMEM((2, 2048), F32)]
    reductions = sum([reduction_scratch(kind, early) for kind, _, early in UNITS], [])
    return pl.pallas_call(
        step_kernel,
        out_shape=(
            jax.ShapeDtypeStruct((512, 512), BF),
            jax.ShapeDtypeStruct((512, 512), BF),
            jax.ShapeDtypeStruct((2, 256, 2048), BF),
            jax.ShapeDtypeStruct((2, 2048, 256), BF),
            jax.ShapeDtypeStruct((128, 512), F32),
        ),
        in_specs=[vmem] * 9 + [pl.BlockSpec(memory_space=pl.ANY)] * 2,
        out_specs=[vmem] * 5,
        scratch_shapes=scratch + extra + reductions,
        compiler_params=pltpu.CompilerParams(
            collective_id=0, has_side_effects=True, vmem_limit_bytes=67043328
        ),
        name="whole_step",
    )(*operands)


def unpack_kernel(
    output, grad_slides, total_in, total_out, small,
    output_end, slides_end, in_end, out_end, kernel_end, channel_end, bias_end,
    maps, low_in, low_out, wide_in, wide_out, get, put,
):
    steps = []
    for which in range(2):
        for cut in range(4):
            for ends, size in (
                ((total_in, low_in, wide_in, in_end), 64),
                ((total_out, low_out, wide_out, out_end), 512),
            ):
                steps.append([ref.at[which, pl.ds(cut * size, size), :] for ref in ends])
    steps.append([output, maps.at[0], maps.at[0], output_end])
    steps.append([grad_slides, maps.at[1], maps.at[1], slides_end])
    for number, (src, low, _, _) in enumerate(steps):
        pltpu.make_async_copy(src, low, get.at[number]).start()
    for number, (src, low, wide, dst) in enumerate(steps):
        pltpu.make_async_copy(src, low, get.at[number]).wait()
        if number < 16:
            wide[...] = low[...].astype(F32)
        pltpu.make_async_copy(wide, dst, put.at[number]).start()
    for which in range(2):
        base = which * 64
        for p in range(7):
            kernel_end[p, :, which, :] = small[base + p * 7 : base + p * 7 + 7, :]
        channel_end[:, which, :] = small[base + 49 : base + 54, :]
        for c in range(4):
            bias_end[which : which + 1, c * 512 : c * 512 + 512] = small[
                base + 54 + c : base + 55 + c, :
            ]
    for number, (_, _, wide, dst) in enumerate(steps):
        pltpu.make_async_copy(wide, dst, put.at[number]).wait()


def unpack(*results):
    vmem = pl.BlockSpec(memory_space=pltpu.VMEM)
    hbm = pl.BlockSpec(memory_space=pl.ANY)
    return pl.pallas_call(
        unpack_kernel,
        out_shape=(
            jax.ShapeDtypeStruct((512, 512), BF),
            jax.ShapeDtypeStruct((512, 512), BF),
            jax.ShapeDtypeStruct((2, 256, 2048), F32),
            jax.ShapeDtypeStruct((2, 2048, 256), F32),
            jax.ShapeDtypeStruct((7, 7, 2, 512), F32),
            jax.ShapeDtypeStruct((5, 2, 512), F32),
            jax.ShapeDtypeStruct((2, 2048), F32),
        ),
        in_specs=[hbm] * 4 + [vmem],
        out_specs=[hbm] * 4 + [vmem] * 3,
        scratch_shapes=[
            pltpu.VMEM((2, 512, 512), BF),
            pltpu.VMEM((2, 256, 2048), BF),
            pltpu.VMEM((2, 2048, 256), BF),
            pltpu.VMEM((2, 256, 2048), F32),
            pltpu.VMEM((2, 2048, 256), F32),
            pltpu.SemaphoreType.DMA((18,)),
            pltpu.SemaphoreType.DMA((18,)),
        ],
        compiler_params=pltpu.CompilerParams(vmem_limit_bytes=67043328),
        name="unpack",
    )(*results)


def per_device(
    slides,
    cotangent,
    kernel,
    kernel_bias,
    norm_gain,
    norm_bias,
    weight_in,
    bias_in,
    weight_out,
    bias_out,
    layer_scale,
):
    channels = slides.shape[-1]
    results = whole_step(
        slides.reshape(-1, channels),
        cotangent.reshape(-1, channels),
        kernel.transpose(1, 2, 0, 3),
        kernel_bias,
        norm_gain,
        norm_bias,
        bias_out,
        layer_scale,
        bias_in,
        weight_in,
        weight_out,
    )
    output, grad_slides, total_in, total_out, taps, sums, biases = unpack(*results)
    return (
        output.reshape(slides.shape),
        grad_slides.reshape(slides.shape),
        total_in,
        total_out,
        taps.transpose(2, 0, 1, 3),
        sums.transpose(1, 0, 2),
        biases,
    )


def solution(mesh):
    whole = P("dp", "row", "col", None)
    return jax.shard_map(
        per_device,
        mesh=mesh,
        in_specs=(whole, whole) + (P(),) * 4 + (P(None, "dp", None), P(), P(None, None, "dp"), P(), P()),
        out_specs=(whole, whole, P(None, "dp", None), P(None, None, "dp"), P(), P(), P()),
        check_vma=False,
    )
```

```python
import functools

import jax
import jax.numpy as jnp
from jax import lax
from jax.experimental import pallas as pl
from jax.experimental.pallas import tpu as pltpu
from jax.sharding import PartitionSpec as P

COEF = 0.7978845608028654
CUBIC = 0.044715
EPSILON = 1e-06

MESH = pl.DeviceIdType.MESH
BF = jnp.bfloat16
F32 = jnp.float32


class Place:
    def __init__(self):
        row = lax.axis_index("row")
        self.z = lax.axis_index("col")
        self.half = lax.axis_index("dp")
        self.core = lax.rem(row, 2)
        self.y = lax.rem(lax.div(row, 2), 4)
        self.x = lax.div(row, 8) * 2 + self.half

    def device(self, x=None, y=None, z=None, core=None):
        x = self.x if x is None else x
        y = self.y if y is None else y
        z = self.z if z is None else z
        core = self.core if core is None else core
        return {"row": (lax.div(x, 2) * 4 + y) * 2 + core, "col": z, "dp": lax.rem(x, 2)}

    def along(self, axis, offset):
        value = lax.rem(getattr(self, axis) + offset, 4)
        return value, self.device(**{axis: value})

    def sibling(self):
        return self.device(core=1 - self.core)


def meet(partners):
    barrier = pltpu.get_barrier_semaphore()
    for partner in partners:
        pl.semaphore_signal(barrier, inc=1, device_id=partner, device_id_type=MESH)
    pl.semaphore_wait(barrier, len(partners))


def part(start, size):
    if isinstance(start, int):
        return pl.ds(start, size)
    return pl.ds(pl.multiple_of(start, size), size)


def remote(src, dst, send, recv, target):
    return pltpu.make_async_remote_copy(
        src_ref=src, dst_ref=dst, send_sem=send, recv_sem=recv, device_id=target, device_id_type=MESH
    )


ORDERS = (("y", "z"), ("z", "y"))


class WeightIn:
    received = (128, 2048)
    turn = (64, 2048)
    first = (64, 512)
    second = (64, 128)
    third = (64, 128)

    def offered(grad, half, core):
        return grad.at[part(half * 256 + core * 128, 128), :]

    def cut(got, halves, turn, index):
        return got.at[halves, turn * 64 : turn * 64 + 64, part(index * 512, 512)]

    def cut_again(block, index):
        return block.at[:, :, part(index * 128, 128)]

    def placed(final, core, turn, one, two):
        return final.at[part(core * 128 + turn * 64, 64), part(one * 512 + two * 128, 128)]

    def line(final, core, turn, one):
        return final.at[part(core * 128 + turn * 64, 64), part(one * 512, 512)]

    def of_core(final, core):
        return final.at[part(core * 128, 128), :]


class WeightOut:
    received = (2048, 128)
    turn = (1024, 128)
    first = (256, 128)
    second = (64, 128)
    third = (64, 128)

    def offered(grad, half, core):
        return grad.at[:, part(half * 256 + core * 128, 128)]

    def cut(got, halves, turn, index):
        return got.at[halves, part(turn * 1024 + index * 256, 256), :]

    def cut_again(block, index):
        return block.at[:, part(index * 64, 64), :]

    def placed(final, core, turn, one, two):
        return final.at[part(turn * 1024 + one * 256 + two * 64, 64), part(core * 128, 128)]

    def line(final, core, turn, one):
        return final.at[part(turn * 1024 + one * 256, 256), part(core * 128, 128)]

    def of_core(final, core):
        return final.at[:, part(core * 128, 128)]


class Reduction:
    def __init__(self, me, kind, early, grad, final, bufs, sems):
        self.me, self.kind, self.early, self.grad, self.final = me, kind, early, grad, final
        self.got, self.given, self.r1, self.b1, self.r2, self.b2, self.r3 = bufs
        self.sems = sems
        self.copies = []
        self.steps = [
            [self.core_start],
            [self.core_finish, lambda: self.split_start(0)],
            [lambda: self.split_finish(0), lambda: self.split_start(1)],
            [lambda: self.split_finish(1), self.across_start],
            [self.across_finish, lambda: self.join_start(1)],
            [lambda: self.join_finish(1), lambda: self.join_start(0)],
            [lambda: self.join_finish(0), self.share_start],
            [self.share_finish],
        ]
        if early:
            self.steps[1:2] = [
                [self.core_finish, self.give_start],
                [self.give_finish, lambda: self.split_start(0)],
            ]

    def advance(self):
        for action in self.steps.pop(0):
            action()

    def sem(self, way, turn, step, slot):
        return self.sems.at[way, (turn * 8 + step) * 4 + slot]

    def go(self, src, dst, turn, step, send_slot, recv_slot, target):
        copy = remote(
            src, dst, self.sem(0, turn, step, send_slot), self.sem(1, turn, step, recv_slot), target
        )
        copy.start()
        self.copies.append(copy)

    def landed(self, dst, turn, step, slot):
        remote(
            dst, dst, self.sem(0, turn, step, slot), self.sem(1, turn, step, slot), self.me.sibling()
        ).wait_recv()

    def core_start(self):
        for half in range(2):
            src = self.kind.offered(self.grad, half, 1 - self.me.core)
            self.go(src, self.got.at[half], 0, 0, half, half, self.me.sibling())

    def core_finish(self):
        for half in range(2):
            self.landed(self.got.at[half], 0, 0, half)
            own = self.kind.offered(self.grad, half, self.me.core)
            total = own[...].astype(F32) + self.got[half].astype(F32)
            self.got[half] = total.astype(self.got.dtype)

    def block(self, turn, step, index):
        if step == 0:
            halves = pl.ds(self.me.half, 1) if self.early else slice(None)
            return self.kind.cut(self.got, halves, turn, index)
        return self.kind.cut_again(self.b1.at[turn], index)

    def split_start(self, step):
        target = (self.r1, self.r2)[step]
        for turn in range(2):
            for offset in (1, 3, 2):
                index, device = self.me.along(ORDERS[turn][step], offset)
                self.go(
                    self.block(turn, step, index),
                    target.at[turn, offset - 1],
                    turn,
                    1 + step,
                    offset,
                    offset,
                    device,
                )

    def split_finish(self, step):
        target, result = ((self.r1, self.b1), (self.r2, self.b2))[step]
        for turn in range(2):
            index = getattr(self.me, ORDERS[turn][step])
            total = self.block(turn, step, index)[...].astype(F32)
            for offset in (1, 3, 2):
                self.landed(target.at[turn, offset - 1], turn, 1 + step, offset)
                total = total + target[turn, offset - 1].astype(F32)
            result[turn] = total.astype(result.dtype)

    def turn_rows(self, half, turn):
        size = self.kind.turn[0]
        return self.got.at[half, turn * size : turn * size + size, :]

    def give_start(self):
        for turn, offset in ((0, 1), (1, 3)):
            _, device = self.me.along("x", offset)
            src = self.turn_rows(1 - self.me.half, turn)
            self.go(src, self.given.at[turn], turn, 7, 0, 0, device)

    def give_finish(self):
        for turn in range(2):
            self.landed(self.given.at[turn], turn, 7, 0)
            own = self.turn_rows(self.me.half, turn)
            total = own[...].astype(F32) + self.given[turn].astype(F32)
            own[...] = total.astype(self.got.dtype)

    def across_start(self):
        for turn in range(2):
            block = self.b2.at[turn]
            if self.early:
                _, device = self.me.along("x", 2)
                self.go(block.at[0], self.r3.at[turn, 0], turn, 3, 0, 0, device)
                continue
            for offset in (1, 3, 2):
                index, device = self.me.along("x", offset)
                src = block.at[lax.rem(index, 2)]
                self.go(src, self.r3.at[turn, self.me.x], turn, 3, offset, self.me.x, device)
            self.r3[turn, self.me.x] = block[self.me.half]

    def across_finish(self):
        me = self.me
        for turn in range(2):
            if self.early:
                self.landed(self.r3.at[turn, 0], turn, 3, 0)
                total = self.b2[turn, 0].astype(F32) + self.r3[turn, 0].astype(F32)
            else:
                for offset in (1, 3, 2):
                    index, _ = me.along("x", offset)
                    self.landed(self.r3.at[turn, index], turn, 3, index)
                total = self.r3[turn, 0].astype(F32)
                for index in range(1, 4):
                    total = total + self.r3[turn, index].astype(F32)
            one, two = (getattr(me, axis) for axis in ORDERS[turn])
            block = self.kind.placed(self.final, me.core, turn, one, two)
            block[...] = total.astype(self.final.dtype)

    def join_start(self, step):
        me = self.me
        for turn in range(2):
            one, two = (getattr(me, axis) for axis in ORDERS[turn])
            for offset in (1, 3, 2):
                _, device = me.along(ORDERS[turn][step], offset)
                if step == 1:
                    block = self.kind.placed(self.final, me.core, turn, one, two)
                else:
                    block = self.kind.line(self.final, me.core, turn, one)
                self.go(block, block, turn, 5 - step, offset, offset, device)

    def join_finish(self, step):
        me = self.me
        for turn in range(2):
            one, two = (getattr(me, axis) for axis in ORDERS[turn])
            for offset in (1, 3, 2):
                source = lax.rem((two if step == 1 else one) + 4 - offset, 4)
                if step == 1:
                    block = self.kind.placed(self.final, me.core, turn, one, source)
                else:
                    block = self.kind.line(self.final, me.core, turn, source)
                self.landed(block, turn, 5 - step, offset)

    def share_start(self):
        block = self.kind.of_core(self.final, self.me.core)
        self.go(block, block, 0, 6, 0, 0, self.me.sibling())

    def share_finish(self):
        block = self.kind.of_core(self.final, 1 - self.me.core)
        self.landed(block, 0, 6, 0)

    def drain(self):
        for copy in self.copies:
            copy.wait_send()


class SmallReduction:
    def __init__(self, me, grad, final, bufs, sems):
        self.me, self.grad, self.final = me, grad, final
        self.got, self.parts, self.lines = bufs
        self.sems = sems
        self.copies = []
        self.steps = [
            self.core_start,
            self.plane_start,
            self.across_start,
            self.join_start,
            self.share_start,
            self.share_finish,
        ]

    def advance(self):
        self.steps.pop(0)()

    def drain(self):
        for copy in self.copies:
            copy.wait_send()

    def go(self, src, dst, slot, target):
        copy = remote(src, dst, self.sems.at[0, slot], self.sems.at[1, slot], target)
        copy.start()
        self.copies.append(copy)

    def landed(self, dst, slot):
        target = self.me.sibling()
        remote(dst, dst, self.sems.at[0, slot], self.sems.at[1, slot], target).wait_recv()

    def others(self):
        for up in range(4):
            for deep in range(4):
                if up or deep:
                    y = lax.rem(self.me.y + up, 4)
                    z = lax.rem(self.me.z + deep, 4)
                    yield up * 4 + deep, y, z, self.me.device(y=y, z=z)

    def cell(self, ref, row, y, z):
        return ref.at[part(row + y * 16, 16), part(z * 128, 128)]

    def core_start(self):
        src = self.grad.at[part((1 - self.me.core) * 64, 64), :]
        self.go(src, self.got, 0, self.me.sibling())

    def plane_start(self):
        self.landed(self.got, 0)
        own = self.grad[part(self.me.core * 64, 64), :]
        self.got[...] = own + self.got[...]
        for slot, y, z, device in self.others():
            self.go(self.cell(self.got, 0, y, z), self.parts.at[slot], slot, device)

    def across_start(self):
        me = self.me
        total = self.cell(self.got, 0, me.y, me.z)[...]
        for slot, _, _, _ in self.others():
            self.landed(self.parts.at[slot], slot)
            total = total + self.parts[slot]
        self.lines[me.x] = total
        for offset in (1, 3, 2):
            _, device = me.along("x", offset)
            copy = remote(
                self.lines.at[me.x],
                self.lines.at[me.x],
                self.sems.at[0, 15 + offset],
                self.sems.at[1, 32 + me.x],
                device,
            )
            copy.start()
            self.copies.append(copy)

    def join_start(self):
        me = self.me
        for offset in (1, 3, 2):
            index, _ = me.along("x", offset)
            self.landed(self.lines.at[index], 32 + index)
        total = self.lines[0] + self.lines[1] + (self.lines[2] + self.lines[3])
        block = self.cell(self.final, me.core * 64, me.y, me.z)
        block[...] = total
        for slot, _, _, device in self.others():
            self.go(block, block, 40 + slot, device)

    def share_start(self):
        me = self.me
        for slot, _, _, _ in self.others():
            y = lax.rem(me.y + 4 - slot // 4, 4)
            z = lax.rem(me.z + 4 - slot % 4, 4)
            self.landed(self.cell(self.final, me.core * 64, y, z), 40 + slot)
        block = self.final.at[part(me.core * 64, 64), :]
        self.go(block, block, 60, me.sibling())

    def share_finish(self):
        block = self.final.at[part((1 - self.me.core) * 64, 64), :]
        self.landed(block, 60)


def reduction_scratch(kind, early):
    halves = 1 if early else 2
    return [
        pltpu.VMEM((2, *kind.received), BF),
        pltpu.VMEM((2, *kind.turn) if early else (2, 8, 128), BF),
        pltpu.VMEM((2, 3, halves, *kind.first), BF),
        pltpu.VMEM((2, halves, *kind.first), BF),
        pltpu.VMEM((2, 3, halves, *kind.second), BF),
        pltpu.VMEM((2, halves, *kind.second), BF),
        pltpu.VMEM((2, 4, *kind.third), BF),
        pltpu.SemaphoreType.DMA((2, 64)),
    ]


UNITS = (
    (WeightOut, 1, False),
    (WeightIn, 1, True),
    (WeightOut, 0, False),
    (WeightIn, 0, True),
)


class Gather:
    def __init__(self, me, shard_in, shard_out, full_in, full_out, sems):
        self.me = me
        self.shards = (shard_in, shard_out)
        self.full = (full_in, full_out)
        self.local, self.send, self.recv, self.send_core, self.recv_core = sems
        self.sides = (me.along("x", 1)[1], me.along("x", 3)[1])
        self.copies = []

    def block(self, which, kind, half, core, side):
        full = self.full[kind].at[which]
        if kind == 0:
            return full.at[part(half * 256 + core * 128 + side * 64, 64), :]
        return full.at[part(core * 1024 + side * 512, 512), part(half * 256, 256)]

    def place(self, which, kind):
        half = part(self.me.half * 256, 256)
        full = self.full[kind].at[which]
        own = full.at[half, :] if kind == 0 else full.at[:, half]
        return pltpu.make_async_copy(self.shards[kind].at[which], own, self.local.at[which, kind])

    def hop(self, which, kind, half, core, side, across):
        block = self.block(which, kind, half, core, side)
        if across:
            sems, target = (self.send, self.recv), self.sides[side]
        else:
            sems, target = (self.send_core, self.recv_core), self.me.sibling()
        return remote(block, block, *(s.at[which, kind, side] for s in sems), target)

    def start(self, which, kind):
        self.place(which, kind).wait()
        for side in range(2):
            copy = self.hop(which, kind, self.me.half, self.me.core, side, True)
            copy.start()
            self.copies.append(copy)

    def forward(self, which, kind):
        other = 1 - self.me.half
        for side in range(2):
            self.hop(which, kind, other, self.me.core, side, True).wait_recv()
            copy = self.hop(which, kind, other, self.me.core, side, False)
            copy.start()
            self.copies.append(copy)

    def finish(self, which, kind):
        for side in range(2):
            self.hop(which, kind, 1 - self.me.half, 1 - self.me.core, side, False).wait_recv()

    def drain(self):
        for copy in self.copies:
            copy.wait_send()


SPAN = 38
BACK, FRONT = 14, 8


def word(i, j):
    start = (i * SPAN + j) * 8
    return pl.ds(start if isinstance(start, int) else pl.multiple_of(start, 8), 8)


def put_row(padded, row, first, values, halves=(0, 1)):
    for half in halves:
        i = row - 8 * half
        if 0 <= i < BACK:
            for group in range(4):
                padded[pl.ds((i * SPAN + first) * 8 + half * 4 + group, values.shape[0], stride=8), :] = (
                    values[:, group * 128 : group * 128 + 128]
                )


def rolled(values):
    return jnp.concatenate([values[4:], values[:4]], axis=0)


class Halo:
    def __init__(self, me, padded, tile, bufs):
        self.me, self.padded, self.tile = me, padded, tile
        self.rows, self.side_out, self.sides, self.corner_out, self.corners, self.sems = bufs
        self.copies = []
        self.row = (lax.div(me.x, 2) * 4 + me.y) * 2 + me.core

    def target(self, down, right):
        row = lax.rem(self.row + down + 16, 16)
        col = lax.rem(self.me.z + right + 4, 4)
        return {"row": row, "col": col, "dp": self.me.half}

    def messages(self):
        tile = self.tile
        yield tile.at[pl.ds(0, 96), :], self.rows.at[1], (-1, 0)
        yield tile.at[pl.ds(416, 96), :], self.rows.at[0], (1, 0)
        for side in range(2):
            yield self.side_out.at[side], self.sides.at[1 - side], (0, 2 * side - 1)
        for low in range(2):
            for side in range(2):
                yield (
                    self.corner_out.at[low, side],
                    self.corners.at[1 - low, 1 - side],
                    (2 * low - 1, 2 * side - 1),
                )

    def start(self):
        padded = self.padded
        for side, first in ((0, 3), (1, 32)):
            for j in range(3):
                lines = [padded[word(i, first + j), :] for i in range(3, 11)]
                self.side_out[side, j * 64 : j * 64 + 64, :] = jnp.concatenate(lines, 0).astype(BF)
            for low, top in ((0, 3), (1, 8)):
                lines = [
                    rolled(padded[word(top + i, first + j), :]) for i in range(3) for j in range(3)
                ]
                self.corner_out[low, side] = jnp.concatenate(lines + lines[:1], 0).astype(BF)
        for number, (src, dst, (down, right)) in enumerate(self.messages()):
            copy = remote(
                src, dst, self.sems.at[0, number], self.sems.at[1, number], self.target(down, right)
            )
            copy.start()
            self.copies.append(copy)

    def finish(self):
        padded = self.padded
        for number, (src, dst, _) in enumerate(self.messages()):
            remote(
                src, dst, self.sems.at[0, number], self.sems.at[1, number], self.target(1, 0)
            ).wait_recv()
        inside = [
            (self.row > 0).astype(F32),
            (self.row < 15).astype(F32),
        ]
        across = [
            (self.me.z > 0).astype(F32),
            (self.me.z < 3).astype(F32),
        ]
        for low in range(2):
            for r in range(3):
                values = self.rows[low, r * 32 : r * 32 + 32, :].astype(F32) * inside[low]
                put_row(padded, r + 19 * low, 3, values, (low,))
        for side, first in ((0, 0), (1, 35)):
            for j in range(3):
                lines = self.sides[side, j * 64 : j * 64 + 64, :].astype(F32) * across[side]
                for m in range(8):
                    line = lines[m * 8 : m * 8 + 8]
                    padded[word(m + 3, first + j), :] = line
                    at = first + j
                    if m >= 5:
                        padded[pl.ds(((m - 5) * SPAN + at) * 8 + 4, 4), :] = line[:4]
                    if m < 3:
                        padded[pl.ds(((m + 11) * SPAN + at) * 8, 4), :] = line[4:]
            for low in range(2):
                lines = self.corners[low, side].astype(F32) * (inside[low] * across[side])
                for i in range(3):
                    for j in range(3):
                        line = lines[(i * 3 + j) * 8 : (i * 3 + j) * 8 + 8]
                        start = ((i + 11 * low) * SPAN + first + j) * 8 + 4 * low
                        padded[pl.ds(start, 4), :] = line[4 * low : 4 * low + 4]

    def drain(self):
        for copy in self.copies:
            copy.wait_send()


def spread_taps(kernel, which, taps):
    for p in range(7):
        for group in range(4):
            values = kernel[p, :, which, group * 128 : group * 128 + 128]
            for half in range(2):
                taps[pl.ds(p * 56 + half * 4 + group, 7, stride=8), :] = values


def depthwise(padded, taps, result, flipped, first=0, last=32):
    def columns(pair, _):
        j = pair * 2
        totals = [[None] * FRONT for _ in range(2)]
        for c in range(8):
            values = [padded[word(i, j + c), :] for i in range(BACK)]
            for side in range(2):
                q = c - side
                if not 0 <= q < 7:
                    continue
                total = totals[side]
                for p in range(7):
                    number = (6 - p) * 7 + 6 - q if flipped else p * 7 + q
                    tap = taps[number * 8 : number * 8 + 8, :]
                    for i in range(FRONT):
                        term = values[i + p] * tap
                        total[i] = term if total[i] is None else total[i] + term
        for side in range(2):
            for i in range(FRONT):
                result[pl.ds(pl.multiple_of((i * 32 + j + side) * 8, 8), 8), :] = totals[side][i]
        return 0

    lax.fori_loop(first // 2, last // 2, columns, 0)


def add_rim(padded, taps, result):
    place = lax.broadcasted_iota(jnp.int32, (8, 128), 0)
    top = jnp.where(place < 4, 1.0, 0.0).astype(F32)
    bottom = 1.0 - top

    def tap_of(p, q):
        return taps[(p * 7 + q) * 8 : (p * 7 + q) * 8 + 8, :]

    def add(i, j, value):
        start = (i * 32 + j) * 8
        at = pl.ds(start if isinstance(start, int) else pl.multiple_of(start, 8), 8)
        result[at, :] = result[at, :] + value

    def rows_of(j, columns):
        for base, mask, outs in ((0, top, (0, 1, 2)), (11, bottom, (5, 6, 7))):
            totals = {}
            for q in columns:
                for line in range(3):
                    value = padded[word(base + line, j + q), :] * mask
                    for i in outs:
                        p = base + line - i
                        if 0 <= p < 7:
                            term = value * tap_of(p, q)
                            totals[i] = term if i not in totals else totals[i] + term
            for i in outs:
                add(i, j, totals[i])

    def column(j, _):
        rows_of(j, range(7))
        return 0

    lax.fori_loop(3, 29, column, 0)
    for j in (0, 1, 2, 29, 30, 31):
        inner = [q for q in range(7) if 3 <= j + q < 35]
        rows_of(j, inner)
        totals = [None] * FRONT
        for q in range(7):
            if q in inner:
                continue
            values = [padded[word(i, j + q), :] for i in range(BACK)]
            for p in range(7):
                for i in range(FRONT):
                    term = values[i + p] * tap_of(p, q)
                    totals[i] = term if totals[i] is None else totals[i] + term
        for i in range(FRONT):
            add(i, j, totals[i])


def tap_grads(padded, upstream, small, base, columns):
    for q in columns:

        def column(j, totals):
            values = [padded[word(i, j + q), :] for i in range(BACK)]
            grads = [upstream[word(i + 3, j + 3), :] for i in range(FRONT)]
            result = []
            for p in range(7):
                total = totals[p]
                for i in range(FRONT):
                    total = total + values[i + p] * grads[i]
                result.append(total)
            return tuple(result)

        zero = jnp.zeros((8, 128), F32)
        totals = lax.fori_loop(0, 32, column, (zero,) * 7, unroll=4)
        for p in range(7):
            both = totals[p][:4] + totals[p][4:]
            for group in range(4):
                small[base + p * 7 + q : base + p * 7 + q + 1, group * 128 : group * 128 + 128] = both[
                    group : group + 1
                ]


def pixels(result, row):
    half, i = row // 8, row % 8
    return jnp.concatenate(
        [result[pl.ds(i * 256 + half * 4 + group, 32, stride=8), :] for group in range(4)], axis=1
    )


def dot(left, right, left_dim=1, right_dim=0):
    return lax.dot_general(
        left, right, (((left_dim,), (right_dim,)), ((), ())), preferred_element_type=F32
    )


def gelu_and_slope(values):
    square = values * values
    tangent = jnp.tanh(COEF * values * (1.0 + CUBIC * square))
    lift = 0.5 * (1.0 + tangent)
    slope = lift + 0.5 * values * (1.0 - tangent * tangent) * (COEF + (3.0 * COEF * CUBIC) * square)
    return values * lift, slope


CHUNK = 256


def step_kernel(
    slides, cotangent, kernel, kernel_bias, norm_gain, norm_bias, bias_out, layer_scale, bias_in,
    shard_in, shard_out,
    output, grad_slides, final_in, final_out, final_small,
    full_in, full_out, padded0, padded1, padded_g0, padded_g1, result, taps,
    normed, rstd, normal, turned, act, slope, hidden_grad, branch, carry, upstream, low,
    gm_tile, middle, grad_in, grad_out, small,
    *rest,
):
    me = Place()
    gather = Gather(me, shard_in, shard_out, full_in, full_out, rest[:5])
    padded = (padded0, padded1)
    padded_g = (padded_g0, padded_g1)
    tiles = (slides, middle)
    halos = [
        Halo(me, grid, tile, rest[5 + 6 * k : 11 + 6 * k])
        for k, (grid, tile) in enumerate(
            ((padded0, slides), (padded1, middle), (padded_g1, gm_tile.at[1]), (padded_g0, gm_tile.at[0]))
        )
    ]
    scratch = rest[30:]
    ways = {}
    for number, (kind, which, early) in enumerate(UNITS):
        bufs = scratch[number * 8 : number * 8 + 7]
        sems = scratch[number * 8 + 7]
        if kind is WeightIn:
            ends = (grad_in.at[which], final_in.at[which])
        else:
            ends = (grad_out.at[which], final_out.at[which])
        ways[kind, which] = Reduction(me, kind, early, *ends, bufs, sems)

    little = SmallReduction(me, small, final_small, scratch[-4:-1], scratch[-1])

    def reducing(which):
        return [ways[WeightOut, which], ways[WeightIn, which]]

    def line(which, ref):
        return ref[which : which + 1, :]

    for which in range(2):
        for kind in range(2):
            gather.place(which, kind).start()

    scope = jax.named_scope

    def fill(grid, tile):
        for r in range(16):
            put_row(grid, r + 3, 3, tile[r * 32 : r * 32 + 32, :].astype(F32))

    partners = [me.along("x", offset)[1] for offset in (1, 2, 3)]
    partners += [device for _, _, _, device in little.others()]
    around = [
        halos[0].target(down, right) for down in (-1, 0, 1) for right in (-1, 0, 1) if down
    ]
    with scope("p00a_fill"):
        padded0[...] = jnp.zeros_like(padded0)
        padded1[...] = jnp.zeros_like(padded1)
        fill(padded0, slides)
        for which in range(2):
            spread_taps(kernel, which, taps.at[which])
        small[...] = jnp.zeros_like(small)
        carry[...] = jnp.zeros_like(carry)
    with scope("p00b_meet"):
        meet(partners + around + [me.sibling()])
    with scope("p00c_start"):
        halos[0].start()
        gather.start(0, 0)
        gather.start(0, 1)
        gather.start(1, 0)

    def filter_map(which, first, last):
        depthwise(padded[which], taps.at[which], result, False, first, last)

    def normalise(which):
        for r in range(16):
            rows = slice(r * 32, r * 32 + 32)
            mixed = pixels(result, r) + line(which, kernel_bias)
            center = mixed - jnp.mean(mixed, -1, keepdims=True)
            inverse = lax.rsqrt(jnp.mean(center * center, -1, keepdims=True) + EPSILON)
            values = center * inverse
            normed[which, rows, :] = values
            rstd[which, rows, :] = jnp.broadcast_to(inverse, (32, 128))
            normal[which, rows, :] = (values * line(which, norm_gain) + line(which, norm_bias)).astype(BF)

    def expand(which, tilts, first=0, last=2048 // CHUNK):
        def chunk(c, _):
            cols = part(c * CHUNK, CHUNK)
            hidden = dot(normal[which], full_in[which, :, cols]) + bias_in[which : which + 1, cols]
            value, tilt = gelu_and_slope(hidden)
            act[which, :, cols] = value.astype(BF)
            if tilts is None:
                grads = dot(low[...], full_out[which, cols, :], 1, 1) * tilt
                keep_hidden_grad(which, c, cols, grads)
            else:
                tilts[:, cols] = tilt.astype(BF)
            return 0

        lax.fori_loop(first, last, chunk, 0)

    def hidden_grads(which, tilts, last):
        def chunk(c, _):
            cols = part(c * CHUNK, CHUNK)
            grads = dot(low[...], full_out[which, cols, :], 1, 1) * tilts[:, cols].astype(F32)
            keep_hidden_grad(which, c, cols, grads)
            return 0

        lax.fori_loop(0, last, chunk, 0)

    def keep_hidden_grad(which, c, cols, grads):
        hidden_grad[:, cols] = grads.astype(BF)
        bias_grad[which : which + 1, cols] = jnp.sum(grads, 0, keepdims=True)

    bias_grad = rest[29]

    def contract(which):
        def chunk(n, _):
            cols = part(n * CHUNK, CHUNK)
            branch[which, :, cols] = (
                dot(act[which], full_out[which, :, cols]) + bias_out[which : which + 1, cols]
            )
            return 0

        lax.fori_loop(0, 512 // CHUNK, chunk, 0)

    def residual(which, into):
        for r in range(16):
            rows = slice(r * 32, r * 32 + 32)
            value = tiles[which][rows, :].astype(F32) + line(which, layer_scale) * branch[which, rows, :]
            into[rows, :] = value.astype(BF)

    def enter(which, read):
        for r in range(16):
            rows = slice(r * 32, r * 32 + 32)
            grads = read(rows) * line(which, layer_scale)
            low[rows, :] = grads.astype(BF)
            add_rows(which, 0, grads)

    def add_rows(which, slot, values):
        total = values[0:8] + values[8:16] + (values[16:24] + values[24:32])
        carry[which, slot] = carry[which, slot] + total

    def weight_grads(which):
        def chunk(c, _):
            cols = part(c * CHUNK, CHUNK)
            grad_out[which, cols, :] = dot(act[which, :, cols], low[...], 0, 0).astype(BF)
            grad_in[which, :, cols] = dot(turned[...], hidden_grad[:, cols]).astype(BF)
            return 0

        turned[...] = normal[which].T
        lax.fori_loop(0, 2048 // CHUNK, chunk, 0)

    def normal_grads(which, target):
        def chunk(n, _):
            rows = part(n * CHUNK, CHUNK)
            target[:, rows] = dot(hidden_grad[...], full_in[which, rows, :], 1, 1)
            return 0

        lax.fori_loop(0, 512 // CHUNK, chunk, 0)

    def leave(which, grads_ref):
        for r in range(16):
            rows = slice(r * 32, r * 32 + 32)
            grads = grads_ref[rows, :]
            values = normed[which, rows, :]
            add_rows(which, 2, grads)
            add_rows(which, 1, grads * values)
            scaled = grads * line(which, norm_gain)
            mean = jnp.mean(scaled, -1, keepdims=True)
            tilt = jnp.mean(scaled * values, -1, keepdims=True)
            mixed = (scaled - mean - values * tilt) * rstd[which, rows, 0:1]
            add_rows(which, 3, mixed)
            put_row(padded_g[which], r + 3, 3, mixed)
            gm_tile[which, rows, :] = mixed.astype(BF)

    def scale_grad(which, read):
        for r in range(16):
            rows = slice(r * 32, r * 32 + 32)
            add_rows(which, 4, read(rows) * branch[which, rows, :])

    def settle(which):
        for slot, row in ((3, 0), (1, 1), (2, 2), (0, 3), (4, 4)):
            at = which * 64 + 49 + row
            small[at : at + 1, :] = jnp.sum(carry[which, slot], 0, keepdims=True)
        for c in range(4):
            at = which * 64 + 54 + c
            small[at : at + 1, :] = bias_grad[which : which + 1, c * 512 : c * 512 + 512]

    def from_cotangent(rows):
        return cotangent[rows, :].astype(F32)

    def from_upstream(rows):
        return upstream[rows, :]

    with scope("p01_depth0"):
        enter(1, from_cotangent)
        filter_map(0, 0, 32)
    with scope("p01_halo0"):
        halos[0].finish()
    with scope("p01_rim0"):
        add_rim(padded0, taps.at[0], result)
    with scope("p02_forward_in0"):
        gather.forward(0, 0)
    with scope("p03_norm0"):
        normalise(0)
    with scope("p04_finish_in0"):
        gather.finish(0, 0)
    with scope("p05_expand0"):
        expand(0, slope, 0, 5)
    with scope("p05_forward_out0"):
        gather.forward(0, 1)
    with scope("p05_expand0b"):
        expand(0, slope, 5)
    with scope("p06_finish_out0"):
        gather.finish(0, 1)
    with scope("p06_contract0"):
        contract(0)
        residual(0, middle)
        fill(padded1, middle)
    with scope("p07_halo1"):
        halos[1].start()
        gather.start(1, 1)
        gather.forward(1, 0)
    with scope("p08_depth1"):
        filter_map(1, 0, 32)
    with scope("p08_halo1_end"):
        halos[1].finish()
    with scope("p09_norm1"):
        add_rim(padded1, taps.at[1], result)
        normalise(1)
    with scope("p09_finish_in1"):
        gather.finish(1, 0)
    with scope("p10_expand1"):
        expand(1, hidden_grad, 0, 2)
    with scope("p10_forward_out1"):
        gather.forward(1, 1)
    with scope("p10_expand1b"):
        expand(1, hidden_grad, 2, 4)
    with scope("p10_finish_out1"):
        gather.finish(1, 1)
    with scope("p11_expand1"):
        expand(1, None, 4)
        hidden_grads(1, hidden_grad, 4)
    with scope("p12_ngrads1"):
        normal_grads(1, upstream)
    with scope("p13_leave1"):
        leave(1, upstream)
        halos[2].start()
    out1, in1 = reducing(1)
    out0, in0 = reducing(0)

    def go(name, *group):
        with scope(name):
            for way in group:
                way.advance()

    with scope("p14_wgrads1"):
        weight_grads(1)
        out1.advance()
        in1.advance()
    with scope("p16_halo2_end"):
        halos[2].finish()
    with scope("p17_depth1"):
        depthwise(padded_g1, taps.at[1], result, True, 0, 10)
    go("p17_go1", out1, in1)
    with scope("p17_depth1b"):
        depthwise(padded_g1, taps.at[1], result, True, 10, 32)
        for r in range(16):
            rows = slice(r * 32, r * 32 + 32)
            upstream[rows, :] = from_cotangent(rows) + pixels(result, r)
    with scope("p18_enter0"):
        enter(0, from_upstream)
        scale_grad(0, from_upstream)

    with scope("p19_hidden0"):
        hidden_grads(0, slope, 2048 // CHUNK)
    go("p20_go1", out1, in1)
    with scope("p21_wgrads0"):
        weight_grads(0)
    in0.advance()
    out0.advance()
    with scope("p23_ngrads0"):
        normal_grads(0, normed.at[1])
    go("p23_go1", out1, in1)
    go("p23_go0", in0)
    with scope("p24_leave0"):
        leave(0, normed.at[1])
        halos[3].start()
    go("p25_go0", out0)
    with scope("p26_contract1"):
        contract(1)
        residual(1, output)
        scale_grad(1, from_cotangent)
        settle(1)
        settle(0)
    go("p27_go1", in1, out1)
    with scope("p28_taps0"):
        tap_grads(padded0, padded_g0, small, 0, range(7))
    go("p29_go0", in0)
    go("p29_go1", in1)
    with scope("p29_taps1"):
        tap_grads(padded1, padded_g1, small, 64, range(7))
    little.advance()
    go("p30_go0", in0)
    go("p30_go0b", out0)
    go("p30_go1", out1, in1)
    with scope("p30_halo3_end"):
        halos[3].finish()
    with scope("p31_depth0"):
        depthwise(padded_g0, taps.at[0], result, True, 0, 16)
    go("p31_go", little, in0, out0)
    with scope("p33_depth0"):
        depthwise(padded_g0, taps.at[0], result, True, 16, 32)
    go("p33_go", in0, little, out0)
    with scope("p33_depth0b"):
        for r in range(16):
            rows = slice(r * 32, r * 32 + 32)
            grad_slides[rows, :] = (upstream[rows, :] + pixels(result, r)).astype(BF)
    go("p34_go", in0, little, out0, out1, in1)
    go("p35_go", in0, little, out0)
    go("p36_go", in0, little, out0, out1, in1)
    every = [out1, in1, little, out0, in0]
    with scope("p38_rest"):
        while any(way.steps for way in every):
            for way in every:
                if way.steps:
                    way.advance()
    with scope("p39_drain"):
        for way in every + halos + [gather]:
            way.drain()


def halo_scratch():
    return [
        pltpu.VMEM((2, 96, 512), BF),
        pltpu.VMEM((2, 192, 128), BF),
        pltpu.VMEM((2, 192, 128), BF),
        pltpu.VMEM((2, 2, 80, 128), BF),
        pltpu.VMEM((2, 2, 80, 128), BF),
        pltpu.SemaphoreType.DMA((2, 8)),
    ]


def whole_step(*operands):
    vmem = pl.BlockSpec(memory_space=pltpu.VMEM)
    grid = pltpu.VMEM((BACK * SPAN * 8, 128), F32)
    scratch = [
        pltpu.VMEM((2, 512, 2048), BF),
        pltpu.VMEM((2, 2048, 512), BF),
        grid,
        grid,
        grid,
        grid,
        pltpu.VMEM((8 * 32 * 8, 128), F32),
        pltpu.VMEM((2, 49 * 8, 128), F32),
        pltpu.VMEM((2, 512, 512), F32),
        pltpu.VMEM((2, 512, 128), F32),
        pltpu.VMEM((2, 512, 512), BF),
        pltpu.VMEM((512, 512), BF),
        pltpu.VMEM((2, 512, 2048), BF),
        pltpu.VMEM((512, 2048), BF),
        pltpu.VMEM((512, 2048), BF),
        pltpu.VMEM((2, 512, 512), F32),
        pltpu.VMEM((2, 5, 8, 512), F32),
        pltpu.VMEM((512, 512), F32),
        pltpu.VMEM((512, 512), BF),
        pltpu.VMEM((2, 512, 512), BF),
        pltpu.VMEM((512, 512), BF),
        pltpu.VMEM((2, 512, 2048), BF),
        pltpu.VMEM((2, 2048, 512), BF),
        pltpu.VMEM((128, 512), F32),
    ]
    scratch += [pltpu.SemaphoreType.DMA((2, 2))]
    scratch += [pltpu.SemaphoreType.DMA((2, 2, 2)) for _ in range(4)]
    for _ in range(4):
        scratch += halo_scratch()
    extra = [pltpu.VMEM((2, 2048), F32)]
    reductions = sum([reduction_scratch(kind, early) for kind, _, early in UNITS], [])
    reductions += [
        pltpu.VMEM((64, 512), F32),
        pltpu.VMEM((16, 16, 128), F32),
        pltpu.VMEM((4, 16, 128), F32),
        pltpu.SemaphoreType.DMA((2, 64)),
    ]
    return pl.pallas_call(
        step_kernel,
        out_shape=(
            jax.ShapeDtypeStruct((512, 512), BF),
            jax.ShapeDtypeStruct((512, 512), BF),
            jax.ShapeDtypeStruct((2, 256, 2048), BF),
            jax.ShapeDtypeStruct((2, 2048, 256), BF),
            jax.ShapeDtypeStruct((128, 512), F32),
        ),
        in_specs=[vmem] * 9 + [pl.BlockSpec(memory_space=pl.ANY)] * 2,
        out_specs=[vmem] * 5,
        scratch_shapes=scratch + extra + reductions,
        compiler_params=pltpu.CompilerParams(
            collective_id=0, has_side_effects=True, vmem_limit_bytes=67043328
        ),
        name="whole_step",
    )(*operands)


def unpack_kernel(
    output, grad_slides, total_in, total_out, small,
    output_end, slides_end, in_end, out_end, kernel_end, channel_end, bias_end,
    maps, low_in, low_out, wide_in, wide_out, get, put,
):
    steps = []
    for which in range(2):
        for cut in range(4):
            for ends, size in (
                ((total_in, low_in, wide_in, in_end), 64),
                ((total_out, low_out, wide_out, out_end), 512),
            ):
                steps.append([ref.at[which, pl.ds(cut * size, size), :] for ref in ends])
    steps.append([output, maps.at[0], maps.at[0], output_end])
    steps.append([grad_slides, maps.at[1], maps.at[1], slides_end])
    for number, (src, low, _, _) in enumerate(steps):
        pltpu.make_async_copy(src, low, get.at[number]).start()
    for number, (src, low, wide, dst) in enumerate(steps):
        pltpu.make_async_copy(src, low, get.at[number]).wait()
        if number < 16:
            wide[...] = low[...].astype(F32)
        pltpu.make_async_copy(wide, dst, put.at[number]).start()
    for which in range(2):
        base = which * 64
        for p in range(7):
            kernel_end[p, :, which, :] = small[base + p * 7 : base + p * 7 + 7, :]
        channel_end[:, which, :] = small[base + 49 : base + 54, :]
        for c in range(4):
            bias_end[which : which + 1, c * 512 : c * 512 + 512] = small[
                base + 54 + c : base + 55 + c, :
            ]
    for number, (_, _, wide, dst) in enumerate(steps):
        pltpu.make_async_copy(wide, dst, put.at[number]).wait()


def unpack(*results):
    vmem = pl.BlockSpec(memory_space=pltpu.VMEM)
    hbm = pl.BlockSpec(memory_space=pl.ANY)
    return pl.pallas_call(
        unpack_kernel,
        out_shape=(
            jax.ShapeDtypeStruct((512, 512), BF),
            jax.ShapeDtypeStruct((512, 512), BF),
            jax.ShapeDtypeStruct((2, 256, 2048), F32),
            jax.ShapeDtypeStruct((2, 2048, 256), F32),
            jax.ShapeDtypeStruct((7, 7, 2, 512), F32),
            jax.ShapeDtypeStruct((5, 2, 512), F32),
            jax.ShapeDtypeStruct((2, 2048), F32),
        ),
        in_specs=[hbm] * 4 + [vmem],
        out_specs=[hbm] * 4 + [vmem] * 3,
        scratch_shapes=[
            pltpu.VMEM((2, 512, 512), BF),
            pltpu.VMEM((2, 256, 2048), BF),
            pltpu.VMEM((2, 2048, 256), BF),
            pltpu.VMEM((2, 256, 2048), F32),
            pltpu.VMEM((2, 2048, 256), F32),
            pltpu.SemaphoreType.DMA((18,)),
            pltpu.SemaphoreType.DMA((18,)),
        ],
        compiler_params=pltpu.CompilerParams(vmem_limit_bytes=67043328),
        name="unpack",
    )(*results)


def per_device(
    slides,
    cotangent,
    kernel,
    kernel_bias,
    norm_gain,
    norm_bias,
    weight_in,
    bias_in,
    weight_out,
    bias_out,
    layer_scale,
):
    channels = slides.shape[-1]
    results = whole_step(
        slides.reshape(-1, channels),
        cotangent.reshape(-1, channels),
        kernel.transpose(1, 2, 0, 3),
        kernel_bias,
        norm_gain,
        norm_bias,
        bias_out,
        layer_scale,
        bias_in,
        weight_in,
        weight_out,
    )
    output, grad_slides, total_in, total_out, taps, sums, biases = unpack(*results)
    return (
        output.reshape(slides.shape),
        grad_slides.reshape(slides.shape),
        total_in,
        total_out,
        taps.transpose(2, 0, 1, 3),
        sums.transpose(1, 0, 2),
        biases,
    )


def solution(mesh):
    whole = P("dp", "row", "col", None)
    return jax.shard_map(
        per_device,
        mesh=mesh,
        in_specs=(whole, whole) + (P(),) * 4 + (P(None, "dp", None), P(), P(None, None, "dp"), P(), P()),
        out_specs=(whole, whole, P(None, "dp", None), P(None, None, "dp"), P(), P(), P()),
        check_vma=False,
    )
```

```python
import functools

import jax
import jax.numpy as jnp
from jax import lax
from jax.experimental import pallas as pl
from jax.experimental.pallas import tpu as pltpu
from jax.sharding import PartitionSpec as P

COEF = 0.7978845608028654
CUBIC = 0.044715
EPSILON = 1e-06

MESH = pl.DeviceIdType.MESH
BF = jnp.bfloat16
F32 = jnp.float32


class Place:
    def __init__(self):
        row = lax.axis_index("row")
        self.z = lax.axis_index("col")
        self.half = lax.axis_index("dp")
        self.core = lax.rem(row, 2)
        self.y = lax.rem(lax.div(row, 2), 4)
        self.x = lax.div(row, 8) * 2 + self.half

    def device(self, x=None, y=None, z=None, core=None):
        x = self.x if x is None else x
        y = self.y if y is None else y
        z = self.z if z is None else z
        core = self.core if core is None else core
        return {"row": (lax.div(x, 2) * 4 + y) * 2 + core, "col": z, "dp": lax.rem(x, 2)}

    def along(self, axis, offset):
        value = lax.rem(getattr(self, axis) + offset, 4)
        return value, self.device(**{axis: value})

    def sibling(self):
        return self.device(core=1 - self.core)


def meet(partners):
    barrier = pltpu.get_barrier_semaphore()
    for partner in partners:
        pl.semaphore_signal(barrier, inc=1, device_id=partner, device_id_type=MESH)
    pl.semaphore_wait(barrier, len(partners))


def part(start, size):
    if isinstance(start, int):
        return pl.ds(start, size)
    return pl.ds(pl.multiple_of(start, size), size)


def remote(src, dst, send, recv, target):
    return pltpu.make_async_remote_copy(
        src_ref=src, dst_ref=dst, send_sem=send, recv_sem=recv, device_id=target, device_id_type=MESH
    )


ORDERS = (("y", "z"), ("z", "y"))


class WeightIn:
    received = (128, 2048)
    turn = (64, 2048)
    first = (64, 512)
    second = (64, 128)
    third = (64, 128)

    def offered(grad, half, core):
        return grad.at[part(half * 256 + core * 128, 128), :]

    def cut(got, halves, turn, index):
        return got.at[halves, turn * 64 : turn * 64 + 64, part(index * 512, 512)]

    def cut_again(block, index):
        return block.at[:, :, part(index * 128, 128)]

    def placed(final, core, turn, one, two):
        return final.at[part(core * 128 + turn * 64, 64), part(one * 512 + two * 128, 128)]

    def line(final, core, turn, one):
        return final.at[part(core * 128 + turn * 64, 64), part(one * 512, 512)]

    def of_core(final, core):
        return final.at[part(core * 128, 128), :]


class WeightOut:
    received = (2048, 128)
    turn = (1024, 128)
    first = (256, 128)
    second = (64, 128)
    third = (64, 128)

    def offered(grad, half, core):
        return grad.at[:, part(half * 256 + core * 128, 128)]

    def cut(got, halves, turn, index):
        return got.at[halves, part(turn * 1024 + index * 256, 256), :]

    def cut_again(block, index):
        return block.at[:, part(index * 64, 64), :]

    def placed(final, core, turn, one, two):
        return final.at[part(turn * 1024 + one * 256 + two * 64, 64), part(core * 128, 128)]

    def line(final, core, turn, one):
        return final.at[part(turn * 1024 + one * 256, 256), part(core * 128, 128)]

    def of_core(final, core):
        return final.at[:, part(core * 128, 128)]


class Reduction:
    def __init__(self, me, kind, early, grad, final, bufs, sems):
        self.me, self.kind, self.early, self.grad, self.final = me, kind, early, grad, final
        self.got, self.given, self.r1, self.b1, self.r2, self.b2, self.r3 = bufs
        self.sems = sems
        self.copies = []
        self.steps = [
            [self.core_start],
            [self.core_finish, lambda: self.split_start(0)],
            [lambda: self.split_finish(0), lambda: self.split_start(1)],
            [lambda: self.split_finish(1), self.across_start],
            [self.across_finish, lambda: self.join_start(1)],
            [lambda: self.join_finish(1), lambda: self.join_start(0)],
            [lambda: self.join_finish(0), self.share_start],
            [self.share_finish],
        ]
        if early:
            self.steps[1:2] = [
                [self.core_finish, self.give_start],
                [self.give_finish, lambda: self.split_start(0)],
            ]

    def advance(self):
        for action in self.steps.pop(0):
            action()

    def sem(self, way, turn, step, slot):
        return self.sems.at[way, (turn * 8 + step) * 4 + slot]

    def go(self, src, dst, turn, step, send_slot, recv_slot, target):
        copy = remote(
            src, dst, self.sem(0, turn, step, send_slot), self.sem(1, turn, step, recv_slot), target
        )
        copy.start()
        self.copies.append(copy)

    def landed(self, dst, turn, step, slot):
        remote(
            dst, dst, self.sem(0, turn, step, slot), self.sem(1, turn, step, slot), self.me.sibling()
        ).wait_recv()

    def core_start(self):
        for half in range(2):
            src = self.kind.offered(self.grad, half, 1 - self.me.core)
            self.go(src, self.got.at[half], 0, 0, half, half, self.me.sibling())

    def core_finish(self):
        for half in range(2):
            self.landed(self.got.at[half], 0, 0, half)
            own = self.kind.offered(self.grad, half, self.me.core)
            total = own[...].astype(F32) + self.got[half].astype(F32)
            self.got[half] = total.astype(self.got.dtype)

    def block(self, turn, step, index):
        if step == 0:
            halves = pl.ds(self.me.half, 1) if self.early else slice(None)
            return self.kind.cut(self.got, halves, turn, index)
        return self.kind.cut_again(self.b1.at[turn], index)

    def split_start(self, step):
        target = (self.r1, self.r2)[step]
        for turn in range(2):
            for offset in (1, 3, 2):
                index, device = self.me.along(ORDERS[turn][step], offset)
                self.go(
                    self.block(turn, step, index),
                    target.at[turn, offset - 1],
                    turn,
                    1 + step,
                    offset,
                    offset,
                    device,
                )

    def split_finish(self, step):
        target, result = ((self.r1, self.b1), (self.r2, self.b2))[step]
        for turn in range(2):
            index = getattr(self.me, ORDERS[turn][step])
            total = self.block(turn, step, index)[...].astype(F32)
            for offset in (1, 3, 2):
                self.landed(target.at[turn, offset - 1], turn, 1 + step, offset)
                total = total + target[turn, offset - 1].astype(F32)
            result[turn] = total.astype(result.dtype)

    def turn_rows(self, half, turn):
        size = self.kind.turn[0]
        return self.got.at[half, turn * size : turn * size + size, :]

    def give_start(self):
        for turn, offset in ((0, 1), (1, 3)):
            _, device = self.me.along("x", offset)
            src = self.turn_rows(1 - self.me.half, turn)
            self.go(src, self.given.at[turn], turn, 7, 0, 0, device)

    def give_finish(self):
        for turn in range(2):
            self.landed(self.given.at[turn], turn, 7, 0)
            own = self.turn_rows(self.me.half, turn)
            total = own[...].astype(F32) + self.given[turn].astype(F32)
            own[...] = total.astype(self.got.dtype)

    def across_start(self):
        for turn in range(2):
            block = self.b2.at[turn]
            if self.early:
                _, device = self.me.along("x", 2)
                self.go(block.at[0], self.r3.at[turn, 0], turn, 3, 0, 0, device)
                continue
            for offset in (1, 3, 2):
                index, device = self.me.along("x", offset)
                src = block.at[lax.rem(index, 2)]
                self.go(src, self.r3.at[turn, self.me.x], turn, 3, offset, self.me.x, device)
            self.r3[turn, self.me.x] = block[self.me.half]

    def across_finish(self):
        me = self.me
        for turn in range(2):
            if self.early:
                self.landed(self.r3.at[turn, 0], turn, 3, 0)
                total = self.b2[turn, 0].astype(F32) + self.r3[turn, 0].astype(F32)
            else:
                for offset in (1, 3, 2):
                    index, _ = me.along("x", offset)
                    self.landed(self.r3.at[turn, index], turn, 3, index)
                total = self.r3[turn, 0].astype(F32)
                for index in range(1, 4):
                    total = total + self.r3[turn, index].astype(F32)
            one, two = (getattr(me, axis) for axis in ORDERS[turn])
            block = self.kind.placed(self.final, me.core, turn, one, two)
            block[...] = total.astype(self.final.dtype)

    def join_start(self, step):
        me = self.me
        for turn in range(2):
            one, two = (getattr(me, axis) for axis in ORDERS[turn])
            for offset in (1, 3, 2):
                _, device = me.along(ORDERS[turn][step], offset)
                if step == 1:
                    block = self.kind.placed(self.final, me.core, turn, one, two)
                else:
                    block = self.kind.line(self.final, me.core, turn, one)
                self.go(block, block, turn, 5 - step, offset, offset, device)

    def join_finish(self, step):
        me = self.me
        for turn in range(2):
            one, two = (getattr(me, axis) for axis in ORDERS[turn])
            for offset in (1, 3, 2):
                source = lax.rem((two if step == 1 else one) + 4 - offset, 4)
                if step == 1:
                    block = self.kind.placed(self.final, me.core, turn, one, source)
                else:
                    block = self.kind.line(self.final, me.core, turn, source)
                self.landed(block, turn, 5 - step, offset)

    def share_start(self):
        block = self.kind.of_core(self.final, self.me.core)
        self.go(block, block, 0, 6, 0, 0, self.me.sibling())

    def share_finish(self):
        block = self.kind.of_core(self.final, 1 - self.me.core)
        self.landed(block, 0, 6, 0)

    def drain(self):
        for copy in self.copies:
            copy.wait_send()


class SmallReduction:
    def __init__(self, me, grad, final, bufs, sems):
        self.me, self.grad, self.final = me, grad, final
        self.got, self.parts, self.lines = bufs
        self.sems = sems
        self.copies = []
        self.steps = [
            self.core_start,
            self.plane_start,
            self.across_start,
            self.join_start,
            self.share_start,
            self.share_finish,
        ]

    def advance(self):
        self.steps.pop(0)()

    def drain(self):
        for copy in self.copies:
            copy.wait_send()

    def go(self, src, dst, slot, target):
        copy = remote(src, dst, self.sems.at[0, slot], self.sems.at[1, slot], target)
        copy.start()
        self.copies.append(copy)

    def landed(self, dst, slot):
        target = self.me.sibling()
        remote(dst, dst, self.sems.at[0, slot], self.sems.at[1, slot], target).wait_recv()

    def others(self):
        for up in range(4):
            for deep in range(4):
                if up or deep:
                    y = lax.rem(self.me.y + up, 4)
                    z = lax.rem(self.me.z + deep, 4)
                    yield up * 4 + deep, y, z, self.me.device(y=y, z=z)

    def cell(self, ref, row, y, z):
        return ref.at[part(row + y * 16, 16), part(z * 128, 128)]

    def core_start(self):
        src = self.grad.at[part((1 - self.me.core) * 64, 64), :]
        self.go(src, self.got, 0, self.me.sibling())

    def plane_start(self):
        self.landed(self.got, 0)
        own = self.grad[part(self.me.core * 64, 64), :]
        self.got[...] = own + self.got[...]
        for slot, y, z, device in self.others():
            self.go(self.cell(self.got, 0, y, z), self.parts.at[slot], slot, device)

    def across_start(self):
        me = self.me
        total = self.cell(self.got, 0, me.y, me.z)[...]
        for slot, _, _, _ in self.others():
            self.landed(self.parts.at[slot], slot)
            total = total + self.parts[slot]
        self.lines[me.x] = total
        for offset in (1, 3, 2):
            _, device = me.along("x", offset)
            copy = remote(
                self.lines.at[me.x],
                self.lines.at[me.x],
                self.sems.at[0, 15 + offset],
                self.sems.at[1, 32 + me.x],
                device,
            )
            copy.start()
            self.copies.append(copy)

    def join_start(self):
        me = self.me
        for offset in (1, 3, 2):
            index, _ = me.along("x", offset)
            self.landed(self.lines.at[index], 32 + index)
        total = self.lines[0] + self.lines[1] + (self.lines[2] + self.lines[3])
        block = self.cell(self.final, me.core * 64, me.y, me.z)
        block[...] = total
        for slot, _, _, device in self.others():
            self.go(block, block, 40 + slot, device)

    def share_start(self):
        me = self.me
        for slot, _, _, _ in self.others():
            y = lax.rem(me.y + 4 - slot // 4, 4)
            z = lax.rem(me.z + 4 - slot % 4, 4)
            self.landed(self.cell(self.final, me.core * 64, y, z), 40 + slot)
        block = self.final.at[part(me.core * 64, 64), :]
        self.go(block, block, 60, me.sibling())

    def share_finish(self):
        block = self.final.at[part((1 - self.me.core) * 64, 64), :]
        self.landed(block, 60)


def reduction_scratch(kind, early):
    halves = 1 if early else 2
    return [
        pltpu.VMEM((2, *kind.received), BF),
        pltpu.VMEM((2, *kind.turn) if early else (2, 8, 128), BF),
        pltpu.VMEM((2, 3, halves, *kind.first), BF),
        pltpu.VMEM((2, halves, *kind.first), BF),
        pltpu.VMEM((2, 3, halves, *kind.second), BF),
        pltpu.VMEM((2, halves, *kind.second), BF),
        pltpu.VMEM((2, 4, *kind.third), BF),
        pltpu.SemaphoreType.DMA((2, 64)),
    ]


UNITS = (
    (WeightOut, 1, False),
    (WeightIn, 1, True),
    (WeightOut, 0, False),
    (WeightIn, 0, True),
)


class Gather:
    def __init__(self, me, shard_in, shard_out, full_in, full_out, sems):
        self.me = me
        self.shards = (shard_in, shard_out)
        self.full = (full_in, full_out)
        self.local, self.send, self.recv, self.send_core, self.recv_core = sems
        self.sides = (me.along("x", 1)[1], me.along("x", 3)[1])
        self.copies = []

    def block(self, which, kind, half, core, side):
        full = self.full[kind].at[which]
        if kind == 0:
            return full.at[part(half * 256 + core * 128 + side * 64, 64), :]
        return full.at[part(core * 1024 + side * 512, 512), part(half * 256, 256)]

    def place(self, which, kind):
        half = part(self.me.half * 256, 256)
        full = self.full[kind].at[which]
        own = full.at[half, :] if kind == 0 else full.at[:, half]
        return pltpu.make_async_copy(self.shards[kind].at[which], own, self.local.at[which, kind])

    def hop(self, which, kind, half, core, side, across):
        block = self.block(which, kind, half, core, side)
        if across:
            sems, target = (self.send, self.recv), self.sides[side]
        else:
            sems, target = (self.send_core, self.recv_core), self.me.sibling()
        return remote(block, block, *(s.at[which, kind, side] for s in sems), target)

    def start(self, which, kind):
        self.place(which, kind).wait()
        for side in range(2):
            copy = self.hop(which, kind, self.me.half, self.me.core, side, True)
            copy.start()
            self.copies.append(copy)

    def forward(self, which, kind):
        other = 1 - self.me.half
        for side in range(2):
            self.hop(which, kind, other, self.me.core, side, True).wait_recv()
            copy = self.hop(which, kind, other, self.me.core, side, False)
            copy.start()
            self.copies.append(copy)

    def finish(self, which, kind):
        for side in range(2):
            self.hop(which, kind, 1 - self.me.half, 1 - self.me.core, side, False).wait_recv()

    def drain(self):
        for copy in self.copies:
            copy.wait_send()


SPAN = 38
BACK, FRONT = 14, 8


def word(i, j):
    start = (i * SPAN + j) * 8
    return pl.ds(start if isinstance(start, int) else pl.multiple_of(start, 8), 8)


def put_row(padded, row, first, values, halves=(0, 1)):
    for half in halves:
        i = row - 8 * half
        if 0 <= i < BACK:
            for group in range(4):
                padded[pl.ds((i * SPAN + first) * 8 + half * 4 + group, values.shape[0], stride=8), :] = (
                    values[:, group * 128 : group * 128 + 128]
                )


def rolled(values):
    return jnp.concatenate([values[4:], values[:4]], axis=0)


class Halo:
    def __init__(self, me, padded, tile, bufs):
        self.me, self.padded, self.tile = me, padded, tile
        self.rows, self.side_out, self.sides, self.corner_out, self.corners, self.sems = bufs
        self.copies = []
        self.row = (lax.div(me.x, 2) * 4 + me.y) * 2 + me.core

    def target(self, down, right):
        row = lax.rem(self.row + down + 16, 16)
        col = lax.rem(self.me.z + right + 4, 4)
        return {"row": row, "col": col, "dp": self.me.half}

    def messages(self):
        tile = self.tile
        yield tile.at[pl.ds(0, 96), :], self.rows.at[1], (-1, 0)
        yield tile.at[pl.ds(416, 96), :], self.rows.at[0], (1, 0)
        for side in range(2):
            yield self.side_out.at[side], self.sides.at[1 - side], (0, 2 * side - 1)
        for low in range(2):
            for side in range(2):
                yield (
                    self.corner_out.at[low, side],
                    self.corners.at[1 - low, 1 - side],
                    (2 * low - 1, 2 * side - 1),
                )

    def start(self):
        padded = self.padded
        for side, first in ((0, 3), (1, 32)):
            for j in range(3):
                lines = [padded[word(i, first + j), :] for i in range(3, 11)]
                self.side_out[side, j * 64 : j * 64 + 64, :] = jnp.concatenate(lines, 0).astype(BF)
            for low, top in ((0, 3), (1, 8)):
                lines = [
                    rolled(padded[word(top + i, first + j), :]) for i in range(3) for j in range(3)
                ]
                self.corner_out[low, side] = jnp.concatenate(lines + lines[:1], 0).astype(BF)
        for number, (src, dst, (down, right)) in enumerate(self.messages()):
            copy = remote(
                src, dst, self.sems.at[0, number], self.sems.at[1, number], self.target(down, right)
            )
            copy.start()
            self.copies.append(copy)

    def finish(self):
        padded = self.padded
        for number, (src, dst, _) in enumerate(self.messages()):
            remote(
                src, dst, self.sems.at[0, number], self.sems.at[1, number], self.target(1, 0)
            ).wait_recv()
        inside = [
            (self.row > 0).astype(F32),
            (self.row < 15).astype(F32),
        ]
        across = [
            (self.me.z > 0).astype(F32),
            (self.me.z < 3).astype(F32),
        ]
        for low in range(2):
            for r in range(3):
                values = self.rows[low, r * 32 : r * 32 + 32, :].astype(F32) * inside[low]
                put_row(padded, r + 19 * low, 3, values, (low,))
        for side, first in ((0, 0), (1, 35)):
            for j in range(3):
                lines = self.sides[side, j * 64 : j * 64 + 64, :].astype(F32) * across[side]
                for m in range(8):
                    line = lines[m * 8 : m * 8 + 8]
                    padded[word(m + 3, first + j), :] = line
                    at = first + j
                    if m >= 5:
                        padded[pl.ds(((m - 5) * SPAN + at) * 8 + 4, 4), :] = line[:4]
                    if m < 3:
                        padded[pl.ds(((m + 11) * SPAN + at) * 8, 4), :] = line[4:]
            for low in range(2):
                lines = self.corners[low, side].astype(F32) * (inside[low] * across[side])
                for i in range(3):
                    for j in range(3):
                        line = lines[(i * 3 + j) * 8 : (i * 3 + j) * 8 + 8]
                        start = ((i + 11 * low) * SPAN + first + j) * 8 + 4 * low
                        padded[pl.ds(start, 4), :] = line[4 * low : 4 * low + 4]

    def drain(self):
        for copy in self.copies:
            copy.wait_send()


def spread_taps(kernel, which, taps):
    for p in range(7):
        for group in range(4):
            values = kernel[p, :, which, group * 128 : group * 128 + 128]
            for half in range(2):
                taps[pl.ds(p * 56 + half * 4 + group, 7, stride=8), :] = values


def depthwise(padded, taps, result, flipped, first=0, last=32):
    def columns(pair, _):
        j = pair * 2
        totals = [[None] * FRONT for _ in range(2)]
        for c in range(8):
            values = [padded[word(i, j + c), :] for i in range(BACK)]
            for side in range(2):
                q = c - side
                if not 0 <= q < 7:
                    continue
                total = totals[side]
                for p in range(7):
                    number = (6 - p) * 7 + 6 - q if flipped else p * 7 + q
                    tap = taps[number * 8 : number * 8 + 8, :]
                    for i in range(FRONT):
                        term = values[i + p] * tap
                        total[i] = term if total[i] is None else total[i] + term
        for side in range(2):
            for i in range(FRONT):
                result[pl.ds(pl.multiple_of((i * 32 + j + side) * 8, 8), 8), :] = totals[side][i]
        return 0

    lax.fori_loop(first // 2, last // 2, columns, 0)


def add_rim(padded, taps, result):
    place = lax.broadcasted_iota(jnp.int32, (8, 128), 0)
    top = jnp.where(place < 4, 1.0, 0.0).astype(F32)
    bottom = 1.0 - top

    def tap_of(p, q):
        return taps[(p * 7 + q) * 8 : (p * 7 + q) * 8 + 8, :]

    def add(i, j, value):
        start = (i * 32 + j) * 8
        at = pl.ds(start if isinstance(start, int) else pl.multiple_of(start, 8), 8)
        result[at, :] = result[at, :] + value

    def rows_of(j, columns):
        for base, mask, outs in ((0, top, (0, 1, 2)), (11, bottom, (5, 6, 7))):
            totals = {}
            for q in columns:
                for line in range(3):
                    value = padded[word(base + line, j + q), :] * mask
                    for i in outs:
                        p = base + line - i
                        if 0 <= p < 7:
                            term = value * tap_of(p, q)
                            totals[i] = term if i not in totals else totals[i] + term
            for i in outs:
                add(i, j, totals[i])

    def column(j, _):
        rows_of(j, range(7))
        return 0

    lax.fori_loop(3, 29, column, 0)
    for j in (0, 1, 2, 29, 30, 31):
        inner = [q for q in range(7) if 3 <= j + q < 35]
        rows_of(j, inner)
        totals = [None] * FRONT
        for q in range(7):
            if q in inner:
                continue
            values = [padded[word(i, j + q), :] for i in range(BACK)]
            for p in range(7):
                for i in range(FRONT):
                    term = values[i + p] * tap_of(p, q)
                    totals[i] = term if totals[i] is None else totals[i] + term
        for i in range(FRONT):
            add(i, j, totals[i])


def tap_grads(padded, upstream, small, base, columns):
    for q in columns:

        def column(j, totals):
            values = [padded[word(i, j + q), :] for i in range(BACK)]
            grads = [upstream[word(i + 3, j + 3), :] for i in range(FRONT)]
            result = []
            for p in range(7):
                total = totals[p]
                for i in range(FRONT):
                    total = total + values[i + p] * grads[i]
                result.append(total)
            return tuple(result)

        zero = jnp.zeros((8, 128), F32)
        totals = lax.fori_loop(0, 32, column, (zero,) * 7, unroll=4)
        for p in range(7):
            both = totals[p][:4] + totals[p][4:]
            for group in range(4):
                small[base + p * 7 + q : base + p * 7 + q + 1, group * 128 : group * 128 + 128] = both[
                    group : group + 1
                ]


def pixels(result, row):
    half, i = row // 8, row % 8
    return jnp.concatenate(
        [result[pl.ds(i * 256 + half * 4 + group, 32, stride=8), :] for group in range(4)], axis=1
    )


def dot(left, right, left_dim=1, right_dim=0):
    return lax.dot_general(
        left, right, (((left_dim,), (right_dim,)), ((), ())), preferred_element_type=F32
    )


def gelu_and_slope(values):
    square = values * values
    share = 0.5 + 0.5 * jnp.tanh(values * (COEF + (COEF * CUBIC) * square))
    value = values * share
    slope = share + value * (1.0 - share) * (2.0 * COEF + (6.0 * COEF * CUBIC) * square)
    return value, slope


CHUNK = 256


def step_kernel(
    slides, cotangent, kernel, kernel_bias, norm_gain, norm_bias, bias_out, layer_scale, bias_in,
    shard_in, shard_out,
    output_end, grad_slides_end, final_in_end, final_out_end, final_small_end,
    output, grad_slides, final_in, final_out, final_small, leave_sems,
    full_in, full_out, padded0, padded1, padded_g0, padded_g1, result, taps,
    normed, rstd, normal, turned, act, slope, hidden_grad, branch, carry, upstream, low,
    gm_tile, middle, grad_in, grad_out, small,
    *rest,
):
    me = Place()
    gather = Gather(me, shard_in, shard_out, full_in, full_out, rest[:5])
    padded = (padded0, padded1)
    padded_g = (padded_g0, padded_g1)
    tiles = (slides, middle)
    halos = [
        Halo(me, grid, tile, rest[5 + 6 * k : 11 + 6 * k])
        for k, (grid, tile) in enumerate(
            ((padded0, slides), (padded1, middle), (padded_g1, gm_tile.at[1]), (padded_g0, gm_tile.at[0]))
        )
    ]
    scratch = rest[30:]
    ways = {}
    for number, (kind, which, early) in enumerate(UNITS):
        bufs = scratch[number * 8 : number * 8 + 7]
        sems = scratch[number * 8 + 7]
        if kind is WeightIn:
            ends = (grad_in.at[which], final_in.at[which])
        else:
            ends = (grad_out.at[which], final_out.at[which])
        ways[kind, which] = Reduction(me, kind, early, *ends, bufs, sems)

    leaving = []

    def send_out(source, target):
        copy = pltpu.make_async_copy(source, target, leave_sems.at[len(leaving)])
        copy.start()
        leaving.append(copy)

    little = SmallReduction(me, small, final_small, scratch[-4:-1], scratch[-1])

    def reducing(which):
        return [ways[WeightOut, which], ways[WeightIn, which]]

    def line(which, ref):
        return ref[which : which + 1, :]

    for which in range(2):
        for kind in range(2):
            gather.place(which, kind).start()

    scope = jax.named_scope

    def fill(grid, tile):
        for r in range(16):
            put_row(grid, r + 3, 3, tile[r * 32 : r * 32 + 32, :].astype(F32))

    partners = [me.along("x", offset)[1] for offset in (1, 2, 3)]
    partners += [device for _, _, _, device in little.others()]
    around = [
        halos[0].target(down, right) for down in (-1, 0, 1) for right in (-1, 0, 1) if down
    ]
    with scope("p00a_fill"):
        padded0[...] = jnp.zeros_like(padded0)
        padded1[...] = jnp.zeros_like(padded1)
        fill(padded0, slides)
        for which in range(2):
            spread_taps(kernel, which, taps.at[which])
        small[...] = jnp.zeros_like(small)
        carry[...] = jnp.zeros_like(carry)
    with scope("p00b_meet"):
        meet(partners + around + [me.sibling()])
    with scope("p00c_start"):
        halos[0].start()
        gather.start(0, 0)
        gather.start(0, 1)
        gather.start(1, 0)

    def filter_map(which, first, last):
        depthwise(padded[which], taps.at[which], result, False, first, last)

    def normalise(which):
        for r in range(16):
            rows = slice(r * 32, r * 32 + 32)
            mixed = pixels(result, r) + line(which, kernel_bias)
            center = mixed - jnp.mean(mixed, -1, keepdims=True)
            inverse = lax.rsqrt(jnp.mean(center * center, -1, keepdims=True) + EPSILON)
            values = center * inverse
            normed[which, rows, :] = values
            rstd[which, rows, :] = jnp.broadcast_to(inverse, (32, 128))
            normal[which, rows, :] = (values * line(which, norm_gain) + line(which, norm_bias)).astype(BF)

    def expand(which, tilts, first=0, last=2048 // CHUNK):
        def chunk(c, _):
            cols = part(c * CHUNK, CHUNK)
            hidden = dot(normal[which], full_in[which, :, cols]) + bias_in[which : which + 1, cols]
            value, tilt = gelu_and_slope(hidden)
            act[which, :, cols] = value.astype(BF)
            if tilts is None:
                grads = dot(low[...], full_out[which, cols, :], 1, 1) * tilt
                keep_hidden_grad(which, c, cols, grads)
            else:
                tilts[:, cols] = tilt.astype(BF)
            return 0

        lax.fori_loop(first, last, chunk, 0)

    def hidden_grads(which, tilts, last):
        def chunk(c, _):
            cols = part(c * CHUNK, CHUNK)
            grads = dot(low[...], full_out[which, cols, :], 1, 1) * tilts[:, cols].astype(F32)
            keep_hidden_grad(which, c, cols, grads)
            return 0

        lax.fori_loop(0, last, chunk, 0)

    def keep_hidden_grad(which, c, cols, grads):
        hidden_grad[:, cols] = grads.astype(BF)
        bias_grad[which : which + 1, cols] = jnp.sum(grads, 0, keepdims=True)

    bias_grad = rest[29]

    def contract(which):
        def chunk(n, _):
            cols = part(n * CHUNK, CHUNK)
            branch[which, :, cols] = (
                dot(act[which], full_out[which, :, cols]) + bias_out[which : which + 1, cols]
            )
            return 0

        lax.fori_loop(0, 512 // CHUNK, chunk, 0)

    def residual(which, into):
        for r in range(16):
            rows = slice(r * 32, r * 32 + 32)
            value = tiles[which][rows, :].astype(F32) + line(which, layer_scale) * branch[which, rows, :]
            into[rows, :] = value.astype(BF)

    def enter(which, read):
        for r in range(16):
            rows = slice(r * 32, r * 32 + 32)
            grads = read(rows) * line(which, layer_scale)
            low[rows, :] = grads.astype(BF)
            add_rows(which, 0, grads)

    def add_rows(which, slot, values):
        total = values[0:8] + values[8:16] + (values[16:24] + values[24:32])
        carry[which, slot] = carry[which, slot] + total

    def weight_grads(which, first=0, last=2048 // CHUNK):
        def chunk(c, _):
            cols = part(c * CHUNK, CHUNK)
            grad_out[which, cols, :] = dot(act[which, :, cols], low[...], 0, 0).astype(BF)
            grad_in[which, :, cols] = dot(turned[...], hidden_grad[:, cols]).astype(BF)
            return 0

        if first == 0:
            turned[...] = normal[which].T
        lax.fori_loop(first, last, chunk, 0)

    def normal_grads(which, target):
        def chunk(n, _):
            rows = part(n * CHUNK, CHUNK)
            target[:, rows] = dot(hidden_grad[...], full_in[which, rows, :], 1, 1)
            return 0

        lax.fori_loop(0, 512 // CHUNK, chunk, 0)

    def leave(which, grads_ref):
        for r in range(16):
            rows = slice(r * 32, r * 32 + 32)
            grads = grads_ref[rows, :]
            values = normed[which, rows, :]
            add_rows(which, 2, grads)
            add_rows(which, 1, grads * values)
            scaled = grads * line(which, norm_gain)
            mean = jnp.mean(scaled, -1, keepdims=True)
            tilt = jnp.mean(scaled * values, -1, keepdims=True)
            mixed = (scaled - mean - values * tilt) * rstd[which, rows, 0:1]
            add_rows(which, 3, mixed)
            put_row(padded_g[which], r + 3, 3, mixed)
            gm_tile[which, rows, :] = mixed.astype(BF)

    def scale_grad(which, read):
        for r in range(16):
            rows = slice(r * 32, r * 32 + 32)
            add_rows(which, 4, read(rows) * branch[which, rows, :])

    def settle(which):
        for slot, row in ((3, 0), (1, 1), (2, 2), (0, 3), (4, 4)):
            at = which * 64 + 49 + row
            small[at : at + 1, :] = jnp.sum(carry[which, slot], 0, keepdims=True)
        for c in range(4):
            at = which * 64 + 54 + c
            small[at : at + 1, :] = bias_grad[which : which + 1, c * 512 : c * 512 + 512]

    def from_cotangent(rows):
        return cotangent[rows, :].astype(F32)

    def from_upstream(rows):
        return upstream[rows, :]

    with scope("p01_depth0"):
        enter(1, from_cotangent)
        filter_map(0, 0, 32)
    with scope("p01_halo0"):
        halos[0].finish()
    with scope("p01_rim0"):
        add_rim(padded0, taps.at[0], result)
    with scope("p02_forward_in0"):
        gather.forward(0, 0)
    with scope("p03_norm0"):
        normalise(0)
    with scope("p04_finish_in0"):
        gather.finish(0, 0)
    with scope("p05_expand0"):
        expand(0, slope, 0, 5)
    with scope("p05_forward_out0"):
        gather.forward(0, 1)
    with scope("p05_expand0b"):
        expand(0, slope, 5)
    with scope("p06_finish_out0"):
        gather.finish(0, 1)
    with scope("p06_contract0"):
        contract(0)
        residual(0, middle)
        fill(padded1, middle)
    with scope("p07_halo1"):
        halos[1].start()
        gather.start(1, 1)
        gather.forward(1, 0)
    with scope("p08_depth1"):
        filter_map(1, 0, 32)
    with scope("p08_halo1_end"):
        halos[1].finish()
    with scope("p09_norm1"):
        add_rim(padded1, taps.at[1], result)
        normalise(1)
    with scope("p09_finish_in1"):
        gather.finish(1, 0)
    with scope("p10_expand1"):
        expand(1, hidden_grad, 0, 2)
    with scope("p10_forward_out1"):
        gather.forward(1, 1)
    with scope("p10_expand1b"):
        expand(1, hidden_grad, 2, 4)
    with scope("p10_finish_out1"):
        gather.finish(1, 1)
    with scope("p11_expand1"):
        expand(1, None, 4)
        hidden_grads(1, hidden_grad, 4)
    with scope("p12_ngrads1"):
        normal_grads(1, upstream)
    with scope("p13_leave1"):
        leave(1, upstream)
        halos[2].start()
    out1, in1 = reducing(1)
    out0, in0 = reducing(0)

    def go(name, *group):
        with scope(name):
            for way in group:
                way.advance()

    with scope("p14_wgrads1"):
        weight_grads(1)
        out1.advance()
        in1.advance()
    with scope("p16_halo2_end"):
        halos[2].finish()
    with scope("p17_depth1"):
        depthwise(padded_g1, taps.at[1], result, True, 0, 10)
    go("p17_go1", out1, in1)
    with scope("p17_depth1b"):
        depthwise(padded_g1, taps.at[1], result, True, 10, 32)
        for r in range(16):
            rows = slice(r * 32, r * 32 + 32)
            upstream[rows, :] = from_cotangent(rows) + pixels(result, r)
    with scope("p18_enter0"):
        enter(0, from_upstream)
        scale_grad(0, from_upstream)

    with scope("p19_hidden0"):
        hidden_grads(0, slope, 2048 // CHUNK)
    with scope("p21_wgrads0"):
        weight_grads(0, 0, 4)
    go("p21_go1", out1, in1)
    with scope("p21_wgrads0b"):
        weight_grads(0, 4)
    in0.advance()
    out0.advance()
    with scope("p23_ngrads0"):
        normal_grads(0, normed.at[1])
    go("p23_go1", out1)
    go("p23_go0", in0)
    with scope("p24_leave0"):
        leave(0, normed.at[1])
        halos[3].start()
    go("p25_go1", in1)
    go("p25_go0", out0)
    with scope("p26_contract1"):
        contract(1)
        residual(1, output)
        send_out(output, output_end)
        scale_grad(1, from_cotangent)
        settle(1)
        settle(0)
    with scope("p28_taps0"):
        tap_grads(padded0, padded_g0, small, 0, range(7))
    go("p29_go0", in0)
    go("p29_go1", in1, out1)
    with scope("p29_taps1"):
        tap_grads(padded1, padded_g1, small, 64, range(4))
    go("p29b_go0", out0)
    with scope("p29_taps1b"):
        tap_grads(padded1, padded_g1, small, 64, range(4, 7))
    little.advance()
    go("p30_go0", in0)
    go("p30_go0b", out0)
    go("p30_go1", out1, in1)
    with scope("p30_halo3_end"):
        halos[3].finish()
    with scope("p31_depth0"):
        depthwise(padded_g0, taps.at[0], result, True, 0, 16)
    go("p31_go", little, in0, out0, in1)
    with scope("p33_depth0"):
        depthwise(padded_g0, taps.at[0], result, True, 16, 32)
    go("p33_go", in0, little, out0, out1)
    with scope("p33_depth0b"):
        for r in range(16):
            rows = slice(r * 32, r * 32 + 32)
            grad_slides[rows, :] = (upstream[rows, :] + pixels(result, r)).astype(BF)
        send_out(grad_slides, grad_slides_end)
    go("p34_go", in0, little, in1)
    go("p35_go", in0, little, out0)
    every = [out1, in1, little, out0, in0]
    with scope("p38_rest"):
        while any(way.steps for way in every):
            for way in every:
                if way.steps:
                    way.advance()
    with scope("p39_drain"):
        for which in (1, 0):
            send_out(final_in.at[which], final_in_end.at[which])
            send_out(final_out.at[which], final_out_end.at[which])
        send_out(final_small, final_small_end)
        for way in every + halos + [gather]:
            way.drain()
        for copy in leaving:
            copy.wait()


def halo_scratch():
    return [
        pltpu.VMEM((2, 96, 512), BF),
        pltpu.VMEM((2, 192, 128), BF),
        pltpu.VMEM((2, 192, 128), BF),
        pltpu.VMEM((2, 2, 80, 128), BF),
        pltpu.VMEM((2, 2, 80, 128), BF),
        pltpu.SemaphoreType.DMA((2, 8)),
    ]


def whole_step(*operands):
    vmem = pl.BlockSpec(memory_space=pltpu.VMEM)
    grid = pltpu.VMEM((BACK * SPAN * 8, 128), F32)
    scratch = [
        pltpu.VMEM((512, 512), BF),
        pltpu.VMEM((512, 512), BF),
        pltpu.VMEM((2, 256, 2048), BF),
        pltpu.VMEM((2, 2048, 256), BF),
        pltpu.VMEM((128, 512), F32),
        pltpu.SemaphoreType.DMA((7,)),
        pltpu.VMEM((2, 512, 2048), BF),
        pltpu.VMEM((2, 2048, 512), BF),
        grid,
        grid,
        grid,
        grid,
        pltpu.VMEM((8 * 32 * 8, 128), F32),
        pltpu.VMEM((2, 49 * 8, 128), F32),
        pltpu.VMEM((2, 512, 512), F32),
        pltpu.VMEM((2, 512, 128), F32),
        pltpu.VMEM((2, 512, 512), BF),
        pltpu.VMEM((512, 512), BF),
        pltpu.VMEM((2, 512, 2048), BF),
        pltpu.VMEM((512, 2048), BF),
        pltpu.VMEM((512, 2048), BF),
        pltpu.VMEM((2, 512, 512), F32),
        pltpu.VMEM((2, 5, 8, 512), F32),
        pltpu.VMEM((512, 512), F32),
        pltpu.VMEM((512, 512), BF),
        pltpu.VMEM((2, 512, 512), BF),
        pltpu.VMEM((512, 512), BF),
        pltpu.VMEM((2, 512, 2048), BF),
        pltpu.VMEM((2, 2048, 512), BF),
        pltpu.VMEM((128, 512), F32),
    ]
    scratch += [pltpu.SemaphoreType.DMA((2, 2))]
    scratch += [pltpu.SemaphoreType.DMA((2, 2, 2)) for _ in range(4)]
    for _ in range(4):
        scratch += halo_scratch()
    extra = [pltpu.VMEM((2, 2048), F32)]
    reductions = sum([reduction_scratch(kind, early) for kind, _, early in UNITS], [])
    reductions += [
        pltpu.VMEM((64, 512), F32),
        pltpu.VMEM((16, 16, 128), F32),
        pltpu.VMEM((4, 16, 128), F32),
        pltpu.SemaphoreType.DMA((2, 64)),
    ]
    return pl.pallas_call(
        step_kernel,
        out_shape=(
            jax.ShapeDtypeStruct((512, 512), BF),
            jax.ShapeDtypeStruct((512, 512), BF),
            jax.ShapeDtypeStruct((2, 256, 2048), BF),
            jax.ShapeDtypeStruct((2, 2048, 256), BF),
            jax.ShapeDtypeStruct((128, 512), F32),
        ),
        in_specs=[vmem] * 9 + [pl.BlockSpec(memory_space=pl.ANY)] * 2,
        out_specs=[pl.BlockSpec(memory_space=pl.ANY)] * 5,
        scratch_shapes=scratch + extra + reductions,
        compiler_params=pltpu.CompilerParams(
            collective_id=0, has_side_effects=True, vmem_limit_bytes=67043328
        ),
        name="whole_step",
    )(*operands)


def unpack_kernel(
    output, grad_slides, total_in, total_out, small,
    output_end, slides_end, in_end, out_end, kernel_end, channel_end, bias_end,
    maps, low_in, low_out, wide_in, wide_out, get, put,
):
    steps = []
    for which in range(2):
        for cut in range(4):
            for ends, size in (
                ((total_in, low_in, wide_in, in_end), 64),
                ((total_out, low_out, wide_out, out_end), 512),
            ):
                steps.append([ref.at[which, pl.ds(cut * size, size), :] for ref in ends])
    steps.append([output, maps.at[0], maps.at[0], output_end])
    steps.append([grad_slides, maps.at[1], maps.at[1], slides_end])
    for number, (src, low, _, _) in enumerate(steps):
        pltpu.make_async_copy(src, low, get.at[number]).start()
    for number, (src, low, wide, dst) in enumerate(steps):
        pltpu.make_async_copy(src, low, get.at[number]).wait()
        if number < 16:
            wide[...] = low[...].astype(F32)
        pltpu.make_async_copy(wide, dst, put.at[number]).start()
    for which in range(2):
        base = which * 64
        for p in range(7):
            kernel_end[p, :, which, :] = small[base + p * 7 : base + p * 7 + 7, :]
        channel_end[:, which, :] = small[base + 49 : base + 54, :]
        for c in range(4):
            bias_end[which : which + 1, c * 512 : c * 512 + 512] = small[
                base + 54 + c : base + 55 + c, :
            ]
    for number, (_, _, wide, dst) in enumerate(steps):
        pltpu.make_async_copy(wide, dst, put.at[number]).wait()


def unpack(*results):
    vmem = pl.BlockSpec(memory_space=pltpu.VMEM)
    hbm = pl.BlockSpec(memory_space=pl.ANY)
    return pl.pallas_call(
        unpack_kernel,
        out_shape=(
            jax.ShapeDtypeStruct((512, 512), BF),
            jax.ShapeDtypeStruct((512, 512), BF),
            jax.ShapeDtypeStruct((2, 256, 2048), F32),
            jax.ShapeDtypeStruct((2, 2048, 256), F32),
            jax.ShapeDtypeStruct((7, 7, 2, 512), F32),
            jax.ShapeDtypeStruct((5, 2, 512), F32),
            jax.ShapeDtypeStruct((2, 2048), F32),
        ),
        in_specs=[hbm] * 4 + [vmem],
        out_specs=[hbm] * 4 + [vmem] * 3,
        scratch_shapes=[
            pltpu.VMEM((2, 512, 512), BF),
            pltpu.VMEM((2, 256, 2048), BF),
            pltpu.VMEM((2, 2048, 256), BF),
            pltpu.VMEM((2, 256, 2048), F32),
            pltpu.VMEM((2, 2048, 256), F32),
            pltpu.SemaphoreType.DMA((18,)),
            pltpu.SemaphoreType.DMA((18,)),
        ],
        compiler_params=pltpu.CompilerParams(vmem_limit_bytes=67043328),
        name="unpack",
    )(*results)


def per_device(
    slides,
    cotangent,
    kernel,
    kernel_bias,
    norm_gain,
    norm_bias,
    weight_in,
    bias_in,
    weight_out,
    bias_out,
    layer_scale,
):
    channels = slides.shape[-1]
    results = whole_step(
        slides.reshape(-1, channels),
        cotangent.reshape(-1, channels),
        kernel.transpose(1, 2, 0, 3),
        kernel_bias,
        norm_gain,
        norm_bias,
        bias_out,
        layer_scale,
        bias_in,
        weight_in,
        weight_out,
    )
    output, grad_slides, total_in, total_out, taps, sums, biases = unpack(*results)
    return (
        output.reshape(slides.shape),
        grad_slides.reshape(slides.shape),
        total_in,
        total_out,
        taps.transpose(2, 0, 1, 3),
        sums.transpose(1, 0, 2),
        biases,
    )


def solution(mesh):
    whole = P("dp", "row", "col", None)
    return jax.shard_map(
        per_device,
        mesh=mesh,
        in_specs=(whole, whole) + (P(),) * 4 + (P(None, "dp", None), P(), P(None, None, "dp"), P(), P()),
        out_specs=(whole, whole, P(None, "dp", None), P(None, None, "dp"), P(), P(), P()),
        check_vma=False,
    )
```

```python
import functools

import jax
import jax.numpy as jnp
from jax import lax
from jax.experimental import pallas as pl
from jax.experimental.pallas import tpu as pltpu
from jax.sharding import PartitionSpec as P

COEF = 0.7978845608028654
CUBIC = 0.044715
EPSILON = 1e-06

MESH = pl.DeviceIdType.MESH
BF = jnp.bfloat16
F32 = jnp.float32


class Place:
    def __init__(self):
        row = lax.axis_index("row")
        self.z = lax.axis_index("col")
        self.half = lax.axis_index("dp")
        self.core = lax.rem(row, 2)
        self.y = lax.rem(lax.div(row, 2), 4)
        self.x = lax.div(row, 8) * 2 + self.half

    def device(self, x=None, y=None, z=None, core=None):
        x = self.x if x is None else x
        y = self.y if y is None else y
        z = self.z if z is None else z
        core = self.core if core is None else core
        return {"row": (lax.div(x, 2) * 4 + y) * 2 + core, "col": z, "dp": lax.rem(x, 2)}

    def along(self, axis, offset):
        value = lax.rem(getattr(self, axis) + offset, 4)
        return value, self.device(**{axis: value})

    def sibling(self):
        return self.device(core=1 - self.core)


def meet(partners):
    barrier = pltpu.get_barrier_semaphore()
    for partner in partners:
        pl.semaphore_signal(barrier, inc=1, device_id=partner, device_id_type=MESH)
    pl.semaphore_wait(barrier, len(partners))


def part(start, size):
    if isinstance(start, int):
        return pl.ds(start, size)
    return pl.ds(pl.multiple_of(start, size), size)


def remote(src, dst, send, recv, target):
    return pltpu.make_async_remote_copy(
        src_ref=src, dst_ref=dst, send_sem=send, recv_sem=recv, device_id=target, device_id_type=MESH
    )


ORDERS = (("y", "z"), ("z", "y"))


class WeightIn:
    received = (128, 2048)
    turn = (64, 2048)
    first = (64, 512)
    second = (64, 128)
    third = (64, 128)

    def offered(grad, half, core):
        return grad.at[part(half * 256 + core * 128, 128), :]

    def cut(got, halves, turn, index):
        return got.at[halves, turn * 64 : turn * 64 + 64, part(index * 512, 512)]

    def cut_again(block, index):
        return block.at[:, :, part(index * 128, 128)]

    def placed(final, core, turn, one, two):
        return final.at[part(core * 128 + turn * 64, 64), part(one * 512 + two * 128, 128)]

    def line(final, core, turn, one):
        return final.at[part(core * 128 + turn * 64, 64), part(one * 512, 512)]

    def of_core(final, core):
        return final.at[part(core * 128, 128), :]


class WeightOut:
    received = (2048, 128)
    turn = (1024, 128)
    first = (256, 128)
    second = (64, 128)
    third = (64, 128)

    def offered(grad, half, core):
        return grad.at[:, part(half * 256 + core * 128, 128)]

    def cut(got, halves, turn, index):
        return got.at[halves, part(turn * 1024 + index * 256, 256), :]

    def cut_again(block, index):
        return block.at[:, part(index * 64, 64), :]

    def placed(final, core, turn, one, two):
        return final.at[part(turn * 1024 + one * 256 + two * 64, 64), part(core * 128, 128)]

    def line(final, core, turn, one):
        return final.at[part(turn * 1024 + one * 256, 256), part(core * 128, 128)]

    def of_core(final, core):
        return final.at[:, part(core * 128, 128)]


class Reduction:
    def __init__(self, me, kind, early, grad, final, bufs, sems):
        self.me, self.kind, self.early, self.grad, self.final = me, kind, early, grad, final
        self.got, self.given, self.r1, self.b1, self.r2, self.b2, self.r3 = bufs
        self.sems = sems
        self.copies = []
        self.steps = [
            [self.core_start],
            [self.core_finish, lambda: self.split_start(0)],
            [lambda: self.split_finish(0), lambda: self.split_start(1)],
            [lambda: self.split_finish(1), self.across_start],
            [self.across_finish, lambda: self.join_start(1)],
            [lambda: self.join_finish(1), lambda: self.join_start(0)],
            [lambda: self.join_finish(0), self.share_start],
            [self.share_finish],
        ]
        if early:
            self.steps[1:2] = [
                [self.core_finish, self.give_start],
                [self.give_finish, lambda: self.split_start(0)],
            ]

    def advance(self):
        for action in self.steps.pop(0):
            action()

    def sem(self, way, turn, step, slot):
        return self.sems.at[way, (turn * 8 + step) * 4 + slot]

    def go(self, src, dst, turn, step, send_slot, recv_slot, target):
        copy = remote(
            src, dst, self.sem(0, turn, step, send_slot), self.sem(1, turn, step, recv_slot), target
        )
        copy.start()
        self.copies.append(copy)

    def landed(self, dst, turn, step, slot):
        remote(
            dst, dst, self.sem(0, turn, step, slot), self.sem(1, turn, step, slot), self.me.sibling()
        ).wait_recv()

    def core_start(self):
        for half in range(2):
            src = self.kind.offered(self.grad, half, 1 - self.me.core)
            self.go(src, self.got.at[half], 0, 0, half, half, self.me.sibling())

    def core_finish(self):
        for half in range(2):
            self.landed(self.got.at[half], 0, 0, half)
            own = self.kind.offered(self.grad, half, self.me.core)
            total = own[...].astype(F32) + self.got[half].astype(F32)
            self.got[half] = total.astype(self.got.dtype)

    def block(self, turn, step, index):
        if step == 0:
            halves = pl.ds(self.me.half, 1) if self.early else slice(None)
            return self.kind.cut(self.got, halves, turn, index)
        return self.kind.cut_again(self.b1.at[turn], index)

    def split_start(self, step):
        target = (self.r1, self.r2)[step]
        for turn in range(2):
            for offset in (1, 3, 2):
                index, device = self.me.along(ORDERS[turn][step], offset)
                self.go(
                    self.block(turn, step, index),
                    target.at[turn, offset - 1],
                    turn,
                    1 + step,
                    offset,
                    offset,
                    device,
                )

    def split_finish(self, step):
        target, result = ((self.r1, self.b1), (self.r2, self.b2))[step]
        for turn in range(2):
            index = getattr(self.me, ORDERS[turn][step])
            total = self.block(turn, step, index)[...].astype(F32)
            for offset in (1, 3, 2):
                self.landed(target.at[turn, offset - 1], turn, 1 + step, offset)
                total = total + target[turn, offset - 1].astype(F32)
            result[turn] = total.astype(result.dtype)

    def turn_rows(self, half, turn):
        size = self.kind.turn[0]
        return self.got.at[half, turn * size : turn * size + size, :]

    def give_start(self):
        for turn, offset in ((0, 1), (1, 3)):
            _, device = self.me.along("x", offset)
            src = self.turn_rows(1 - self.me.half, turn)
            self.go(src, self.given.at[turn], turn, 7, 0, 0, device)

    def give_finish(self):
        for turn in range(2):
            self.landed(self.given.at[turn], turn, 7, 0)
            own = self.turn_rows(self.me.half, turn)
            total = own[...].astype(F32) + self.given[turn].astype(F32)
            own[...] = total.astype(self.got.dtype)

    def across_start(self):
        for turn in range(2):
            block = self.b2.at[turn]
            if self.early:
                _, device = self.me.along("x", 2)
                self.go(block.at[0], self.r3.at[turn, 0], turn, 3, 0, 0, device)
                continue
            for offset in (1, 3, 2):
                index, device = self.me.along("x", offset)
                src = block.at[lax.rem(index, 2)]
                self.go(src, self.r3.at[turn, self.me.x], turn, 3, offset, self.me.x, device)
            self.r3[turn, self.me.x] = block[self.me.half]

    def across_finish(self):
        me = self.me
        for turn in range(2):
            if self.early:
                self.landed(self.r3.at[turn, 0], turn, 3, 0)
                total = self.b2[turn, 0].astype(F32) + self.r3[turn, 0].astype(F32)
            else:
                for offset in (1, 3, 2):
                    index, _ = me.along("x", offset)
                    self.landed(self.r3.at[turn, index], turn, 3, index)
                total = self.r3[turn, 0].astype(F32)
                for index in range(1, 4):
                    total = total + self.r3[turn, index].astype(F32)
            one, two = (getattr(me, axis) for axis in ORDERS[turn])
            block = self.kind.placed(self.final, me.core, turn, one, two)
            block[...] = total.astype(self.final.dtype)

    def join_start(self, step):
        me = self.me
        for turn in range(2):
            one, two = (getattr(me, axis) for axis in ORDERS[turn])
            for offset in (1, 3, 2):
                _, device = me.along(ORDERS[turn][step], offset)
                if step == 1:
                    block = self.kind.placed(self.final, me.core, turn, one, two)
                else:
                    block = self.kind.line(self.final, me.core, turn, one)
                self.go(block, block, turn, 5 - step, offset, offset, device)

    def join_finish(self, step):
        me = self.me
        for turn in range(2):
            one, two = (getattr(me, axis) for axis in ORDERS[turn])
            for offset in (1, 3, 2):
                source = lax.rem((two if step == 1 else one) + 4 - offset, 4)
                if step == 1:
                    block = self.kind.placed(self.final, me.core, turn, one, source)
                else:
                    block = self.kind.line(self.final, me.core, turn, source)
                self.landed(block, turn, 5 - step, offset)

    def share_start(self):
        block = self.kind.of_core(self.final, self.me.core)
        self.go(block, block, 0, 6, 0, 0, self.me.sibling())

    def share_finish(self):
        block = self.kind.of_core(self.final, 1 - self.me.core)
        self.landed(block, 0, 6, 0)

    def drain(self):
        for copy in self.copies:
            copy.wait_send()


class SmallReduction:
    def __init__(self, me, grad, final, bufs, sems):
        self.me, self.grad, self.final = me, grad, final
        self.got, self.parts, self.lines = bufs
        self.sems = sems
        self.copies = []
        self.steps = [
            self.core_start,
            self.plane_start,
            self.across_start,
            self.join_start,
            self.share_start,
            self.share_finish,
        ]

    def advance(self):
        self.steps.pop(0)()

    def drain(self):
        for copy in self.copies:
            copy.wait_send()

    def go(self, src, dst, slot, target):
        copy = remote(src, dst, self.sems.at[0, slot], self.sems.at[1, slot], target)
        copy.start()
        self.copies.append(copy)

    def landed(self, dst, slot):
        target = self.me.sibling()
        remote(dst, dst, self.sems.at[0, slot], self.sems.at[1, slot], target).wait_recv()

    def others(self):
        for up in range(4):
            for deep in range(4):
                if up or deep:
                    y = lax.rem(self.me.y + up, 4)
                    z = lax.rem(self.me.z + deep, 4)
                    yield up * 4 + deep, y, z, self.me.device(y=y, z=z)

    def cell(self, ref, row, y, z):
        return ref.at[part(row + y * 16, 16), part(z * 128, 128)]

    def core_start(self):
        src = self.grad.at[part((1 - self.me.core) * 64, 64), :]
        self.go(src, self.got, 0, self.me.sibling())

    def plane_start(self):
        self.landed(self.got, 0)
        own = self.grad[part(self.me.core * 64, 64), :]
        self.got[...] = own + self.got[...]
        for slot, y, z, device in self.others():
            self.go(self.cell(self.got, 0, y, z), self.parts.at[slot], slot, device)

    def across_start(self):
        me = self.me
        total = self.cell(self.got, 0, me.y, me.z)[...]
        for slot, _, _, _ in self.others():
            self.landed(self.parts.at[slot], slot)
            total = total + self.parts[slot]
        self.lines[me.x] = total
        for offset in (1, 3, 2):
            _, device = me.along("x", offset)
            copy = remote(
                self.lines.at[me.x],
                self.lines.at[me.x],
                self.sems.at[0, 15 + offset],
                self.sems.at[1, 32 + me.x],
                device,
            )
            copy.start()
            self.copies.append(copy)

    def join_start(self):
        me = self.me
        for offset in (1, 3, 2):
            index, _ = me.along("x", offset)
            self.landed(self.lines.at[index], 32 + index)
        total = self.lines[0] + self.lines[1] + (self.lines[2] + self.lines[3])
        block = self.cell(self.final, me.core * 64, me.y, me.z)
        block[...] = total
        for slot, _, _, device in self.others():
            self.go(block, block, 40 + slot, device)

    def share_start(self):
        me = self.me
        for slot, _, _, _ in self.others():
            y = lax.rem(me.y + 4 - slot // 4, 4)
            z = lax.rem(me.z + 4 - slot % 4, 4)
            self.landed(self.cell(self.final, me.core * 64, y, z), 40 + slot)
        block = self.final.at[part(me.core * 64, 64), :]
        self.go(block, block, 60, me.sibling())

    def share_finish(self):
        block = self.final.at[part((1 - self.me.core) * 64, 64), :]
        self.landed(block, 60)


def reduction_scratch(kind, early):
    halves = 1 if early else 2
    return [
        pltpu.VMEM((2, *kind.received), BF),
        pltpu.VMEM((2, *kind.turn) if early else (2, 8, 128), BF),
        pltpu.VMEM((2, 3, halves, *kind.first), BF),
        pltpu.VMEM((2, halves, *kind.first), BF),
        pltpu.VMEM((2, 3, halves, *kind.second), BF),
        pltpu.VMEM((2, halves, *kind.second), BF),
        pltpu.VMEM((2, 4, *kind.third), BF),
        pltpu.SemaphoreType.DMA((2, 64)),
    ]


UNITS = (
    (WeightOut, 1, False),
    (WeightIn, 1, True),
    (WeightOut, 0, False),
    (WeightIn, 0, True),
)


class Gather:
    def __init__(self, me, shard_in, shard_out, full_in, full_out, sems):
        self.me = me
        self.shards = (shard_in, shard_out)
        self.full = (full_in, full_out)
        self.local, self.send, self.recv, self.send_core, self.recv_core = sems
        self.sides = (me.along("x", 1)[1], me.along("x", 3)[1])
        self.copies = []

    def block(self, which, kind, half, core, side):
        full = self.full[kind].at[which]
        if kind == 0:
            return full.at[part(half * 256 + core * 128 + side * 64, 64), :]
        return full.at[part(core * 1024 + side * 512, 512), part(half * 256, 256)]

    def place(self, which, kind):
        half = part(self.me.half * 256, 256)
        full = self.full[kind].at[which]
        own = full.at[half, :] if kind == 0 else full.at[:, half]
        return pltpu.make_async_copy(self.shards[kind].at[which], own, self.local.at[which, kind])

    def hop(self, which, kind, half, core, side, across):
        block = self.block(which, kind, half, core, side)
        if across:
            sems, target = (self.send, self.recv), self.sides[side]
        else:
            sems, target = (self.send_core, self.recv_core), self.me.sibling()
        return remote(block, block, *(s.at[which, kind, side] for s in sems), target)

    def start(self, which, kind):
        self.place(which, kind).wait()
        for side in range(2):
            copy = self.hop(which, kind, self.me.half, self.me.core, side, True)
            copy.start()
            self.copies.append(copy)

    def forward(self, which, kind):
        other = 1 - self.me.half
        for side in range(2):
            self.hop(which, kind, other, self.me.core, side, True).wait_recv()
            copy = self.hop(which, kind, other, self.me.core, side, False)
            copy.start()
            self.copies.append(copy)

    def finish(self, which, kind):
        for side in range(2):
            self.hop(which, kind, 1 - self.me.half, 1 - self.me.core, side, False).wait_recv()

    def drain(self):
        for copy in self.copies:
            copy.wait_send()


SPAN = 38
BACK, FRONT = 14, 8


def word(i, j):
    start = (i * SPAN + j) * 8
    return pl.ds(start if isinstance(start, int) else pl.multiple_of(start, 8), 8)


def put_row(padded, row, first, values, halves=(0, 1)):
    for half in halves:
        i = row - 8 * half
        if 0 <= i < BACK:
            for group in range(4):
                padded[pl.ds((i * SPAN + first) * 8 + half * 4 + group, values.shape[0], stride=8), :] = (
                    values[:, group * 128 : group * 128 + 128]
                )


def rolled(values):
    return jnp.concatenate([values[4:], values[:4]], axis=0)


class Halo:
    def __init__(self, me, padded, tile, bufs):
        self.me, self.padded, self.tile = me, padded, tile
        self.rows, self.side_out, self.sides, self.corner_out, self.corners, self.sems = bufs
        self.copies = []
        self.row = (lax.div(me.x, 2) * 4 + me.y) * 2 + me.core

    def target(self, down, right):
        row = lax.rem(self.row + down + 16, 16)
        col = lax.rem(self.me.z + right + 4, 4)
        return {"row": row, "col": col, "dp": self.me.half}

    def messages(self):
        tile = self.tile
        yield tile.at[pl.ds(0, 96), :], self.rows.at[1], (-1, 0)
        yield tile.at[pl.ds(416, 96), :], self.rows.at[0], (1, 0)
        for side in range(2):
            yield self.side_out.at[side], self.sides.at[1 - side], (0, 2 * side - 1)
        for low in range(2):
            for side in range(2):
                yield (
                    self.corner_out.at[low, side],
                    self.corners.at[1 - low, 1 - side],
                    (2 * low - 1, 2 * side - 1),
                )

    def start(self):
        padded = self.padded
        for side, first in ((0, 3), (1, 32)):
            for j in range(3):
                lines = [padded[word(i, first + j), :] for i in range(3, 11)]
                self.side_out[side, j * 64 : j * 64 + 64, :] = jnp.concatenate(lines, 0).astype(BF)
            for low, top in ((0, 3), (1, 8)):
                lines = [
                    rolled(padded[word(top + i, first + j), :]) for i in range(3) for j in range(3)
                ]
                self.corner_out[low, side] = jnp.concatenate(lines + lines[:1], 0).astype(BF)
        for number, (src, dst, (down, right)) in enumerate(self.messages()):
            copy = remote(
                src, dst, self.sems.at[0, number], self.sems.at[1, number], self.target(down, right)
            )
            copy.start()
            self.copies.append(copy)

    def finish(self):
        padded = self.padded
        for number, (src, dst, _) in enumerate(self.messages()):
            remote(
                src, dst, self.sems.at[0, number], self.sems.at[1, number], self.target(1, 0)
            ).wait_recv()
        inside = [
            (self.row > 0).astype(F32),
            (self.row < 15).astype(F32),
        ]
        across = [
            (self.me.z > 0).astype(F32),
            (self.me.z < 3).astype(F32),
        ]
        for low in range(2):
            for r in range(3):
                values = self.rows[low, r * 32 : r * 32 + 32, :].astype(F32) * inside[low]
                put_row(padded, r + 19 * low, 3, values, (low,))
        for side, first in ((0, 0), (1, 35)):
            for j in range(3):
                lines = self.sides[side, j * 64 : j * 64 + 64, :].astype(F32) * across[side]
                for m in range(8):
                    line = lines[m * 8 : m * 8 + 8]
                    padded[word(m + 3, first + j), :] = line
                    at = first + j
                    if m >= 5:
                        padded[pl.ds(((m - 5) * SPAN + at) * 8 + 4, 4), :] = line[:4]
                    if m < 3:
                        padded[pl.ds(((m + 11) * SPAN + at) * 8, 4), :] = line[4:]
            for low in range(2):
                lines = self.corners[low, side].astype(F32) * (inside[low] * across[side])
                for i in range(3):
                    for j in range(3):
                        line = lines[(i * 3 + j) * 8 : (i * 3 + j) * 8 + 8]
                        start = ((i + 11 * low) * SPAN + first + j) * 8 + 4 * low
                        padded[pl.ds(start, 4), :] = line[4 * low : 4 * low + 4]

    def drain(self):
        for copy in self.copies:
            copy.wait_send()


def spread_taps(kernel, which, taps):
    for p in range(7):
        for group in range(4):
            values = kernel[p, :, which, group * 128 : group * 128 + 128]
            for half in range(2):
                taps[pl.ds(p * 56 + half * 4 + group, 7, stride=8), :] = values


def depthwise(padded, taps, result, flipped, first=0, last=32):
    def columns(pair, _):
        j = pair * 2
        totals = [[None] * FRONT for _ in range(2)]
        for c in range(8):
            values = [padded[word(i, j + c), :] for i in range(BACK)]
            for side in range(2):
                q = c - side
                if not 0 <= q < 7:
                    continue
                total = totals[side]
                for p in range(7):
                    number = (6 - p) * 7 + 6 - q if flipped else p * 7 + q
                    tap = taps[number * 8 : number * 8 + 8, :]
                    for i in range(FRONT):
                        term = values[i + p] * tap
                        total[i] = term if total[i] is None else total[i] + term
        for side in range(2):
            for i in range(FRONT):
                result[pl.ds(pl.multiple_of((i * 32 + j + side) * 8, 8), 8), :] = totals[side][i]
        return 0

    lax.fori_loop(first // 2, last // 2, columns, 0)


def add_rim(padded, taps, result):
    place = lax.broadcasted_iota(jnp.int32, (8, 128), 0)
    top = jnp.where(place < 4, 1.0, 0.0).astype(F32)
    bottom = 1.0 - top

    def tap_of(p, q):
        return taps[(p * 7 + q) * 8 : (p * 7 + q) * 8 + 8, :]

    def add(i, j, value):
        start = (i * 32 + j) * 8
        at = pl.ds(start if isinstance(start, int) else pl.multiple_of(start, 8), 8)
        result[at, :] = result[at, :] + value

    def rows_of(j, columns):
        for base, mask, outs in ((0, top, (0, 1, 2)), (11, bottom, (5, 6, 7))):
            totals = {}
            for q in columns:
                for line in range(3):
                    value = padded[word(base + line, j + q), :] * mask
                    for i in outs:
                        p = base + line - i
                        if 0 <= p < 7:
                            term = value * tap_of(p, q)
                            totals[i] = term if i not in totals else totals[i] + term
            for i in outs:
                add(i, j, totals[i])

    def column(j, _):
        rows_of(j, range(7))
        return 0

    lax.fori_loop(3, 29, column, 0)
    for j in (0, 1, 2, 29, 30, 31):
        inner = [q for q in range(7) if 3 <= j + q < 35]
        rows_of(j, inner)
        totals = [None] * FRONT
        for q in range(7):
            if q in inner:
                continue
            values = [padded[word(i, j + q), :] for i in range(BACK)]
            for p in range(7):
                for i in range(FRONT):
                    term = values[i + p] * tap_of(p, q)
                    totals[i] = term if totals[i] is None else totals[i] + term
        for i in range(FRONT):
            add(i, j, totals[i])


def tap_grads(padded, upstream, small, base, columns):
    for q in columns:

        def column(j, totals):
            values = [padded[word(i, j + q), :] for i in range(BACK)]
            grads = [upstream[word(i + 3, j + 3), :] for i in range(FRONT)]
            result = []
            for p in range(7):
                total = totals[p]
                for i in range(FRONT):
                    total = total + values[i + p] * grads[i]
                result.append(total)
            return tuple(result)

        zero = jnp.zeros((8, 128), F32)
        totals = lax.fori_loop(0, 32, column, (zero,) * 7, unroll=4)
        for p in range(7):
            both = totals[p][:4] + totals[p][4:]
            for group in range(4):
                small[base + p * 7 + q : base + p * 7 + q + 1, group * 128 : group * 128 + 128] = both[
                    group : group + 1
                ]


def pixels(result, row):
    half, i = row // 8, row % 8
    return jnp.concatenate(
        [result[pl.ds(i * 256 + half * 4 + group, 32, stride=8), :] for group in range(4)], axis=1
    )


def dot(left, right, left_dim=1, right_dim=0):
    return lax.dot_general(
        left, right, (((left_dim,), (right_dim,)), ((), ())), preferred_element_type=F32
    )


def gelu_and_slope(values):
    square = values * values
    share = 0.5 + 0.5 * jnp.tanh(values * (COEF + (COEF * CUBIC) * square))
    value = values * share
    slope = share + value * (1.0 - share) * (2.0 * COEF + (6.0 * COEF * CUBIC) * square)
    return value, slope


CHUNK = 256


def step_kernel(
    slides, cotangent, kernel, kernel_bias, norm_gain, norm_bias, bias_out, layer_scale, bias_in,
    shard_in, shard_out,
    output_end, grad_slides_end, final_in_end, final_out_end, final_small_end,
    output, grad_slides, final_in, final_out, final_small, leave_sems,
    full_in, full_out, padded0, padded1, padded_g0, padded_g1, result, taps,
    normed, rstd, normal, turned, act, slope, hidden_grad, branch, carry, upstream, low,
    gm_tile, middle, grad_in, grad_out, small,
    *rest,
):
    me = Place()
    gather = Gather(me, shard_in, shard_out, full_in, full_out, rest[:5])
    padded = (padded0, padded1)
    padded_g = (padded_g0, padded_g1)
    tiles = (slides, middle)
    halos = [
        Halo(me, grid, tile, rest[5 + 6 * k : 11 + 6 * k])
        for k, (grid, tile) in enumerate(
            ((padded0, slides), (padded1, middle), (padded_g1, gm_tile.at[1]), (padded_g0, gm_tile.at[0]))
        )
    ]
    scratch = rest[30:]
    ways = {}
    for number, (kind, which, early) in enumerate(UNITS):
        bufs = scratch[number * 8 : number * 8 + 7]
        sems = scratch[number * 8 + 7]
        if kind is WeightIn:
            ends = (grad_in.at[which], final_in.at[which])
        else:
            ends = (grad_out.at[which], final_out.at[which])
        ways[kind, which] = Reduction(me, kind, early, *ends, bufs, sems)

    leaving = []

    def send_out(source, target):
        copy = pltpu.make_async_copy(source, target, leave_sems.at[len(leaving)])
        copy.start()
        leaving.append(copy)

    little = SmallReduction(me, small, final_small, scratch[-4:-1], scratch[-1])

    def reducing(which):
        return [ways[WeightOut, which], ways[WeightIn, which]]

    def line(which, ref):
        return ref[which : which + 1, :]

    for which in range(2):
        for kind in range(2):
            gather.place(which, kind).start()

    scope = jax.named_scope

    def fill(grid, tile):
        for r in range(16):
            put_row(grid, r + 3, 3, tile[r * 32 : r * 32 + 32, :].astype(F32))

    partners = [me.along("x", offset)[1] for offset in (1, 2, 3)]
    partners += [device for _, _, _, device in little.others()]
    around = [
        halos[0].target(down, right) for down in (-1, 0, 1) for right in (-1, 0, 1) if down
    ]
    with scope("p00a_fill"):
        padded0[...] = jnp.zeros_like(padded0)
        padded1[...] = jnp.zeros_like(padded1)
        fill(padded0, slides)
        for which in range(2):
            spread_taps(kernel, which, taps.at[which])
        small[...] = jnp.zeros_like(small)
        carry[...] = jnp.zeros_like(carry)
    with scope("p00b_meet"):
        meet(partners + around + [me.sibling()])
    with scope("p00c_start"):
        halos[0].start()
        gather.start(0, 0)
        gather.start(0, 1)
        gather.start(1, 0)

    def filter_map(which, first, last):
        depthwise(padded[which], taps.at[which], result, False, first, last)

    def normalise(which):
        for r in range(16):
            rows = slice(r * 32, r * 32 + 32)
            mixed = pixels(result, r) + line(which, kernel_bias)
            center = mixed - jnp.mean(mixed, -1, keepdims=True)
            inverse = lax.rsqrt(jnp.mean(center * center, -1, keepdims=True) + EPSILON)
            values = center * inverse
            normed[which, rows, :] = values
            rstd[which, rows, :] = jnp.broadcast_to(inverse, (32, 128))
            normal[which, rows, :] = (values * line(which, norm_gain) + line(which, norm_bias)).astype(BF)

    def expand(which, tilts, first=0, last=2048 // CHUNK):
        def chunk(c, _):
            cols = part(c * CHUNK, CHUNK)
            hidden = dot(normal[which], full_in[which, :, cols]) + bias_in[which : which + 1, cols]
            value, tilt = gelu_and_slope(hidden)
            act[which, :, cols] = value.astype(BF)
            if tilts is None:
                grads = dot(low[...], full_out[which, cols, :], 1, 1) * tilt
                keep_hidden_grad(which, c, cols, grads)
            else:
                tilts[:, cols] = tilt.astype(BF)
            return 0

        lax.fori_loop(first, last, chunk, 0)

    def hidden_grads(which, tilts, last):
        def chunk(c, _):
            cols = part(c * CHUNK, CHUNK)
            grads = dot(low[...], full_out[which, cols, :], 1, 1) * tilts[:, cols].astype(F32)
            keep_hidden_grad(which, c, cols, grads)
            return 0

        lax.fori_loop(0, last, chunk, 0)

    def keep_hidden_grad(which, c, cols, grads):
        hidden_grad[:, cols] = grads.astype(BF)
        bias_grad[which : which + 1, cols] = jnp.sum(grads, 0, keepdims=True)

    bias_grad = rest[29]

    def contract(which):
        def chunk(n, _):
            cols = part(n * CHUNK, CHUNK)
            branch[which, :, cols] = (
                dot(act[which], full_out[which, :, cols]) + bias_out[which : which + 1, cols]
            )
            return 0

        lax.fori_loop(0, 512 // CHUNK, chunk, 0)

    def residual(which, into):
        for r in range(16):
            rows = slice(r * 32, r * 32 + 32)
            value = tiles[which][rows, :].astype(F32) + line(which, layer_scale) * branch[which, rows, :]
            into[rows, :] = value.astype(BF)

    def enter(which, read):
        for r in range(16):
            rows = slice(r * 32, r * 32 + 32)
            grads = read(rows) * line(which, layer_scale)
            low[rows, :] = grads.astype(BF)
            add_rows(which, 0, grads)

    def add_rows(which, slot, values):
        total = values[0:8] + values[8:16] + (values[16:24] + values[24:32])
        carry[which, slot] = carry[which, slot] + total

    def weight_grads(which):
        def chunk(c, _):
            cols = part(c * CHUNK, CHUNK)
            grad_out[which, cols, :] = dot(act[which, :, cols], low[...], 0, 0).astype(BF)
            grad_in[which, :, cols] = dot(turned[...], hidden_grad[:, cols]).astype(BF)
            return 0

        turned[...] = normal[which].T
        lax.fori_loop(0, 2048 // CHUNK, chunk, 0)

    def normal_grads(which, target):
        def chunk(n, _):
            rows = part(n * CHUNK, CHUNK)
            target[:, rows] = dot(hidden_grad[...], full_in[which, rows, :], 1, 1)
            return 0

        lax.fori_loop(0, 512 // CHUNK, chunk, 0)

    def leave(which, grads_ref):
        for r in range(16):
            rows = slice(r * 32, r * 32 + 32)
            grads = grads_ref[rows, :]
            values = normed[which, rows, :]
            add_rows(which, 2, grads)
            add_rows(which, 1, grads * values)
            scaled = grads * line(which, norm_gain)
            mean = jnp.mean(scaled, -1, keepdims=True)
            tilt = jnp.mean(scaled * values, -1, keepdims=True)
            mixed = (scaled - mean - values * tilt) * rstd[which, rows, 0:1]
            add_rows(which, 3, mixed)
            put_row(padded_g[which], r + 3, 3, mixed)
            gm_tile[which, rows, :] = mixed.astype(BF)

    def scale_grad(which, read):
        for r in range(16):
            rows = slice(r * 32, r * 32 + 32)
            add_rows(which, 4, read(rows) * branch[which, rows, :])

    def settle(which):
        for slot, row in ((3, 0), (1, 1), (2, 2), (0, 3), (4, 4)):
            at = which * 64 + 49 + row
            small[at : at + 1, :] = jnp.sum(carry[which, slot], 0, keepdims=True)
        for c in range(4):
            at = which * 64 + 54 + c
            small[at : at + 1, :] = bias_grad[which : which + 1, c * 512 : c * 512 + 512]

    def from_cotangent(rows):
        return cotangent[rows, :].astype(F32)

    def from_upstream(rows):
        return upstream[rows, :]

    with scope("p01_depth0"):
        enter(1, from_cotangent)
        filter_map(0, 0, 32)
    with scope("p01_halo0"):
        halos[0].finish()
    with scope("p01_rim0"):
        add_rim(padded0, taps.at[0], result)
    with scope("p02_forward_in0"):
        gather.forward(0, 0)
    with scope("p03_norm0"):
        normalise(0)
    with scope("p04_finish_in0"):
        gather.finish(0, 0)
    with scope("p05_expand0"):
        expand(0, slope, 0, 5)
    with scope("p05_forward_out0"):
        gather.forward(0, 1)
    with scope("p05_expand0b"):
        expand(0, slope, 5)
    with scope("p06_finish_out0"):
        gather.finish(0, 1)
    with scope("p06_contract0"):
        contract(0)
        residual(0, middle)
        fill(padded1, middle)
    with scope("p07_halo1"):
        halos[1].start()
        gather.start(1, 1)
        gather.forward(1, 0)
    with scope("p08_depth1"):
        filter_map(1, 0, 32)
    with scope("p08_halo1_end"):
        halos[1].finish()
    with scope("p09_norm1"):
        add_rim(padded1, taps.at[1], result)
        normalise(1)
    with scope("p09_finish_in1"):
        gather.finish(1, 0)
    with scope("p10_expand1"):
        expand(1, hidden_grad, 0, 2)
    with scope("p10_forward_out1"):
        gather.forward(1, 1)
    with scope("p10_expand1b"):
        expand(1, hidden_grad, 2, 4)
    with scope("p10_finish_out1"):
        gather.finish(1, 1)
    with scope("p11_expand1"):
        expand(1, None, 4)
        hidden_grads(1, hidden_grad, 4)
    with scope("p12_ngrads1"):
        normal_grads(1, upstream)
    with scope("p13_leave1"):
        leave(1, upstream)
        halos[2].start()
    out1, in1 = reducing(1)
    out0, in0 = reducing(0)

    def go(name, *group):
        with scope(name):
            for way in group:
                way.advance()

    with scope("p14_wgrads1"):
        weight_grads(1)
        out1.advance()
        in1.advance()
    with scope("p16_halo2_end"):
        halos[2].finish()
    with scope("p17_depth1"):
        depthwise(padded_g1, taps.at[1], result, True, 0, 10)
    go("p17_go1", out1, in1)
    with scope("p17_depth1b"):
        depthwise(padded_g1, taps.at[1], result, True, 10, 32)
        for r in range(16):
            rows = slice(r * 32, r * 32 + 32)
            upstream[rows, :] = from_cotangent(rows) + pixels(result, r)
    with scope("p18_enter0"):
        enter(0, from_upstream)
        scale_grad(0, from_upstream)

    with scope("p19_hidden0"):
        hidden_grads(0, slope, 2048 // CHUNK)
    with scope("p21_wgrads0"):
        weight_grads(0)
    in0.advance()
    out0.advance()
    go("p21_go1", out1, in1)
    with scope("p23_ngrads0"):
        normal_grads(0, normed.at[1])
    go("p23_go0", in0)
    with scope("p24_leave0"):
        leave(0, normed.at[1])
        halos[3].start()
    go("p25_go0", out0)
    with scope("p26_contract1"):
        contract(1)
        residual(1, output)
        send_out(output, output_end)
        scale_grad(1, from_cotangent)
        settle(1)
        settle(0)
    go("p27_go1", out1)
    with scope("p28_taps0"):
        tap_grads(padded0, padded_g0, small, 0, range(7))
    go("p29_go0", in0)
    go("p29_go1", in1)
    with scope("p29_taps1"):
        tap_grads(padded1, padded_g1, small, 64, range(7))
    little.advance()
    go("p30_go0", in0)
    go("p30_go0b", out0)
    go("p30_go1", in1, out1)
    with scope("p30_halo3_end"):
        halos[3].finish()
    with scope("p31_depth0"):
        depthwise(padded_g0, taps.at[0], result, True, 0, 16)
    go("p31_go", little, in0, out0, in1, out1)
    with scope("p33_depth0"):
        depthwise(padded_g0, taps.at[0], result, True, 16, 32)
    go("p33_go", in0, little, out0, in1)
    with scope("p33_depth0b"):
        for r in range(16):
            rows = slice(r * 32, r * 32 + 32)
            grad_slides[rows, :] = (upstream[rows, :] + pixels(result, r)).astype(BF)
        send_out(grad_slides, grad_slides_end)
    go("p34_go", in0, little, out0, out1)
    go("p35_go", in0, little, out0, in1)
    go("p36_go", in0, little, out0, out1, in1)
    every = [out1, in1, little, out0, in0]
    with scope("p38_rest"):
        while any(way.steps for way in every):
            for way in every:
                if way.steps:
                    way.advance()
    with scope("p39_drain"):
        for which in (1, 0):
            send_out(final_in.at[which], final_in_end.at[which])
            send_out(final_out.at[which], final_out_end.at[which])
        send_out(final_small, final_small_end)
        for way in every + halos + [gather]:
            way.drain()
        for copy in leaving:
            copy.wait()


def halo_scratch():
    return [
        pltpu.VMEM((2, 96, 512), BF),
        pltpu.VMEM((2, 192, 128), BF),
        pltpu.VMEM((2, 192, 128), BF),
        pltpu.VMEM((2, 2, 80, 128), BF),
        pltpu.VMEM((2, 2, 80, 128), BF),
        pltpu.SemaphoreType.DMA((2, 8)),
    ]


def whole_step(*operands):
    vmem = pl.BlockSpec(memory_space=pltpu.VMEM)
    grid = pltpu.VMEM((BACK * SPAN * 8, 128), F32)
    scratch = [
        pltpu.VMEM((512, 512), BF),
        pltpu.VMEM((512, 512), BF),
        pltpu.VMEM((2, 256, 2048), BF),
        pltpu.VMEM((2, 2048, 256), BF),
        pltpu.VMEM((128, 512), F32),
        pltpu.SemaphoreType.DMA((7,)),
        pltpu.VMEM((2, 512, 2048), BF),
        pltpu.VMEM((2, 2048, 512), BF),
        grid,
        grid,
        grid,
        grid,
        pltpu.VMEM((8 * 32 * 8, 128), F32),
        pltpu.VMEM((2, 49 * 8, 128), F32),
        pltpu.VMEM((2, 512, 512), F32),
        pltpu.VMEM((2, 512, 128), F32),
        pltpu.VMEM((2, 512, 512), BF),
        pltpu.VMEM((512, 512), BF),
        pltpu.VMEM((2, 512, 2048), BF),
        pltpu.VMEM((512, 2048), BF),
        pltpu.VMEM((512, 2048), BF),
        pltpu.VMEM((2, 512, 512), F32),
        pltpu.VMEM((2, 5, 8, 512), F32),
        pltpu.VMEM((512, 512), F32),
        pltpu.VMEM((512, 512), BF),
        pltpu.VMEM((2, 512, 512), BF),
        pltpu.VMEM((512, 512), BF),
        pltpu.VMEM((2, 512, 2048), BF),
        pltpu.VMEM((2, 2048, 512), BF),
        pltpu.VMEM((128, 512), F32),
    ]
    scratch += [pltpu.SemaphoreType.DMA((2, 2))]
    scratch += [pltpu.SemaphoreType.DMA((2, 2, 2)) for _ in range(4)]
    for _ in range(4):
        scratch += halo_scratch()
    extra = [pltpu.VMEM((2, 2048), F32)]
    reductions = sum([reduction_scratch(kind, early) for kind, _, early in UNITS], [])
    reductions += [
        pltpu.VMEM((64, 512), F32),
        pltpu.VMEM((16, 16, 128), F32),
        pltpu.VMEM((4, 16, 128), F32),
        pltpu.SemaphoreType.DMA((2, 64)),
    ]
    return pl.pallas_call(
        step_kernel,
        out_shape=(
            jax.ShapeDtypeStruct((512, 512), BF),
            jax.ShapeDtypeStruct((512, 512), BF),
            jax.ShapeDtypeStruct((2, 256, 2048), BF),
            jax.ShapeDtypeStruct((2, 2048, 256), BF),
            jax.ShapeDtypeStruct((128, 512), F32),
        ),
        in_specs=[vmem] * 9 + [pl.BlockSpec(memory_space=pl.ANY)] * 2,
        out_specs=[pl.BlockSpec(memory_space=pl.ANY)] * 5,
        scratch_shapes=scratch + extra + reductions,
        compiler_params=pltpu.CompilerParams(
            collective_id=0, has_side_effects=True, vmem_limit_bytes=67043328
        ),
        name="whole_step",
    )(*operands)


def unpack_kernel(
    output, grad_slides, total_in, total_out, small,
    output_end, slides_end, in_end, out_end, kernel_end, channel_end, bias_end,
    maps, low_in, low_out, wide_in, wide_out, get, put,
):
    steps = []
    for which in range(2):
        for cut in range(4):
            for ends, size in (
                ((total_in, low_in, wide_in, in_end), 64),
                ((total_out, low_out, wide_out, out_end), 512),
            ):
                steps.append([ref.at[which, pl.ds(cut * size, size), :] for ref in ends])
    steps.append([output, maps.at[0], maps.at[0], output_end])
    steps.append([grad_slides, maps.at[1], maps.at[1], slides_end])
    for number, (src, low, _, _) in enumerate(steps):
        pltpu.make_async_copy(src, low, get.at[number]).start()
    for number, (src, low, wide, dst) in enumerate(steps):
        pltpu.make_async_copy(src, low, get.at[number]).wait()
        if number < 16:
            wide[...] = low[...].astype(F32)
        pltpu.make_async_copy(wide, dst, put.at[number]).start()
    for which in range(2):
        base = which * 64
        for p in range(7):
            kernel_end[p, :, which, :] = small[base + p * 7 : base + p * 7 + 7, :]
        channel_end[:, which, :] = small[base + 49 : base + 54, :]
        for c in range(4):
            bias_end[which : which + 1, c * 512 : c * 512 + 512] = small[
                base + 54 + c : base + 55 + c, :
            ]
    for number, (_, _, wide, dst) in enumerate(steps):
        pltpu.make_async_copy(wide, dst, put.at[number]).wait()


def unpack(*results):
    vmem = pl.BlockSpec(memory_space=pltpu.VMEM)
    hbm = pl.BlockSpec(memory_space=pl.ANY)
    return pl.pallas_call(
        unpack_kernel,
        out_shape=(
            jax.ShapeDtypeStruct((512, 512), BF),
            jax.ShapeDtypeStruct((512, 512), BF),
            jax.ShapeDtypeStruct((2, 256, 2048), F32),
            jax.ShapeDtypeStruct((2, 2048, 256), F32),
            jax.ShapeDtypeStruct((7, 7, 2, 512), F32),
            jax.ShapeDtypeStruct((5, 2, 512), F32),
            jax.ShapeDtypeStruct((2, 2048), F32),
        ),
        in_specs=[hbm] * 4 + [vmem],
        out_specs=[hbm] * 4 + [vmem] * 3,
        scratch_shapes=[
            pltpu.VMEM((2, 512, 512), BF),
            pltpu.VMEM((2, 256, 2048), BF),
            pltpu.VMEM((2, 2048, 256), BF),
            pltpu.VMEM((2, 256, 2048), F32),
            pltpu.VMEM((2, 2048, 256), F32),
            pltpu.SemaphoreType.DMA((18,)),
            pltpu.SemaphoreType.DMA((18,)),
        ],
        compiler_params=pltpu.CompilerParams(vmem_limit_bytes=67043328),
        name="unpack",
    )(*results)


def per_device(
    slides,
    cotangent,
    kernel,
    kernel_bias,
    norm_gain,
    norm_bias,
    weight_in,
    bias_in,
    weight_out,
    bias_out,
    layer_scale,
):
    channels = slides.shape[-1]
    results = whole_step(
        slides.reshape(-1, channels),
        cotangent.reshape(-1, channels),
        kernel.transpose(1, 2, 0, 3),
        kernel_bias,
        norm_gain,
        norm_bias,
        bias_out,
        layer_scale,
        bias_in,
        weight_in,
        weight_out,
    )
    output, grad_slides, total_in, total_out, taps, sums, biases = unpack(*results)
    return (
        output.reshape(slides.shape),
        grad_slides.reshape(slides.shape),
        total_in,
        total_out,
        taps.transpose(2, 0, 1, 3),
        sums.transpose(1, 0, 2),
        biases,
    )


def solution(mesh):
    whole = P("dp", "row", "col", None)
    return jax.shard_map(
        per_device,
        mesh=mesh,
        in_specs=(whole, whole) + (P(),) * 4 + (P(None, "dp", None), P(), P(None, None, "dp"), P(), P()),
        out_specs=(whole, whole, P(None, "dp", None), P(None, None, "dp"), P(), P(), P()),
        check_vma=False,
    )
```
